32 devices in a mesh: groups: 2 (over y), seq: 4 (over z), exp: 2 (over x), rep: 2 (over core).
Axes of the slice: x: 2, y: 2, z: 4, core: 2. Of those that a mesh axis runs over, the one named last changes fastest.
Arguments:
- queries: bfloat16 [512, 4096], P(('groups', 'seq'), ('exp', 'rep')), parts along dimension 0, may hold values from -4 to 4
- key_rows: bfloat16 [512, 4096], P(('groups', 'seq'), ('exp', 'rep')), parts along dimension 0, may hold values from -4 to 4
- value_rows: bfloat16 [512, 4096], P(('groups', 'seq'), ('exp', 'rep')), parts along dimension 0, may hold values from -6 to 6
- decay_log: float32 [512, 32], P(('groups', 'seq'), ('exp', 'rep')), parts along dimension 0, may hold values from -1.5 to 0
- residual: bfloat16 [512, 4096], P(('groups', 'seq'), ('exp', 'rep')), parts along dimension 0, may hold values from -6 to 6
- out_gate: bfloat16 [512, 4096], P(('groups', 'seq'), ('exp', 'rep')), parts along dimension 0, may hold values from -6 to 6
- attn_gain: float32 [4096], P(('exp', 'rep')), may hold values from 0.1 to 1.9
- moe_gain: float32 [4096], P(('exp', 'rep')), may hold values from 0.1 to 1.9
- routes: int32 [512, 2], P(('groups', 'seq')), parts along dimension 0, may hold values from 0 to 31, as said below
- route_weights: float32 [512, 2], P(('groups', 'seq')), parts along dimension 0, may hold values from 0.3 to 1
- w_gate: bfloat16 [2, 4608, 4096], P('exp', 'seq'), may hold values from -0.09375 to 0.09375
- w_up: bfloat16 [2, 4608, 4096], P('exp', 'seq'), may hold values from -0.09375 to 0.09375
- w_down: bfloat16 [2, 4608, 4096], P('exp', 'seq'), may hold values from -0.09375 to 0.09375
Outputs:
- layer_out: bfloat16 [512, 4096], P(('groups', 'seq'), ('exp', 'rep')), parts along dimension 0
The draws below stay inside these ranges and needn't reach their ends.
There are 2 independent parts, one for each index of `groups`. The reference program is written for one: setup_inputs(seed, part) draws one part's arguments, and reference() takes and returns one part's arrays. A program takes and returns all parts, laid end to end along the dimension named above; an argument that names none is the same for every part. Nothing has to cross between parts.
Inputs may be any that keep to these rules, and one draw needn't show every extreme that they name: `routes`: each row names two different experts. Within each aligned block of 64 rows no expert is named by more than 6 rows, every expert is named in every block, and one expert below 2 is named by exactly 6 rows in every block.
All inputs are finite; a program needn't handle non-finite values.
Results may differ from the reference program's by a relative error of at most 0.01.
Values may be sent and summed in bfloat16 or wider, within the bound.
A program may use at most 64 MiB of HBM per device.

```python
from functools import partial
import jax
import jax.numpy as jnp
from jax import lax

HEAD = 128
HEAD_COUNT = 32
D = 4096
FF = 4608
ROUTED = 32
BLOCK = 64
EXPERTS = 2
CAP = 6
L = 256
N_SEQ = 4
N_EXP = 2


def draw_routes(key, part):
    blocks = N_SEQ
    unit = BLOCK // ROUTED
    half_count = ROUTED // 2
    random_subkeys = jax.random.split(jax.random.fold_in(key, 11), 4)
    hot_expert = jax.random.randint(random_subkeys[0], (), 0, N_EXP)
    shifts = jax.random.randint(random_subkeys[1], (blocks, half_count), -unit, unit + 1)
    shifts = jnp.where(jnp.arange(half_count)[None, :] == hot_expert, unit, shifts)
    counts = jnp.concatenate([2 * unit + shifts, 2 * unit - shifts], axis=1)
    bounds = jnp.cumsum(counts, axis=1)
    places = jnp.arange(2 * BLOCK)
    sorted_ids = jnp.sum((bounds[:, None, :] <= places[None, :, None]).astype(jnp.int32), axis=2)

    def shuffle(block_key):
        return jax.random.permutation(block_key, BLOCK)
    orders = jax.vmap(shuffle)(jax.random.split(random_subkeys[2], blocks))
    first_ids = jnp.take_along_axis(sorted_ids, orders, axis=1)
    second_ids = jnp.take_along_axis(sorted_ids, orders + BLOCK, axis=1)
    flips = jax.random.randint(random_subkeys[3], (blocks, BLOCK), 0, 2)
    left_ids = jnp.where(flips == 1, second_ids, first_ids)
    right_ids = jnp.where(flips == 1, first_ids, second_ids)
    return jnp.stack([left_ids, right_ids], axis=2).reshape(blocks * BLOCK, 2).astype(jnp.int32)


def draw_decay_log(key, part):
    sequence_length = BLOCK * N_SEQ
    random_subkeys = jax.random.split(jax.random.fold_in(key, 23), 7)
    fast_share = 0.5
    fast_heads = jax.random.uniform(random_subkeys[0], (HEAD_COUNT,)) < fast_share
    fast_rate = jnp.exp(jax.random.uniform(random_subkeys[1], (HEAD_COUNT,), minval=jnp.log(1.0 / 50.0), maxval=jnp.log(1.0 / 30.0)))
    slow_rate = -jnp.log(jax.random.uniform(random_subkeys[2], (HEAD_COUNT,), minval=0.8, maxval=0.95)) / sequence_length
    rates = jnp.where(fast_heads, fast_rate, slow_rate)
    block_factor = jnp.repeat(jax.random.uniform(random_subkeys[3], (N_SEQ, HEAD_COUNT), minval=0.6, maxval=1.5), BLOCK, axis=0)
    token_factor = jax.random.uniform(random_subkeys[4], (sequence_length, HEAD_COUNT), minval=0.5, maxval=1.5)
    steady_portion = -rates[None, :] * block_factor * token_factor
    surge_position = jax.random.randint(random_subkeys[5], (2, HEAD_COUNT), 0, sequence_length)
    surge_length = jnp.log(jax.random.uniform(random_subkeys[6], (2, HEAD_COUNT), minval=0.5, maxval=0.8))
    token_positions = jnp.arange(sequence_length)[:, None]
    surge_events = jnp.where(token_positions == surge_position[0][None, :], surge_length[0][None, :], 0.0)
    surge_events = surge_events + jnp.where(token_positions == surge_position[1][None, :], surge_length[1][None, :], 0.0)
    return (steady_portion + surge_events).astype(jnp.float32)


def steps_of(stream_key, shape, cuts, least, largest):
    level = 1.0
    for position, blocks in cuts:
        heights = jax.random.uniform(jax.random.fold_in(jax.random.fold_in(stream_key, 6), position), (blocks,), jnp.float32, least / len(cuts), largest / len(cuts))
        level = level * jnp.repeat(jnp.exp(heights), shape[position] // blocks).reshape((-1,) + (1,) * (len(shape) - 1 - position))
    return level


def scatter_about(stream_key, shape, scale, limit, cuts=(), kind=jnp.bfloat16):
    drawn = scale * jax.random.normal(stream_key, shape, jnp.float32)
    if cuts:
        drawn = drawn * steps_of(stream_key, shape, cuts, -0.22, 0.18)
    return jnp.clip(drawn, -limit, limit).astype(kind)


def setup_inputs(seed: int = 0, part: int = 0) -> dict:
    key_of = jax.random.split(jax.random.key(seed), 14)
    own_keys = jax.random.split(jax.random.fold_in(key_of[13], part), 14)
    return {
        "queries": scatter_about(own_keys[0], (L, D), 0.3, 4.0, ((0, 4), (1, 4))),
        "key_rows": scatter_about(own_keys[1], (L, D), 0.3, 4.0, ((0, 4), (1, 4))),
        "value_rows": scatter_about(own_keys[2], (L, D), 1.0, 6.0, ((0, 4), (1, 4))),
        "decay_log": draw_decay_log(jax.random.fold_in(jax.random.fold_in(key_of[13], part), 71), part),
        "residual": scatter_about(own_keys[4], (L, D), 1.0, 6.0, ((0, 4), (1, 4))),
        "out_gate": scatter_about(own_keys[5], (L, D), 1.0, 6.0, ((0, 4), (1, 4))),
        "attn_gain": jnp.clip(1.0 + 0.18 * jax.random.normal(key_of[6], (D,), jnp.float32), 0.1, 1.9),
        "moe_gain": jnp.clip(1.0 + 0.18 * jax.random.normal(key_of[7], (D,), jnp.float32), 0.1, 1.9),
        "routes": draw_routes(jax.random.fold_in(jax.random.fold_in(key_of[13], part), 71), part),
        "route_weights": jnp.clip(0.3 + 0.7 * jax.random.uniform(own_keys[9], (L, 2), jnp.float32) ** steps_of(own_keys[9], (L, 2), ((0, 4),), -0.2, 0.2), 0.3, 1.0),
        "w_gate": scatter_about(key_of[10], (EXPERTS, FF, D), D ** -0.5, 0.09375, ((0, 2), (1, 4))),
        "w_up": scatter_about(key_of[11], (EXPERTS, FF, D), D ** -0.5, 0.09375, ((0, 2), (1, 4))),
        "w_down": scatter_about(key_of[12], (EXPERTS, FF, D), FF ** -0.5, 0.09375, ((0, 2), (1, 4))),
    }


EPSILON = 1e-06

def slot_tables(route_block, weight_block, experts, capacity):
    expert_ids = jnp.arange(experts, dtype=jnp.int32)
    onehot = (route_block[:, :, None] == expert_ids[None, None, :]).astype(jnp.int32)
    tokens = route_block.shape[0]
    flat_hits = onehot.reshape(tokens * 2, experts)
    before = jnp.cumsum(flat_hits, axis=0) - flat_hits
    places = jnp.arange(capacity, dtype=jnp.int32)
    hit_table = flat_hits[:, :, None] * (before[:, :, None] == places[None, None, :]).astype(jnp.int32)
    hit_table = hit_table.astype(jnp.float32).reshape(tokens, 2, experts * capacity)
    dispatch = lax.optimization_barrier(jnp.sum(hit_table, axis=1))
    combine = lax.optimization_barrier(jnp.sum(hit_table * weight_block[:, :, None], axis=1))
    return (dispatch, combine)

def block_attention(carried, inputs):
    query_blk, key_blk, value_blk, decay_blk = inputs
    cumulative = jnp.cumsum(decay_blk, axis=0)
    token_positions = jnp.arange(decay_blk.shape[0])
    causal = (token_positions[:, None] >= token_positions[None, :])[:, :, None]
    log_gaps = cumulative[:, None, :] - cumulative[None, :, :]
    decay_mask = jnp.where(causal, jnp.exp(jnp.where(causal, log_gaps, 0.0)), 0.0)
    scores = jnp.einsum('thd,jhd->htj', query_blk.astype(jnp.float32), key_blk.astype(jnp.float32))
    mixing = (scores * jnp.transpose(decay_mask, (2, 0, 1))).astype(jnp.bfloat16)
    local_part = jnp.einsum('htj,jhd->thd', mixing.astype(jnp.float32), value_blk.astype(jnp.float32))
    lifted = query_blk.astype(jnp.float32) * jnp.exp(cumulative)[:, :, None]
    carried_part = jnp.einsum('thd,hde->the', lifted, carried, precision=lax.Precision.HIGHEST)
    ending = cumulative[-1]
    faded_keys = key_blk.astype(jnp.float32) * jnp.exp(ending[None, :] - cumulative)[:, :, None]
    block_state = jnp.einsum('jhd,jhe->hde', faded_keys, value_blk.astype(jnp.float32), precision=lax.Precision.HIGHEST)
    updated = jnp.exp(ending)[:, None, None] * carried + block_state
    return (updated, local_part + carried_part)

def expert_apply(items):
    slot_rows, gate_mat, up_mat, down_mat = items
    gate_val = jnp.dot(slot_rows, jnp.transpose(gate_mat), preferred_element_type=jnp.float32)
    up_val = jnp.dot(slot_rows, jnp.transpose(up_mat), preferred_element_type=jnp.float32)
    inner_act = (jax.nn.silu(gate_val) * up_val).astype(jnp.bfloat16)
    row_count = slot_rows.shape[0]
    model_width = down_mat.shape[1]
    slab_width = down_mat.shape[0] // N_SEQ
    inner_slabs = jnp.transpose(inner_act.reshape(row_count, N_SEQ, slab_width), (1, 0, 2))
    down_slabs = down_mat.reshape(N_SEQ, slab_width, model_width)

    def add_slab(running, slab_pair):
        slab_out = jnp.dot(slab_pair[0], slab_pair[1], preferred_element_type=jnp.float32).astype(jnp.bfloat16)
        slab_out = lax.optimization_barrier(slab_out)
        return (running + slab_out.astype(jnp.float32), None)
    running, _ = lax.scan(add_slab, jnp.zeros((row_count, model_width), jnp.float32), (inner_slabs, down_slabs))
    return running.astype(jnp.bfloat16)

def reference(queries, key_rows, value_rows, decay_log, residual, out_gate, attn_gain, moe_gain, routes, route_weights, w_gate, w_up, w_down):
    sequence_length = queries.shape[0]
    blocks = sequence_length // BLOCK
    model_width = HEAD_COUNT * HEAD
    query_blocks = queries.reshape(blocks, BLOCK, HEAD_COUNT, HEAD)
    key_blocks = key_rows.reshape(blocks, BLOCK, HEAD_COUNT, HEAD)
    value_blocks = value_rows.reshape(blocks, BLOCK, HEAD_COUNT, HEAD)
    decay_blocks = decay_log.reshape(blocks, BLOCK, HEAD_COUNT)
    start_state = jnp.zeros((HEAD_COUNT, HEAD, HEAD), jnp.float32)
    final_state, mixed_out = lax.scan(block_attention, start_state, (query_blocks, key_blocks, value_blocks, decay_blocks))
    attended = mixed_out.reshape(sequence_length, model_width)
    attn_scale = lax.rsqrt(lax.optimization_barrier(jnp.mean(attended * attended, axis=1, keepdims=True)) + EPSILON)
    hidden = residual.astype(jnp.float32) + jax.nn.sigmoid(out_gate.astype(jnp.float32)) * (attended * attn_scale * attn_gain)
    second = lax.rsqrt(lax.optimization_barrier(jnp.mean(hidden * hidden, axis=1, keepdims=True)) + EPSILON)
    normed = (hidden * second * moe_gain).astype(jnp.bfloat16)
    experts = w_gate.shape[0]
    tables = jax.vmap(partial(slot_tables, experts=experts, capacity=CAP))
    dispatch, combine = tables(routes.reshape(N_SEQ, BLOCK, 2), route_weights.reshape(N_SEQ, BLOCK, 2))
    gathered = jnp.einsum('sbc,sbd->scd', dispatch, normed.reshape(N_SEQ, BLOCK, model_width).astype(jnp.float32)).astype(jnp.bfloat16)
    per_expert = jnp.transpose(gathered.reshape(N_SEQ, experts, CAP, model_width), (1, 0, 2, 3)).reshape(experts, N_SEQ * CAP, model_width)
    outputs = lax.map(expert_apply, (per_expert, w_gate, w_up, w_down))
    returned = jnp.transpose(outputs.reshape(experts, N_SEQ, CAP, model_width), (1, 0, 2, 3)).reshape(N_SEQ, experts * CAP, model_width)
    expert_mix = jnp.einsum('sbc,scd->sbd', combine, returned.astype(jnp.float32), precision=lax.Precision.HIGHEST)
    return (hidden + expert_mix.reshape(sequence_length, model_width)).astype(jnp.bfloat16)
```

```python
import jax
import jax.numpy as jnp
from jax import lax
from jax.experimental import pallas as pl
from jax.experimental.pallas import tpu as pltpu
from jax.sharding import PartitionSpec as P

CAP = 6
SLOTS = 8
PARTS = 2
EPSILON = 1e-06
MESH = pl.DeviceIdType.MESH
F32 = jnp.float32
BF16 = jnp.bfloat16


def sweep(count, body):
    if count <= 16:
        for i in range(count):
            body(i)
    else:
        lax.fori_loop(0, count, lambda i, c: (body(i), c)[1], 0)


def nt_dot(a, b):
    return lax.dot_general(a, b, (((1,), (1,)), ((), ())), preferred_element_type=F32)


def kernel(
    n_seq,
    n_exp,
    n_rep,
    k_hbm,
    v_hbm,
    decay_hbm,
    q_hbm,
    routes_hbm,
    rw_hbm,
    res_hbm,
    gate_hbm,
    again_hbm,
    mgain_hbm,
    wg_hbm,
    wu_hbm,
    wd_hbm,
    out_ref,
    k_ref,
    v_ref,
    decay_ref,
    q_ref,
    routes_ref,
    rw_ref,
    res_ref,
    gate_ref,
    again_ref,
    mgain_ref,
    wg,
    wu,
    wd,
    state_in,
    state_out,
    block_state,
    att,
    u_buf,
    sums,
    pack,
    rows,
    half_send,
    half_recv,
    fin,
    back,
    in_sem,
    w_sem,
    go_sem,
    chain_send,
    chain_recv,
    sums_send,
    sums_recv,
    disp_send,
    disp_recv,
    swap_send,
    swap_recv,
    half_ssem,
    half_rsem,
    back_send,
    back_recv,
):
    z = lax.axis_index("seq")
    x = lax.axis_index("exp")
    r = lax.axis_index("rep")
    other = 1 - r
    tokens, columns = q_ref.shape
    heads = decay_ref.shape[0]
    hd = columns // heads
    part_rows = hd // PARTS
    hidden_rows = wg.shape[0]
    width = columns * n_exp * n_rep
    whole_rows = wg_hbm.shape[1]

    inputs = [
        pltpu.make_async_copy(src, dst, in_sem.at[i])
        for i, (src, dst) in enumerate(
            (
                (k_hbm, k_ref),
                (v_hbm, v_ref),
                (decay_hbm, decay_ref),
                (q_hbm, q_ref),
                (routes_hbm, routes_ref),
                (rw_hbm, rw_ref),
                (res_hbm, res_ref),
                (gate_hbm, gate_ref),
                (again_hbm, again_ref),
                (mgain_hbm, mgain_ref),
            )
        )
    ]
    for load in inputs:
        load.start()
    first = pl.multiple_of(r * hidden_rows, 16) if hidden_rows != whole_rows else 0
    loads = [
        pltpu.make_async_copy(src.at[0, pl.ds(first, hidden_rows), :], dst, w_sem.at[i])
        for i, (src, dst) in enumerate(((wg_hbm, wg), (wu_hbm, wu), (wd_hbm, wd)))
    ]

    barrier = pltpu.get_barrier_semaphore()
    plane = n_exp * n_seq
    peers = n_exp * n_rep
    me = x * n_rep + r
    last = n_seq - 1

    def greet(where):
        pl.semaphore_signal(barrier, inc=1, device_id=where, device_id_type=MESH)

    @pl.when(z < last)
    def _():
        greet({"seq": z + 1})

    @pl.when(z > 0)
    def _():
        greet({"seq": z - 1})

    def greet_peer(i):
        to = lax.rem(me + 1 + i, peers)
        greet({"exp": lax.div(to, n_rep), "rep": lax.rem(to, n_rep)})

    sweep(peers - 1, greet_peer)
    for load in loads:
        load.start()
    for load in inputs[:3]:
        load.wait()

    ti = lax.broadcasted_iota(jnp.int32, (tokens, tokens), 0)
    tj = lax.broadcasted_iota(jnp.int32, (tokens, tokens), 1)
    causal = ti >= tj
    upper = jnp.where(tj >= ti, 1.0, 0.0).astype(F32)
    cum_t = jnp.dot(
        decay_ref[...], upper, precision=lax.Precision.HIGHEST, preferred_element_type=F32
    )
    cum = jnp.transpose(cum_t)
    ending = cum[tokens - 1 : tokens, :]
    fading = jnp.exp(ending)
    to_end = jnp.exp(ending - cum)
    lift = jnp.exp(cum)
    for h in range(heads):
        cols = slice(h * hd, (h + 1) * hd)
        faded = k_ref[:, cols].astype(F32) * to_end[:, h : h + 1]
        block_state[h] = jnp.dot(
            jnp.transpose(faded).astype(BF16), v_ref[:, cols], preferred_element_type=F32
        )

    ends = (z > 0).astype(jnp.int32) + (z < last).astype(jnp.int32)
    pl.semaphore_wait(barrier, peers - 1 + ends)

    def hop(h, p):
        piece = pl.ds(p * part_rows, part_rows)
        return pltpu.make_async_remote_copy(
            src_ref=state_out.at[h, piece],
            dst_ref=state_in.at[h, piece],
            send_sem=chain_send.at[h, p],
            recv_sem=chain_recv.at[h, p],
            device_id={"seq": z + 1},
            device_id_type=MESH,
        )

    @pl.when(z == 0)
    def _():
        for h in range(heads):
            state_out[h] = block_state[h].astype(BF16)
            for p in range(PARTS):
                hop(h, p).start()

    inputs[3].wait()

    for h in range(heads):
        cols = slice(h * hd, (h + 1) * hd)
        scores = nt_dot(q_ref[:, cols], k_ref[:, cols])
        gaps = cum[:, h : h + 1] - cum_t[h : h + 1, :]
        mixing = jnp.where(causal, scores * jnp.exp(jnp.where(causal, gaps, 0.0)), 0.0)
        att[:, cols] = jnp.dot(mixing.astype(BF16), v_ref[:, cols], preferred_element_type=F32)

    for load in inputs[4:]:
        load.wait()
    lane = lax.broadcasted_iota(jnp.int32, (tokens, 128), 1)
    expert_of = lax.div(lane, SLOTS)
    slot_of = lax.rem(lane, SLOTS)
    named = jnp.transpose(routes_ref[...].astype(F32)).astype(jnp.int32)
    shares = jnp.transpose(rw_ref[...])
    first_hit = named[:, 0:1] == expert_of
    second_hit = named[:, 1:2] == expert_of
    hit = jnp.where(first_hit | second_hit, 1.0, 0.0)
    strict = jnp.where(ti > tj, 1.0, 0.0).astype(BF16)
    before = jnp.dot(strict, hit.astype(BF16), preferred_element_type=F32)
    taken = (hit > 0.5) & (before.astype(jnp.int32) == slot_of) & (slot_of < CAP)
    onehot = jnp.where(taken, 1.0, 0.0)
    combine = jnp.where(first_hit, shares[:, 0:1], shares[:, 1:2]) * onehot
    dispatch = jnp.transpose(onehot)[0 : n_exp * SLOTS, :].astype(BF16)

    def let_go(i):
        pl.semaphore_signal(go_sem, inc=1, device_id={"seq": i}, device_id_type=MESH)

    for h in range(heads):
        cols = slice(h * hd, (h + 1) * hd)

        @pl.when(z > 0)
        def _():
            for p in range(PARTS):
                piece = slice(p * part_rows, (p + 1) * part_rows)
                hop(h, p).wait_recv()

                @pl.when(z < last)
                def _():
                    state_out[h, piece] = (
                        fading[:, h : h + 1] * state_in[h, piece].astype(F32)
                        + block_state[h, piece]
                    ).astype(BF16)
                    hop(h, p).start()

            lifted = (q_ref[:, cols].astype(F32) * lift[:, h : h + 1]).astype(BF16)
            att[:, cols] += jnp.dot(lifted, state_in[h], preferred_element_type=F32)

        if h == max(heads - 3, 0):

            @pl.when(z == last)
            def _():
                sweep(last, let_go)

    res = res_ref[...].astype(F32)
    attended = att[...]
    u = jax.nn.sigmoid(gate_ref[...].astype(F32)) * attended * again_ref[...]
    u_buf[...] = u
    parts = (attended * attended, res * u, u * u, res * res)
    table = jnp.zeros((tokens, 128), F32)
    for i, part in enumerate(parts):
        table = jnp.where(lane == i, jnp.sum(part, axis=1, keepdims=True), table)
    sums[me] = jnp.transpose(table)[0:8, :]

    def tell(i):
        to = lax.rem(me + 1 + i, peers)
        pltpu.make_async_remote_copy(
            src_ref=sums.at[me],
            dst_ref=sums.at[me],
            send_sem=sums_send,
            recv_sem=sums_recv,
            device_id={"exp": lax.div(to, n_rep), "rep": lax.rem(to, n_rep)},
            device_id_type=MESH,
        ).start()

    sweep(peers - 1, tell)
    many = sums.at[pl.ds(0, peers - 1)]
    pltpu.make_async_copy(many, many, sums_recv).wait()
    total = jnp.sum(sums[...], axis=0)
    s1 = lax.rsqrt(total[0:1, :] / width + EPSILON)
    moe = total[3:4, :] + s1 * (2.0 * total[1:2, :] + s1 * total[2:3, :])
    s2 = lax.rsqrt(jnp.maximum(moe, 0.0) / width + EPSILON)
    row8 = lax.broadcasted_iota(jnp.int32, (8, tokens), 0)
    scales = jnp.transpose(jnp.where(row8 == 0, s1, s2))
    hidden = res_ref[...].astype(F32) + scales[:, 0:1] * u_buf[...]
    u_buf[...] = hidden
    normed = (hidden * scales[:, 1:2] * mgain_ref[...]).astype(BF16)

    packed = jnp.dot(dispatch, normed, preferred_element_type=F32)
    for e in range(n_exp):
        pack[e] = packed[e * SLOTS : (e + 1) * SLOTS, :].astype(BF16)
    here = x * n_seq + z
    rows[r, here] = pack[x]

    def deal(e, to, source, target, send_sem, recv_sem):
        pltpu.make_async_remote_copy(
            src_ref=source,
            dst_ref=target,
            send_sem=send_sem,
            recv_sem=recv_sem,
            device_id={"exp": e, "seq": to},
            device_id_type=MESH,
        ).start()

    def deal_rows(e, to):
        used = pl.ds(0, CAP)
        deal(e, to, pack.at[e, used], rows.at[r, here, used], disp_send, disp_recv)

    def earlier(send):
        def one(i):
            @pl.when(i < z)
            def _():
                for e in range(n_exp):
                    send(e, i)

        sweep(n_seq, one)

    def level(send):
        for j in range(1, n_exp):
            send(lax.rem(x + j, n_exp), z)

    def later(send):
        def one(i):
            @pl.when(last - i > z)
            def _():
                for e in range(n_exp):
                    send(e, last - i)

        sweep(n_seq, one)

    earlier(deal_rows)
    level(deal_rows)

    @pl.when(z < last)
    def _():
        pl.semaphore_wait(go_sem, 1)

    later(deal_rows)
    arrived = rows.at[r, pl.ds(0, plane - 1), pl.ds(0, CAP)]
    pltpu.make_async_copy(arrived, arrived, disp_recv).wait()
    swap = pltpu.make_async_remote_copy(
        src_ref=rows.at[r],
        dst_ref=rows.at[r],
        send_sem=swap_send,
        recv_sem=swap_recv,
        device_id={"rep": other},
        device_id_type=MESH,
    )
    swap.start()
    for load in loads:
        load.wait()
    slots = n_seq * SLOTS

    def project(s):
        gate_part = up_part = 0.0
        for e in range(n_exp):
            chunk = rows[s, pl.ds(e * n_seq, n_seq)].astype(F32).reshape(slots, columns)
            chunk = chunk.astype(BF16)
            at = pl.ds(pl.multiple_of((e * n_rep + s) * columns, 128), columns)
            gate_part += nt_dot(wg[:, at], chunk)
            up_part += nt_dot(wu[:, at], chunk)
        return gate_part, up_part

    gate_val, up_val = project(r)
    swap.wait()
    gate_part, up_part = project(other)
    gate_val += gate_part
    up_val += up_part
    inner = gate_val / (1.0 + jnp.exp(-gate_val)) * up_val
    if hidden_rows == whole_rows:
        unit = lax.broadcasted_iota(jnp.int32, inner.shape, 0)
        inner = jnp.where(lax.div(unit, whole_rows // n_rep) == r, inner, 0.0)
    inner = jnp.transpose(inner).astype(BF16)

    def product(e, s):
        at = pl.multiple_of((e * n_rep + s) * columns, 128)
        return jnp.dot(inner, wd[:, pl.ds(at, columns)], preferred_element_type=F32)

    def half(e):
        return pltpu.make_async_remote_copy(
            src_ref=half_send.at[e],
            dst_ref=half_recv.at[e],
            send_sem=half_ssem.at[e],
            recv_sem=half_rsem.at[e],
            device_id={"rep": other},
            device_id_type=MESH,
        )

    for e in range(n_exp):
        half_send[e] = product(e, other).astype(BF16)
        half(e).start()

    here_back = x * n_seq + z
    for e in range(n_exp):
        own = product(e, r)
        half(e).wait_recv()
        whole = (own + half_recv[e].astype(F32)).reshape(n_seq, SLOTS, columns)
        fin[pl.ds(e * n_seq, n_seq)] = whole.astype(BF16)

    back[here_back] = fin[here_back]

    def hand_back(e, to):
        used = pl.ds(0, CAP)
        source = fin.at[e * n_seq + to, used]
        deal(e, to, source, back.at[here_back, used], back_send, back_recv)

    earlier(hand_back)
    later(hand_back)
    level(hand_back)
    returned = back.at[pl.ds(0, plane - 1), pl.ds(0, CAP)]
    pltpu.make_async_copy(returned, returned, back_recv).wait()
    coarse = combine.astype(BF16)
    fine = (combine - coarse.astype(F32)).astype(BF16)
    result = u_buf[...]
    for e in range(n_exp):
        rows_e = jnp.sum(back[pl.ds(e * n_seq, n_seq)].astype(F32), axis=0)
        slot = lax.broadcasted_iota(jnp.int32, rows_e.shape, 0)
        rows_e = jnp.where(slot < CAP, rows_e, 0.0).astype(BF16)
        lanes = slice(e * SLOTS, (e + 1) * SLOTS)
        result += jnp.dot(coarse[:, lanes], rows_e, preferred_element_type=F32)
        result += jnp.dot(fine[:, lanes], rows_e, preferred_element_type=F32)
    out_ref[...] = result.astype(BF16)

    for h in range(heads):

        @pl.when(z < last)
        def _():
            for p in range(PARTS):
                hop(h, p).wait_send()

    pltpu.make_async_copy(many, many, sums_send).wait()
    pltpu.make_async_copy(arrived, arrived, disp_send).wait()
    for e in range(n_exp):
        half(e).wait_send()
    pltpu.make_async_copy(returned, returned, back_send).wait()


def solution(mesh):
    n_seq, n_exp, n_rep = (mesh.shape[a] for a in ("seq", "exp", "rep"))

    def shards(
        queries,
        key_rows,
        value_rows,
        decay_log,
        residual,
        out_gate,
        attn_gain,
        moe_gain,
        routes,
        route_weights,
        w_gate,
        w_up,
        w_down,
    ):
        tokens, columns = queries.shape
        heads = decay_log.shape[1]
        hd = columns // heads
        _, whole_rows, width = w_gate.shape
        even = whole_rows % (16 * n_rep) == 0
        hidden_rows = whole_rows // n_rep if even else whole_rows
        plane = n_exp * n_seq
        slots = n_seq * SLOTS
        vmem = pl.BlockSpec(memory_space=pltpu.VMEM)
        hbm = pl.BlockSpec(memory_space=pltpu.HBM)
        dma = pltpu.SemaphoreType.DMA
        return pl.pallas_call(
            lambda *refs: kernel(n_seq, n_exp, n_rep, *refs),
            name="layer",
            out_shape=pltpu.VMEM((tokens, columns), BF16),
            in_specs=[hbm] * 13,
            out_specs=vmem,
            scratch_shapes=[
                pltpu.VMEM((tokens, columns), BF16),
                pltpu.VMEM((tokens, columns), BF16),
                pltpu.VMEM((heads, tokens), F32),
                pltpu.VMEM((tokens, columns), BF16),
                pltpu.VMEM((2, tokens), jnp.int32),
                pltpu.VMEM((2, tokens), F32),
                pltpu.VMEM((tokens, columns), BF16),
                pltpu.VMEM((tokens, columns), BF16),
                pltpu.VMEM((1, columns), F32),
                pltpu.VMEM((1, columns), F32),
                pltpu.VMEM((hidden_rows, width), BF16),
                pltpu.VMEM((hidden_rows, width), BF16),
                pltpu.VMEM((hidden_rows, width), BF16),
                pltpu.VMEM((heads, hd, hd), BF16),
                pltpu.VMEM((heads, hd, hd), BF16),
                pltpu.VMEM((heads, hd, hd), F32),
                pltpu.VMEM((tokens, columns), F32),
                pltpu.VMEM((tokens, columns), F32),
                pltpu.VMEM((n_exp * n_rep, 8, tokens), F32),
                pltpu.VMEM((n_exp, SLOTS, columns), BF16),
                pltpu.VMEM((n_rep, plane, SLOTS, columns), BF16),
                pltpu.VMEM((n_exp, slots, columns), BF16),
                pltpu.VMEM((n_exp, slots, columns), BF16),
                pltpu.VMEM((plane, SLOTS, columns), BF16),
                pltpu.VMEM((plane, SLOTS, columns), BF16),
                dma((10,)),
                dma((3,)),
                pltpu.SemaphoreType.REGULAR,
                dma((heads, PARTS)),
                dma((heads, PARTS)),
                dma,
                dma,
                dma,
                dma,
                dma,
                dma,
                dma((n_exp,)),
                dma((n_exp,)),
                dma,
                dma,
            ],
            compiler_params=pltpu.CompilerParams(collective_id=0, has_side_effects=True, vmem_limit_bytes=63000000),
        )(
            key_rows,
            value_rows,
            decay_log.T,
            queries,
            routes.T,
            route_weights.T,
            residual,
            out_gate,
            attn_gain.reshape(1, columns),
            moe_gain.reshape(1, columns),
            w_gate,
            w_up,
            w_down,
        )

    block = P(("groups", "seq"), ("exp", "rep"))
    gain = P(("exp", "rep"))
    route = P(("groups", "seq"), None)
    weight = P("exp", "seq", None)
    return jax.shard_map(
        shards,
        mesh=mesh,
        in_specs=(block,) * 6 + (gain, gain, route, route) + (weight,) * 3,
        out_specs=block,
        check_vma=False,
    )
```

```python
import jax
import jax.numpy as jnp
from jax import lax
from jax.experimental import pallas as pl
from jax.experimental.pallas import tpu as pltpu
from jax.sharding import PartitionSpec as P

CAP = 6
SLOTS = 8
PARTS = 2
SHORT = 4
EPSILON = 1e-06
MESH = pl.DeviceIdType.MESH
F32 = jnp.float32
BF16 = jnp.bfloat16


def sweep(count, body):
    if count <= 16:
        for i in range(count):
            body(i)
    else:
        lax.fori_loop(0, count, lambda i, c: (body(i), c)[1], 0)


def nt_dot(a, b):
    return lax.dot_general(a, b, (((1,), (1,)), ((), ())), preferred_element_type=F32)


def chain_kernel(
    n_seq,
    n_exp,
    n_rep,
    k_hbm,
    v_hbm,
    decay_hbm,
    q_hbm,
    routes_hbm,
    rw_hbm,
    res_hbm,
    gate_hbm,
    again_hbm,
    mgain_hbm,
    wg_hbm,
    wu_hbm,
    wd_hbm,
    out_ref,
    k_ref,
    v_ref,
    decay_ref,
    q_ref,
    routes_ref,
    rw_ref,
    res_ref,
    gate_ref,
    again_ref,
    mgain_ref,
    wg,
    wu,
    wd,
    state_in,
    state_out,
    block_state,
    att,
    u_buf,
    sums,
    pack,
    rows,
    half_send,
    half_recv,
    fin,
    back,
    in_sem,
    w_sem,
    go_sem,
    chain_send,
    chain_recv,
    sums_send,
    sums_recv,
    disp_send,
    disp_recv,
    swap_send,
    swap_recv,
    half_ssem,
    half_rsem,
    back_send,
    back_recv,
):
    z = lax.axis_index("seq")
    x = lax.axis_index("exp")
    r = lax.axis_index("rep")
    other = 1 - r
    tokens, columns = q_ref.shape
    heads = decay_ref.shape[0]
    hd = columns // heads
    part_rows = hd // PARTS
    hidden_rows = wg.shape[0]
    width = columns * n_exp * n_rep
    whole_rows = wg_hbm.shape[1]

    inputs = [
        pltpu.make_async_copy(src, dst, in_sem.at[i])
        for i, (src, dst) in enumerate(
            (
                (k_hbm, k_ref),
                (v_hbm, v_ref),
                (decay_hbm, decay_ref),
                (q_hbm, q_ref),
                (routes_hbm, routes_ref),
                (rw_hbm, rw_ref),
                (res_hbm, res_ref),
                (gate_hbm, gate_ref),
                (again_hbm, again_ref),
                (mgain_hbm, mgain_ref),
            )
        )
    ]
    for load in inputs:
        load.start()
    first = pl.multiple_of(r * hidden_rows, 16) if hidden_rows != whole_rows else 0
    loads = [
        pltpu.make_async_copy(src.at[0, pl.ds(first, hidden_rows), :], dst, w_sem.at[i])
        for i, (src, dst) in enumerate(((wg_hbm, wg), (wu_hbm, wu), (wd_hbm, wd)))
    ]

    barrier = pltpu.get_barrier_semaphore()
    plane = n_exp * n_seq
    peers = n_exp * n_rep
    me = x * n_rep + r
    last = n_seq - 1

    def greet(where):
        pl.semaphore_signal(barrier, inc=1, device_id=where, device_id_type=MESH)

    @pl.when(z < last)
    def _():
        greet({"seq": z + 1})

    @pl.when(z > 0)
    def _():
        greet({"seq": z - 1})

    def greet_peer(i):
        to = lax.rem(me + 1 + i, peers)
        greet({"exp": lax.div(to, n_rep), "rep": lax.rem(to, n_rep)})

    sweep(peers - 1, greet_peer)
    for load in loads:
        load.start()
    for load in inputs[:3]:
        load.wait()

    ti = lax.broadcasted_iota(jnp.int32, (tokens, tokens), 0)
    tj = lax.broadcasted_iota(jnp.int32, (tokens, tokens), 1)
    causal = ti >= tj
    upper = jnp.where(tj >= ti, 1.0, 0.0).astype(F32)
    cum_t = jnp.dot(
        decay_ref[...], upper, precision=lax.Precision.HIGHEST, preferred_element_type=F32
    )
    cum = jnp.transpose(cum_t)
    ending = cum[tokens - 1 : tokens, :]
    fading = jnp.exp(ending)
    to_end = jnp.exp(ending - cum)
    lift = jnp.exp(cum)
    for h in range(heads):
        cols = slice(h * hd, (h + 1) * hd)
        faded = k_ref[:, cols].astype(F32) * to_end[:, h : h + 1]
        block_state[h] = jnp.dot(
            jnp.transpose(faded).astype(BF16), v_ref[:, cols], preferred_element_type=F32
        )

    ends = (z > 0).astype(jnp.int32) + (z < last).astype(jnp.int32)
    pl.semaphore_wait(barrier, peers - 1 + ends)

    def hop(h, p):
        piece = pl.ds(p * part_rows, part_rows)
        return pltpu.make_async_remote_copy(
            src_ref=state_out.at[h, piece],
            dst_ref=state_in.at[h, piece],
            send_sem=chain_send.at[h, p],
            recv_sem=chain_recv.at[h, p],
            device_id={"seq": z + 1},
            device_id_type=MESH,
        )

    @pl.when(z == 0)
    def _():
        for h in range(heads):
            state_out[h] = block_state[h].astype(BF16)
            for p in range(PARTS):
                hop(h, p).start()

    inputs[3].wait()

    for h in range(heads):
        cols = slice(h * hd, (h + 1) * hd)
        scores = nt_dot(q_ref[:, cols], k_ref[:, cols])
        gaps = cum[:, h : h + 1] - cum_t[h : h + 1, :]
        mixing = jnp.where(causal, scores * jnp.exp(jnp.where(causal, gaps, 0.0)), 0.0)
        att[:, cols] = jnp.dot(mixing.astype(BF16), v_ref[:, cols], preferred_element_type=F32)

    for load in inputs[4:]:
        load.wait()
    lane = lax.broadcasted_iota(jnp.int32, (tokens, 128), 1)
    expert_of = lax.div(lane, SLOTS)
    slot_of = lax.rem(lane, SLOTS)
    named = jnp.transpose(routes_ref[...].astype(F32)).astype(jnp.int32)
    shares = jnp.transpose(rw_ref[...])
    first_hit = named[:, 0:1] == expert_of
    second_hit = named[:, 1:2] == expert_of
    hit = jnp.where(first_hit | second_hit, 1.0, 0.0)
    strict = jnp.where(ti > tj, 1.0, 0.0).astype(BF16)
    before = jnp.dot(strict, hit.astype(BF16), preferred_element_type=F32)
    taken = (hit > 0.5) & (before.astype(jnp.int32) == slot_of) & (slot_of < CAP)
    onehot = jnp.where(taken, 1.0, 0.0)
    combine = jnp.where(first_hit, shares[:, 0:1], shares[:, 1:2]) * onehot
    dispatch = jnp.transpose(onehot)[0 : n_exp * SLOTS, :].astype(BF16)

    def let_go(i):
        pl.semaphore_signal(go_sem, inc=1, device_id={"seq": i}, device_id_type=MESH)

    for h in range(heads):
        cols = slice(h * hd, (h + 1) * hd)

        @pl.when(z > 0)
        def _():
            for p in range(PARTS):
                piece = slice(p * part_rows, (p + 1) * part_rows)
                hop(h, p).wait_recv()

                @pl.when(z < last)
                def _():
                    state_out[h, piece] = (
                        fading[:, h : h + 1] * state_in[h, piece].astype(F32)
                        + block_state[h, piece]
                    ).astype(BF16)
                    hop(h, p).start()

            lifted = (q_ref[:, cols].astype(F32) * lift[:, h : h + 1]).astype(BF16)
            att[:, cols] += jnp.dot(lifted, state_in[h], preferred_element_type=F32)

        if h == max(heads - 3, 0):

            @pl.when(z == last)
            def _():
                sweep(last, let_go)

    res = res_ref[...].astype(F32)
    attended = att[...]
    u = jax.nn.sigmoid(gate_ref[...].astype(F32)) * attended * again_ref[...]
    u_buf[...] = u
    parts = (attended * attended, res * u, u * u, res * res)
    table = jnp.zeros((tokens, 128), F32)
    for i, part in enumerate(parts):
        table = jnp.where(lane == i, jnp.sum(part, axis=1, keepdims=True), table)
    sums[me] = jnp.transpose(table)[0:8, :]

    def tell(i):
        to = lax.rem(me + 1 + i, peers)
        pltpu.make_async_remote_copy(
            src_ref=sums.at[me],
            dst_ref=sums.at[me],
            send_sem=sums_send,
            recv_sem=sums_recv,
            device_id={"exp": lax.div(to, n_rep), "rep": lax.rem(to, n_rep)},
            device_id_type=MESH,
        ).start()

    sweep(peers - 1, tell)
    many = sums.at[pl.ds(0, peers - 1)]
    pltpu.make_async_copy(many, many, sums_recv).wait()
    total = jnp.sum(sums[...], axis=0)
    s1 = lax.rsqrt(total[0:1, :] / width + EPSILON)
    moe = total[3:4, :] + s1 * (2.0 * total[1:2, :] + s1 * total[2:3, :])
    s2 = lax.rsqrt(jnp.maximum(moe, 0.0) / width + EPSILON)
    row8 = lax.broadcasted_iota(jnp.int32, (8, tokens), 0)
    scales = jnp.transpose(jnp.where(row8 == 0, s1, s2))
    hidden = res_ref[...].astype(F32) + scales[:, 0:1] * u_buf[...]
    u_buf[...] = hidden
    normed = (hidden * scales[:, 1:2] * mgain_ref[...]).astype(BF16)

    packed = jnp.dot(dispatch, normed, preferred_element_type=F32)
    for e in range(n_exp):
        pack[e] = packed[e * SLOTS : (e + 1) * SLOTS, :].astype(BF16)
    here = x * n_seq + z
    rows[r, here] = pack[x]

    def deal(e, to, source, target, send_sem, recv_sem):
        pltpu.make_async_remote_copy(
            src_ref=source,
            dst_ref=target,
            send_sem=send_sem,
            recv_sem=recv_sem,
            device_id={"exp": e, "seq": to},
            device_id_type=MESH,
        ).start()

    def deal_rows(e, to):
        used = pl.ds(0, CAP)
        deal(e, to, pack.at[e, used], rows.at[r, here, used], disp_send, disp_recv)

    def earlier(send):
        def one(i):
            @pl.when(i < z)
            def _():
                for e in range(n_exp):
                    send(e, i)

        sweep(n_seq, one)

    def level(send):
        for j in range(1, n_exp):
            send(lax.rem(x + j, n_exp), z)

    def later(send):
        def one(i):
            @pl.when(last - i > z)
            def _():
                for e in range(n_exp):
                    send(e, last - i)

        sweep(n_seq, one)

    earlier(deal_rows)
    level(deal_rows)

    @pl.when(z < last)
    def _():
        pl.semaphore_wait(go_sem, 1)

    later(deal_rows)
    arrived = rows.at[r, pl.ds(0, plane - 1), pl.ds(0, CAP)]
    pltpu.make_async_copy(arrived, arrived, disp_recv).wait()
    swap = pltpu.make_async_remote_copy(
        src_ref=rows.at[r],
        dst_ref=rows.at[r],
        send_sem=swap_send,
        recv_sem=swap_recv,
        device_id={"rep": other},
        device_id_type=MESH,
    )
    swap.start()
    for load in loads:
        load.wait()
    slots = n_seq * SLOTS

    def project(s):
        gate_part = up_part = 0.0
        for e in range(n_exp):
            chunk = rows[s, pl.ds(e * n_seq, n_seq)].astype(F32).reshape(slots, columns)
            chunk = chunk.astype(BF16)
            at = pl.ds(pl.multiple_of((e * n_rep + s) * columns, 128), columns)
            gate_part += nt_dot(wg[:, at], chunk)
            up_part += nt_dot(wu[:, at], chunk)
        return gate_part, up_part

    gate_val, up_val = project(r)
    swap.wait()
    gate_part, up_part = project(other)
    gate_val += gate_part
    up_val += up_part
    inner = gate_val / (1.0 + jnp.exp(-gate_val)) * up_val
    if hidden_rows == whole_rows:
        unit = lax.broadcasted_iota(jnp.int32, inner.shape, 0)
        inner = jnp.where(lax.div(unit, whole_rows // n_rep) == r, inner, 0.0)
    inner = jnp.transpose(inner).astype(BF16)

    def product(e, s):
        at = pl.multiple_of((e * n_rep + s) * columns, 128)
        return jnp.dot(inner, wd[:, pl.ds(at, columns)], preferred_element_type=F32)

    def half(e):
        return pltpu.make_async_remote_copy(
            src_ref=half_send.at[e],
            dst_ref=half_recv.at[e],
            send_sem=half_ssem.at[e],
            recv_sem=half_rsem.at[e],
            device_id={"rep": other},
            device_id_type=MESH,
        )

    for e in range(n_exp):
        half_send[e] = product(e, other).astype(BF16)
        half(e).start()

    here_back = x * n_seq + z
    for e in range(n_exp):
        own = product(e, r)
        half(e).wait_recv()
        whole = (own + half_recv[e].astype(F32)).reshape(n_seq, SLOTS, columns)
        fin[pl.ds(e * n_seq, n_seq)] = whole.astype(BF16)

    back[here_back] = fin[here_back]

    def hand_back(e, to):
        used = pl.ds(0, CAP)
        source = fin.at[e * n_seq + to, used]
        deal(e, to, source, back.at[here_back, used], back_send, back_recv)

    earlier(hand_back)
    later(hand_back)
    level(hand_back)
    returned = back.at[pl.ds(0, plane - 1), pl.ds(0, CAP)]
    pltpu.make_async_copy(returned, returned, back_recv).wait()
    coarse = combine.astype(BF16)
    fine = (combine - coarse.astype(F32)).astype(BF16)
    result = u_buf[...]
    for e in range(n_exp):
        rows_e = jnp.sum(back[pl.ds(e * n_seq, n_seq)].astype(F32), axis=0)
        slot = lax.broadcasted_iota(jnp.int32, rows_e.shape, 0)
        rows_e = jnp.where(slot < CAP, rows_e, 0.0).astype(BF16)
        lanes = slice(e * SLOTS, (e + 1) * SLOTS)
        result += jnp.dot(coarse[:, lanes], rows_e, preferred_element_type=F32)
        result += jnp.dot(fine[:, lanes], rows_e, preferred_element_type=F32)
    out_ref[...] = result.astype(BF16)

    for h in range(heads):

        @pl.when(z < last)
        def _():
            for p in range(PARTS):
                hop(h, p).wait_send()

    pltpu.make_async_copy(many, many, sums_send).wait()
    pltpu.make_async_copy(arrived, arrived, disp_send).wait()
    for e in range(n_exp):
        half(e).wait_send()
    pltpu.make_async_copy(returned, returned, back_send).wait()


def direct_kernel(
    n_seq,
    n_exp,
    n_rep,
    k_hbm,
    v_hbm,
    decay_hbm,
    q_hbm,
    routes_hbm,
    rw_hbm,
    res_hbm,
    gate_hbm,
    again_hbm,
    mgain_hbm,
    wg_hbm,
    wu_hbm,
    wd_hbm,
    out_ref,
    k_ref,
    v_ref,
    decay_ref,
    q_ref,
    routes_ref,
    rw_ref,
    res_ref,
    gate_ref,
    again_ref,
    mgain_ref,
    wg,
    wu,
    wd,
    state_in,
    state_out,
    own_state,
    block_state,
    lifted,
    att,
    u_buf,
    sums,
    first_sums,
    end_send,
    end_recv,
    q_send,
    q_recv,
    part_send,
    part_recv,
    tail_recv,
    extra_send,
    extra_recv,
    near,
    acc,
    res_pack,
    res_rows,
    pack,
    rows,
    gate_early,
    up_early,
    half_send,
    half_recv,
    fin,
    back,
    in_sem,
    w_sem,
    go_sem,
    chain_send,
    chain_recv,
    sums_send,
    sums_recv,
    first_ssem,
    first_rsem,
    q_ssem,
    q_rsem,
    end_ssem,
    end_rsem,
    part_ssem,
    part_rsem,
    extra_ssem,
    extra_rsem,
    res_ssem,
    res_rsem,
    disp_send,
    disp_recv,
    swap_send,
    swap_recv,
    half_ssem,
    half_rsem,
    back_send,
    back_recv,
):
    z = lax.axis_index("seq")
    x = lax.axis_index("exp")
    r = lax.axis_index("rep")
    other = 1 - r
    tokens, columns = q_ref.shape
    heads = decay_ref.shape[0]
    hd = columns // heads
    part_rows = hd // PARTS
    hidden_rows = wg.shape[0]
    width = columns * n_exp * n_rep
    whole_rows = wg_hbm.shape[1]
    plane = n_exp * n_seq
    peers = n_exp * n_rep
    me = x * n_rep + r
    last = n_seq - 1
    middle = last // 2
    picked = n_exp * SLOTS
    used = pl.ds(0, CAP)
    here = x * n_seq + z

    def home(b):
        return b if b < last else middle

    inputs = {
        name: pltpu.make_async_copy(src, dst, in_sem.at[i])
        for i, (name, src, dst) in enumerate(
            (
                ("decay", decay_hbm, decay_ref),
                ("routes", routes_hbm, routes_ref),
                ("q", q_hbm, q_ref),
                ("k", k_hbm, k_ref),
                ("v", v_hbm, v_ref),
                ("res", res_hbm, res_ref),
                ("gate", gate_hbm, gate_ref),
                ("again", again_hbm, again_ref),
                ("mgain", mgain_hbm, mgain_ref),
                ("rw", rw_hbm, rw_ref),
            )
        )
    }
    for load in inputs.values():
        load.start()

    barrier = pltpu.get_barrier_semaphore()

    def greet(where):
        pl.semaphore_signal(barrier, inc=1, device_id=where, device_id_type=MESH)

    for i in range(n_seq):

        @pl.when((i != z) & ((i > 0) | (z == 1)))
        def _():
            greet({"seq": i})

    for i in range(peers - 1):
        to = lax.rem(me + 1 + i, peers)
        greet({"exp": lax.div(to, n_rep), "rep": lax.rem(to, n_rep)})

    first = pl.multiple_of(r * hidden_rows, 16) if hidden_rows != whole_rows else 0
    loads = [
        pltpu.make_async_copy(src.at[0, pl.ds(first, hidden_rows), :], dst, w_sem.at[i])
        for i, (src, dst) in enumerate(((wg_hbm, wg), (wu_hbm, wu), (wd_hbm, wd)))
    ]
    for load in loads:
        load.start()

    def remote(src, dst, send_sem, recv_sem, where):
        return pltpu.make_async_remote_copy(
            src_ref=src,
            dst_ref=dst,
            send_sem=send_sem,
            recv_sem=recv_sem,
            device_id=where,
            device_id_type=MESH,
        )

    inputs["decay"].wait()
    ti = lax.broadcasted_iota(jnp.int32, (tokens, tokens), 0)
    tj = lax.broadcasted_iota(jnp.int32, (tokens, tokens), 1)
    causal = ti >= tj
    upper = jnp.where(tj >= ti, 1.0, 0.0).astype(F32)
    cum_t = jnp.dot(
        decay_ref[...], upper, precision=lax.Precision.HIGHEST, preferred_element_type=F32
    )
    cum = jnp.transpose(cum_t)
    ending = cum[tokens - 1 : tokens, :]
    fading = jnp.exp(ending)
    to_end = jnp.exp(ending - cum)
    lift = jnp.exp(cum)
    end_send[...] = jnp.zeros(end_send.shape, F32)
    end_send[:, 0:heads] = ending
    inputs["routes"].wait()
    lane = lax.broadcasted_iota(jnp.int32, (tokens, 128), 1)
    expert_of = lax.div(lane, SLOTS)
    slot_of = lax.rem(lane, SLOTS)
    named = jnp.transpose(routes_ref[...].astype(F32)).astype(jnp.int32)
    first_hit = named[:, 0:1] == expert_of
    second_hit = named[:, 1:2] == expert_of
    hit = jnp.where(first_hit | second_hit, 1.0, 0.0)
    strict = jnp.where(ti > tj, 1.0, 0.0).astype(BF16)
    before = jnp.dot(strict, hit.astype(BF16), preferred_element_type=F32)
    taken = (hit > 0.5) & (before.astype(jnp.int32) == slot_of) & (slot_of < CAP)
    onehot = jnp.where(taken, 1.0, 0.0)
    dispatch = jnp.transpose(onehot)[0:picked, :].astype(BF16)

    def pick(values):
        return jnp.dot(dispatch, values, preferred_element_type=F32)

    def put(ref, values):
        for e in range(n_exp):
            ref[e, :, 0:columns] = values[e * SLOTS : (e + 1) * SLOTS, :].astype(BF16)

    def take(ref):
        return ref[...].astype(F32)[:, :, 0:columns].reshape(picked, columns)

    inputs["q"].wait()
    for h in range(heads):
        cols = slice(h * hd, (h + 1) * hd)
        lifted[:, cols] = (q_ref[:, cols].astype(F32) * lift[:, h : h + 1]).astype(BF16)
    put(q_send, pick(lifted[...]))

    def keep_state():
        inputs["k"].wait()
        inputs["v"].wait()
        for h in range(heads):
            cols = slice(h * hd, (h + 1) * hd)
            faded = k_ref[:, cols].astype(F32) * to_end[:, h : h + 1]
            state = jnp.dot(
                jnp.transpose(faded).astype(BF16), v_ref[:, cols], preferred_element_type=F32
            )
            block_state[h] = state
            own_state[h] = state.astype(BF16)

    @pl.when(z < last - 1)
    def _():
        keep_state()

    pl.semaphore_wait(barrier, jnp.where(z == 0, 1, last) + peers - 1)

    def let_go():
        for i in range(1, n_exp):
            pl.semaphore_signal(
                go_sem,
                inc=1,
                device_id={"exp": lax.rem(x + i, n_exp)},
                device_id_type=MESH,
            )

    @pl.when(z > 0)
    def _():
        let_go()


    def ask(to):
        where = {"seq": to}
        return (
            remote(
                q_send.at[:, used], q_recv.at[z, :, used], q_ssem.at[to], q_rsem.at[z], where
            ),
            remote(end_send, end_recv.at[z], end_ssem.at[to], end_rsem.at[z], where),
        )

    for to in range(last):

        @pl.when(to < z)
        def _():
            for copy in ask(to):
                copy.start()

    @pl.when(z == last - 1)
    def _():
        keep_state()

    def hop(h, p, src):
        piece = pl.ds(p * part_rows, part_rows)
        return remote(
            src.at[h, piece],
            state_in.at[h, piece],
            chain_send.at[h, p],
            chain_recv.at[h, p],
            {"seq": z + 1},
        )

    def set_off(which):
        @pl.when((z == 0) & (z < last))
        def _():
            for h in which:
                for p in range(PARTS):
                    hop(h, p, own_state).start()

    lead = heads - heads // 4
    ahead = max(lead - max(last - 1, 0), 0)
    set_off(range(ahead))

    @pl.when(z == last)
    def _():
        inputs["k"].wait()
        inputs["v"].wait()

    for h in range(heads):
        cols = slice(h * hd, (h + 1) * hd)
        scores = nt_dot(q_ref[:, cols], k_ref[:, cols])
        gaps = cum[:, h : h + 1] - cum_t[h : h + 1, :]
        mixing = jnp.where(causal, scores * jnp.exp(jnp.where(causal, gaps, 0.0)), 0.0)
        att[:, cols] = jnp.dot(mixing.astype(BF16), v_ref[:, cols], preferred_element_type=F32)

    for name in ("res", "gate", "again", "mgain", "rw"):
        inputs[name].wait()
    near_att = pick(att[...].astype(BF16))
    near_res = pick(res_ref[...])
    near_v = jax.nn.sigmoid(pick(gate_ref[...])) * again_ref[...]
    near[0] = near_att
    near[1] = near_v
    near[2] = near_res

    spot = lax.broadcasted_iota(jnp.int32, (picked, 128), 1)

    def peer_of(i):
        to = lax.rem(me + 1 + i, peers)
        return {"exp": lax.div(to, n_rep), "rep": lax.rem(to, n_rep)}

    def products(attended, gated, residual):
        u = gated * attended
        parts = (attended * attended, residual * u, u * u, residual * residual)
        return u, [jnp.sum(part, axis=1, keepdims=True) for part in parts]

    def first_tell(i):
        return remote(
            first_sums.at[me], first_sums.at[me], first_ssem, first_rsem, peer_of(i)
        )

    @pl.when(z == 0)
    def _():
        _, wholes = products(near_att, near_v, near_res)
        table = jnp.zeros((picked, 128), F32)
        for n, whole in enumerate(wholes):
            table = jnp.where(spot == n, whole, table)
        first_sums[me] = table
        for i in range(peers - 1):
            first_tell(i).start()

    def to_home(i):
        return remote(
            extra_send.at[i, :, used],
            extra_recv.at[i, :, used],
            extra_ssem.at[i],
            extra_rsem.at[i],
            {"seq": middle},
        )

    @pl.when(z > 0)
    def _():
        put(res_pack, near_res * mgain_ref[...])
        res_rows[r, here] = res_pack[x]

    if middle != last:

        @pl.when(z == last)
        def _():
            for i, value in enumerate((near_att, near_v, near_res)):
                put(extra_send.at[i], value)
                to_home(i).start()

    def own_line(send, order=None):
        for i in order or [n for k in range(n_seq) for n in (last - k, k)][:n_seq]:

            @pl.when(i != z)
            def _():
                send(x, i)

    def other_lines(send, order=None):
        for j in range(1, n_exp):
            for i in order or [n for k in range(n_seq) for n in (last - k, k)][:n_seq]:
                send(lax.rem(x + j, n_exp), i)

    def send_res(e, to):
        remote(
            res_pack.at[e, used],
            res_rows.at[r, here, used],
            res_ssem,
            res_rsem,
            {"exp": e, "seq": to},
        ).start()

    def keep(b, i):
        rows[r, x * n_seq + b] = pack[i, x]

    def spread(b, i):
        spot_of = x * n_seq + b

        def send(e, to):
            remote(
                pack.at[i, e, used],
                rows.at[r, spot_of, used],
                disp_send,
                disp_recv,
                {"exp": e, "seq": to},
            ).start()

        return send

    def hand_out(b, i, attended, gated, residual):
        u, wholes = products(attended, gated, residual)
        table = jnp.zeros((picked, 128), F32)
        for n, whole in enumerate(wholes):
            coarse = whole.astype(BF16).astype(F32)
            table = jnp.where(spot == n, coarse, table)
            table = jnp.where(spot == n + len(wholes), whole - coarse, table)
        put(pack.at[i], u * mgain_ref[...])
        for e in range(n_exp):
            pack[i, e, :, columns:] = table[e * SLOTS : (e + 1) * SLOTS, :].astype(BF16)
        keep(b, i)
        return spread(b, i)

    def norms(total):
        s1 = lax.rsqrt(total[0] / width + EPSILON)
        moe = total[3] + s1 * (2.0 * total[1] + s1 * total[2])
        return s1, lax.rsqrt(jnp.maximum(moe, 0.0) / width + EPSILON)

    @pl.when(z > 0)
    def _():
        own_line(send_res)
        pl.semaphore_wait(go_sem, n_exp - 1)
        other_lines(send_res)

    def offer(b):
        target = tail_recv if b == last else part_recv
        return remote(
            part_send.at[b, :, used],
            target.at[z, :, used],
            part_ssem.at[b],
            part_rsem.at[1 if b == last else 0, z],
            {"seq": home(b)},
        )

    def relay(h):
        cols = slice(h * hd, (h + 1) * hd)
        for p in range(PARTS):
            piece = slice(p * part_rows, (p + 1) * part_rows)
            hop(h, p, state_out).wait_recv()

            @pl.when(z < last)
            def _():
                state_out[h, piece] = (
                    fading[:, h : h + 1] * state_in[h, piece].astype(F32)
                    + block_state[h, piece]
                ).astype(BF16)
                hop(h, p, state_out).start()

        att[:, cols] += jnp.dot(lifted[:, cols], state_in[h], preferred_element_type=F32)

    def relays(where, which):
        @pl.when(where)
        def _():
            for h in which:
                relay(h)

    chained = (z > 0) & (z < last)
    for b in range(1, n_seq):

        @pl.when(z < b)
        def _():
            ask_q = remote(q_send.at[:, used], q_recv.at[b, :, used], q_ssem.at[0], q_rsem.at[b], {"seq": 0})
            ask_e = remote(end_send, end_recv.at[b], end_ssem.at[0], end_rsem.at[b], {"seq": 0})
            ask_q.wait_recv()
            ask_e.wait_recv()
            between = jnp.zeros((1, 128), F32)
            for m in range(1, b):
                between += jnp.where(m > z, end_recv[m], 0.0)
            between = jnp.exp(between)
            asked = take(q_recv.at[b]).astype(BF16)
            given = [
                jnp.dot(
                    asked[:, h * hd : (h + 1) * hd], own_state[h], preferred_element_type=F32
                )
                * between[:, h : h + 1]
                for h in range(heads)
            ]
            given = jnp.concatenate(given, axis=1)
            put(part_send.at[b], given)

            @pl.when(z != home(b))
            def _():
                offer(b).start()

            if b == last:

                @pl.when(z == home(b))
                def _():
                    put(tail_recv.at[z], given)

        if b < last:
            set_off(range(ahead + b - 1, min(ahead + b, lead)))

    @pl.when(z == 0)
    def _():
        let_go()

    @pl.when(z == 0)
    def _():
        everyone = first_sums.at[pl.ds(0, peers - 1)]
        pltpu.make_async_copy(everyone, everyone, first_rsem).wait()
        total = jnp.sum(first_sums[...], axis=0)
        s1, s2 = norms([total[:, n : n + 1] for n in range(4)])
        normed = (near[2] + s1 * (near[0] * near[1])) * s2 * mgain_ref[...]
        put(pack.at[0], normed)
        keep(0, 0)
        own_line(spread(0, 0))

        pl.semaphore_wait(go_sem, n_exp - 1)
        other_lines(spread(0, 0))

    set_off(range(lead, heads))

    def wait_part(which, source):
        buffer = tail_recv if which else part_recv
        remote(
            part_send.at[0, :, used],
            buffer.at[source, :, used],
            part_ssem.at[0],
            part_rsem.at[which, source],
            {"seq": 0},
        ).wait_recv()

    @pl.when((z > 0) & (z < last))
    def _():
        acc[...] = near[0]
        for source in range(last):

            @pl.when(source < z)
            def _():
                wait_part(0, source)
                acc[...] += take(part_recv.at[source])

        send = hand_out(z, 0, acc[...], near[1], near[2])
        own_line(send)
        other_lines(send)

    relays(chained & (z == 1), range(ahead))

    @pl.when(z == middle)
    def _():
        for i in range(3):
            to_home(i).wait_recv()
        whole = take(extra_recv.at[0])
        whole += take(tail_recv.at[middle])
        for source in range(last):
            if source != middle:
                wait_part(1, source)
                whole += take(tail_recv.at[source])
        send = hand_out(last, 1, whole, take(extra_recv.at[1]), take(extra_recv.at[2]))
        order = sorted(range(n_seq), key=lambda i: -abs(i - middle))
        own_line(send, order)
        other_lines(send, order)

    relays(chained & (z == 1), range(ahead, lead))

    slots = n_seq * SLOTS

    def project(table, s):
        gate_part = up_part = 0.0
        for e in range(n_exp):
            chunk = table[s, pl.ds(e * n_seq, n_seq)].astype(F32)[:, :, 0:columns]
            chunk = chunk.reshape(slots, columns).astype(BF16)
            at = pl.ds(pl.multiple_of((e * n_rep + s) * columns, 128), columns)
            gate_part += nt_dot(wg[:, at], chunk)
            up_part += nt_dot(wu[:, at], chunk)
        return gate_part, up_part

    def swap(table, i):
        return remote(
            table.at[r], table.at[r], swap_send.at[i], swap_recv.at[i], {"rep": other}
        )

    res_sent = res_rows.at[r, pl.ds(0, plane - 1), used]
    for n in range(2):

        @pl.when(jnp.where(z > 0, 1, 0) == n)
        def _():
            arrived = res_rows.at[r, pl.ds(0, plane - n_exp - n), used]
            pltpu.make_async_copy(arrived, arrived, res_rsem).wait()

    swap(res_rows, 0).start()
    for load in loads:
        load.wait()
    gate_val, up_val = project(res_rows, r)
    swap(res_rows, 0).wait()
    gate_part, up_part = project(res_rows, other)
    gate_early[...] = gate_val + gate_part
    up_early[...] = up_val + up_part

    relays(chained & (z == 1), range(lead, heads))
    relays(chained & (z > 1), range(ahead))

    mine = jnp.where(z < last, 1, 0) + jnp.where(z == middle, 1, 0)
    for n in range(3):

        @pl.when(mine == n)
        def _():
            arrived = rows.at[r, pl.ds(0, plane - n), used]
            pltpu.make_async_copy(arrived, arrived, disp_recv).wait()

    swap(rows, 1).start()
    gate_val, up_val = project(rows, r)
    relays(chained & (z > 1), range(ahead, lead))
    swap(rows, 1).wait()
    gate_part, up_part = project(rows, other)
    table = 0.0
    for s in range(n_rep):
        for e in range(n_exp):
            table += rows[s, pl.ds(e * n_seq, n_seq)].astype(F32)[:, :, columns:]
    table = jnp.transpose(table.reshape(slots, 128))
    total = table[0:4, :] + table[4:8, :]
    s1, s2 = norms([total[n : n + 1, :] for n in range(4)])
    whole = lax.broadcasted_iota(jnp.int32, (hidden_rows, slots), 1) < SLOTS
    gate_b, up_b = gate_val + gate_part, up_val + up_part
    gate_val = jnp.where(whole, gate_b, s2 * (gate_early[...] + s1 * gate_b))
    up_val = jnp.where(whole, up_b, s2 * (up_early[...] + s1 * up_b))
    inner = gate_val / (1.0 + jnp.exp(-gate_val)) * up_val
    if hidden_rows == whole_rows:
        unit = lax.broadcasted_iota(jnp.int32, inner.shape, 0)
        inner = jnp.where(lax.div(unit, whole_rows // n_rep) == r, inner, 0.0)
    inner = jnp.transpose(inner).astype(BF16)
    relays(chained & (z > 1), range(lead, heads))

    def product(e, s):
        at = pl.multiple_of((e * n_rep + s) * columns, 128)
        return jnp.dot(inner, wd[:, pl.ds(at, columns)], preferred_element_type=F32)

    def half(e):
        return remote(
            half_send.at[e], half_recv.at[e], half_ssem.at[e], half_rsem.at[e], {"rep": other}
        )

    for e in range(n_exp):
        half_send[e] = product(e, other).astype(BF16)
        half(e).start()

    for e in range(n_exp):
        own = product(e, r)
        half(e).wait_recv()
        whole = (own + half_recv[e].astype(F32)).reshape(n_seq, SLOTS, columns)
        fin[pl.ds(e * n_seq, n_seq)] = whole.astype(BF16)

    back[here] = fin[here]

    def hand_back(e, to):
        remote(
            fin.at[e * n_seq + to, used],
            back.at[here, used],
            back_send,
            back_recv,
            {"exp": e, "seq": to},
        ).start()

    other_lines(hand_back)
    own_line(hand_back)

    relays((z > 0) & (z == last), range(heads))
    attended = att[...]
    square = jnp.sum(attended * attended, axis=1, keepdims=True)
    table = jnp.where(lane == 0, square, 0.0)
    sums[me] = jnp.transpose(table)[0:8, :]

    def tell(i):
        return remote(sums.at[me], sums.at[me], sums_send, sums_recv, peer_of(i))

    for i in range(peers - 1):
        tell(i).start()
    u_buf[...] = jax.nn.sigmoid(gate_ref[...].astype(F32)) * attended * again_ref[...]
    shares = jnp.transpose(rw_ref[...])
    combine = jnp.where(first_hit, shares[:, 0:1], shares[:, 1:2]) * onehot
    coarse = combine.astype(BF16)
    fine = (combine - coarse.astype(F32)).astype(BF16)

    for to in range(last):

        @pl.when(to < z)
        def _():
            for copy in ask(to):
                copy.wait_send()

    if middle != last:

        @pl.when(z == last)
        def _():
            for i in range(3):
                to_home(i).wait_send()

    for b in range(1, n_seq):

        @pl.when((z < b) & (z != home(b)))
        def _():
            offer(b).wait_send()

    @pl.when(z < last)
    def _():
        for h in range(heads):
            for p in range(PARTS):
                hop(h, p, state_out).wait_send()

    @pl.when(z > 0)
    def _():
        pltpu.make_async_copy(res_sent, res_sent, res_ssem).wait()

    @pl.when(z == 0)
    def _():
        everyone = first_sums.at[pl.ds(0, peers - 1)]
        pltpu.make_async_copy(everyone, everyone, first_ssem).wait()

    for n in range(1, 3):

        @pl.when(mine == n)
        def _():
            for _ in range(n):
                sent = rows.at[r, pl.ds(0, plane - 1), used]
                pltpu.make_async_copy(sent, sent, disp_send).wait()

    for e in range(n_exp):
        half(e).wait_send()

    many = sums.at[pl.ds(0, peers - 1)]
    pltpu.make_async_copy(many, many, sums_recv).wait()
    total = jnp.sum(sums[...], axis=0)
    scale = lax.rsqrt(total / width + EPSILON)
    scale = jnp.transpose(scale)[:, 0:1]
    u_buf[...] = res_ref[...].astype(F32) + scale * u_buf[...]
    pltpu.make_async_copy(many, many, sums_send).wait()

    returned = back.at[pl.ds(0, plane - 1), used]
    pltpu.make_async_copy(returned, returned, back_recv).wait()
    result = u_buf[...]
    for e in range(n_exp):
        rows_e = jnp.sum(back[pl.ds(e * n_seq, n_seq)].astype(F32), axis=0)
        slot = lax.broadcasted_iota(jnp.int32, rows_e.shape, 0)
        rows_e = jnp.where(slot < CAP, rows_e, 0.0).astype(BF16)
        lanes = slice(e * SLOTS, (e + 1) * SLOTS)
        result += jnp.dot(coarse[:, lanes], rows_e, preferred_element_type=F32)
        result += jnp.dot(fine[:, lanes], rows_e, preferred_element_type=F32)
    out_ref[...] = result.astype(BF16)
    pltpu.make_async_copy(returned, returned, back_send).wait()


def solution(mesh):
    n_seq, n_exp, n_rep = (mesh.shape[a] for a in ("seq", "exp", "rep"))

    def shards(
        queries,
        key_rows,
        value_rows,
        decay_log,
        residual,
        out_gate,
        attn_gain,
        moe_gain,
        routes,
        route_weights,
        w_gate,
        w_up,
        w_down,
    ):
        tokens, columns = queries.shape
        heads = decay_log.shape[1]
        hd = columns // heads
        _, whole_rows, width = w_gate.shape
        even = whole_rows % (16 * n_rep) == 0
        hidden_rows = whole_rows // n_rep if even else whole_rows
        plane = n_exp * n_seq
        slots = n_seq * SLOTS
        vmem = pl.BlockSpec(memory_space=pltpu.VMEM)
        hbm = pl.BlockSpec(memory_space=pltpu.HBM)
        dma = pltpu.SemaphoreType.DMA
        if 2 < n_seq <= SHORT:
            wide = columns + 128
            return pl.pallas_call(
                lambda *refs: direct_kernel(n_seq, n_exp, n_rep, *refs),
                name="layer",
                out_shape=pltpu.VMEM((tokens, columns), BF16),
                in_specs=[hbm] * 13,
                out_specs=vmem,
                scratch_shapes=[
                    pltpu.VMEM((tokens, columns), BF16),
                    pltpu.VMEM((tokens, columns), BF16),
                    pltpu.VMEM((heads, tokens), F32),
                    pltpu.VMEM((tokens, columns), BF16),
                    pltpu.VMEM((2, tokens), jnp.int32),
                    pltpu.VMEM((2, tokens), F32),
                    pltpu.VMEM((tokens, columns), BF16),
                    pltpu.VMEM((tokens, columns), BF16),
                    pltpu.VMEM((1, columns), F32),
                    pltpu.VMEM((1, columns), F32),
                    pltpu.VMEM((hidden_rows, width), BF16),
                    pltpu.VMEM((hidden_rows, width), BF16),
                    pltpu.VMEM((hidden_rows, width), BF16),
                    pltpu.VMEM((heads, hd, hd), BF16),
                    pltpu.VMEM((heads, hd, hd), BF16),
                    pltpu.VMEM((heads, hd, hd), BF16),
                    pltpu.VMEM((heads, hd, hd), F32),
                    pltpu.VMEM((tokens, columns), BF16),
                    pltpu.VMEM((tokens, columns), F32),
                    pltpu.VMEM((tokens, columns), F32),
                    pltpu.VMEM((n_exp * n_rep, 8, tokens), F32),
                    pltpu.VMEM((n_exp * n_rep, n_exp * SLOTS, 128), F32),
                    pltpu.VMEM((1, 128), F32),
                    pltpu.VMEM((n_seq, 1, 128), F32),
                    pltpu.VMEM((n_exp, SLOTS, columns), BF16),
                    pltpu.VMEM((n_seq, n_exp, SLOTS, columns), BF16),
                    pltpu.VMEM((n_seq, n_exp, SLOTS, columns), BF16),
                    pltpu.VMEM((n_seq, n_exp, SLOTS, columns), BF16),
                    pltpu.VMEM((n_seq, n_exp, SLOTS, columns), BF16),
                    pltpu.VMEM((3, n_exp, SLOTS, columns), BF16),
                    pltpu.VMEM((3, n_exp, SLOTS, columns), BF16),
                    pltpu.VMEM((3, n_exp * SLOTS, columns), F32),
                    pltpu.VMEM((n_exp * SLOTS, columns), F32),
                    pltpu.VMEM((n_exp, SLOTS, columns), BF16),
                    pltpu.VMEM((n_rep, plane, SLOTS, columns), BF16),
                    pltpu.VMEM((2, n_exp, SLOTS, wide), BF16),
                    pltpu.VMEM((n_rep, plane, SLOTS, wide), BF16),
                    pltpu.VMEM((hidden_rows, slots), F32),
                    pltpu.VMEM((hidden_rows, slots), F32),
                    pltpu.VMEM((n_exp, slots, columns), BF16),
                    pltpu.VMEM((n_exp, slots, columns), BF16),
                    pltpu.VMEM((plane, SLOTS, columns), BF16),
                    pltpu.VMEM((plane, SLOTS, columns), BF16),
                    dma((10,)),
                    dma((3,)),
                    pltpu.SemaphoreType.REGULAR,
                    dma((heads, PARTS)),
                    dma((heads, PARTS)),
                    dma,
                    dma,
                    dma,
                    dma,
                    dma((n_seq,)),
                    dma((n_seq,)),
                    dma((n_seq,)),
                    dma((n_seq,)),
                    dma((n_seq,)),
                    dma((2, n_seq)),
                    dma((3,)),
                    dma((3,)),
                    dma,
                    dma,
                    dma,
                    dma,
                    dma((2,)),
                    dma((2,)),
                    dma((n_exp,)),
                    dma((n_exp,)),
                    dma,
                    dma,
                ],
                compiler_params=pltpu.CompilerParams(
                    collective_id=0, has_side_effects=True, vmem_limit_bytes=63000000
                ),
            )(
                key_rows,
                value_rows,
                decay_log.T,
                queries,
                routes.T,
                route_weights.T,
                residual,
                out_gate,
                attn_gain.reshape(1, columns),
                moe_gain.reshape(1, columns),
                w_gate,
                w_up,
                w_down,
            )
        return pl.pallas_call(
            lambda *refs: chain_kernel(n_seq, n_exp, n_rep, *refs),
            name="layer",
            out_shape=pltpu.VMEM((tokens, columns), BF16),
            in_specs=[hbm] * 13,
            out_specs=vmem,
            scratch_shapes=[
                pltpu.VMEM((tokens, columns), BF16),
                pltpu.VMEM((tokens, columns), BF16),
                pltpu.VMEM((heads, tokens), F32),
                pltpu.VMEM((tokens, columns), BF16),
                pltpu.VMEM((2, tokens), jnp.int32),
                pltpu.VMEM((2, tokens), F32),
                pltpu.VMEM((tokens, columns), BF16),
                pltpu.VMEM((tokens, columns), BF16),
                pltpu.VMEM((1, columns), F32),
                pltpu.VMEM((1, columns), F32),
                pltpu.VMEM((hidden_rows, width), BF16),
                pltpu.VMEM((hidden_rows, width), BF16),
                pltpu.VMEM((hidden_rows, width), BF16),
                pltpu.VMEM((heads, hd, hd), BF16),
                pltpu.VMEM((heads, hd, hd), BF16),
                pltpu.VMEM((heads, hd, hd), F32),
                pltpu.VMEM((tokens, columns), F32),
                pltpu.VMEM((tokens, columns), F32),
                pltpu.VMEM((n_exp * n_rep, 8, tokens), F32),
                pltpu.VMEM((n_exp, SLOTS, columns), BF16),
                pltpu.VMEM((n_rep, plane, SLOTS, columns), BF16),
                pltpu.VMEM((n_exp, slots, columns), BF16),
                pltpu.VMEM((n_exp, slots, columns), BF16),
                pltpu.VMEM((plane, SLOTS, columns), BF16),
                pltpu.VMEM((plane, SLOTS, columns), BF16),
                dma((10,)),
                dma((3,)),
                pltpu.SemaphoreType.REGULAR,
                dma((heads, PARTS)),
                dma((heads, PARTS)),
                dma,
                dma,
                dma,
                dma,
                dma,
                dma,
                dma((n_exp,)),
                dma((n_exp,)),
                dma,
                dma,
            ],
            compiler_params=pltpu.CompilerParams(collective_id=0, has_side_effects=True, vmem_limit_bytes=63000000),
        )(
            key_rows,
            value_rows,
            decay_log.T,
            queries,
            routes.T,
            route_weights.T,
            residual,
            out_gate,
            attn_gain.reshape(1, columns),
            moe_gain.reshape(1, columns),
            w_gate,
            w_up,
            w_down,
        )

    block = P(("groups", "seq"), ("exp", "rep"))
    gain = P(("exp", "rep"))
    route = P(("groups", "seq"), None)
    weight = P("exp", "seq", None)
    return jax.shard_map(
        shards,
        mesh=mesh,
        in_specs=(block,) * 6 + (gain, gain, route, route) + (weight,) * 3,
        out_specs=block,
        check_vma=False,
    )
```

```python
import jax
import jax.numpy as jnp
from jax import lax
from jax.experimental import pallas as pl
from jax.experimental.pallas import tpu as pltpu
from jax.sharding import PartitionSpec as P

CAP = 6
SLOTS = 8
PARTS = 2
SHORT = 4
EPSILON = 1e-06
MESH = pl.DeviceIdType.MESH
F32 = jnp.float32
BF16 = jnp.bfloat16


def sweep(count, body):
    if count <= 16:
        for i in range(count):
            body(i)
    else:
        lax.fori_loop(0, count, lambda i, c: (body(i), c)[1], 0)


def nt_dot(a, b):
    return lax.dot_general(a, b, (((1,), (1,)), ((), ())), preferred_element_type=F32)


def chain_kernel(
    n_seq,
    n_exp,
    n_rep,
    k_hbm,
    v_hbm,
    decay_hbm,
    q_hbm,
    routes_hbm,
    rw_hbm,
    res_hbm,
    gate_hbm,
    again_hbm,
    mgain_hbm,
    wg_hbm,
    wu_hbm,
    wd_hbm,
    out_ref,
    k_ref,
    v_ref,
    decay_ref,
    q_ref,
    routes_ref,
    rw_ref,
    res_ref,
    gate_ref,
    again_ref,
    mgain_ref,
    wg,
    wu,
    wd,
    state_in,
    state_out,
    block_state,
    att,
    u_buf,
    sums,
    pack,
    rows,
    half_send,
    half_recv,
    fin,
    back,
    in_sem,
    w_sem,
    go_sem,
    chain_send,
    chain_recv,
    sums_send,
    sums_recv,
    disp_send,
    disp_recv,
    swap_send,
    swap_recv,
    half_ssem,
    half_rsem,
    back_send,
    back_recv,
):
    z = lax.axis_index("seq")
    x = lax.axis_index("exp")
    r = lax.axis_index("rep")
    other = 1 - r
    tokens, columns = q_ref.shape
    heads = decay_ref.shape[0]
    hd = columns // heads
    part_rows = hd // PARTS
    hidden_rows = wg.shape[0]
    width = columns * n_exp * n_rep
    whole_rows = wg_hbm.shape[1]

    inputs = [
        pltpu.make_async_copy(src, dst, in_sem.at[i])
        for i, (src, dst) in enumerate(
            (
                (k_hbm, k_ref),
                (v_hbm, v_ref),
                (decay_hbm, decay_ref),
                (q_hbm, q_ref),
                (routes_hbm, routes_ref),
                (rw_hbm, rw_ref),
                (res_hbm, res_ref),
                (gate_hbm, gate_ref),
                (again_hbm, again_ref),
                (mgain_hbm, mgain_ref),
            )
        )
    ]
    for load in inputs:
        load.start()
    first = pl.multiple_of(r * hidden_rows, 16) if hidden_rows != whole_rows else 0
    loads = [
        pltpu.make_async_copy(src.at[0, pl.ds(first, hidden_rows), :], dst, w_sem.at[i])
        for i, (src, dst) in enumerate(((wg_hbm, wg), (wu_hbm, wu), (wd_hbm, wd)))
    ]

    barrier = pltpu.get_barrier_semaphore()
    plane = n_exp * n_seq
    peers = n_exp * n_rep
    me = x * n_rep + r
    last = n_seq - 1

    def greet(where):
        pl.semaphore_signal(barrier, inc=1, device_id=where, device_id_type=MESH)

    @pl.when(z < last)
    def _():
        greet({"seq": z + 1})

    @pl.when(z > 0)
    def _():
        greet({"seq": z - 1})

    def greet_peer(i):
        to = lax.rem(me + 1 + i, peers)
        greet({"exp": lax.div(to, n_rep), "rep": lax.rem(to, n_rep)})

    sweep(peers - 1, greet_peer)
    for load in loads:
        load.start()
    for load in inputs[:3]:
        load.wait()

    ti = lax.broadcasted_iota(jnp.int32, (tokens, tokens), 0)
    tj = lax.broadcasted_iota(jnp.int32, (tokens, tokens), 1)
    causal = ti >= tj
    upper = jnp.where(tj >= ti, 1.0, 0.0).astype(F32)
    cum_t = jnp.dot(
        decay_ref[...], upper, precision=lax.Precision.HIGHEST, preferred_element_type=F32
    )
    cum = jnp.transpose(cum_t)
    ending = cum[tokens - 1 : tokens, :]
    fading = jnp.exp(ending)
    to_end = jnp.exp(ending - cum)
    lift = jnp.exp(cum)
    for h in range(heads):
        cols = slice(h * hd, (h + 1) * hd)
        faded = k_ref[:, cols].astype(F32) * to_end[:, h : h + 1]
        block_state[h] = jnp.dot(
            jnp.transpose(faded).astype(BF16), v_ref[:, cols], preferred_element_type=F32
        )

    ends = (z > 0).astype(jnp.int32) + (z < last).astype(jnp.int32)
    pl.semaphore_wait(barrier, peers - 1 + ends)

    def hop(h, p):
        piece = pl.ds(p * part_rows, part_rows)
        return pltpu.make_async_remote_copy(
            src_ref=state_out.at[h, piece],
            dst_ref=state_in.at[h, piece],
            send_sem=chain_send.at[h, p],
            recv_sem=chain_recv.at[h, p],
            device_id={"seq": z + 1},
            device_id_type=MESH,
        )

    @pl.when(z == 0)
    def _():
        for h in range(heads):
            state_out[h] = block_state[h].astype(BF16)
            for p in range(PARTS):
                hop(h, p).start()

    inputs[3].wait()

    for h in range(heads):
        cols = slice(h * hd, (h + 1) * hd)
        scores = nt_dot(q_ref[:, cols], k_ref[:, cols])
        gaps = cum[:, h : h + 1] - cum_t[h : h + 1, :]
        mixing = jnp.where(causal, scores * jnp.exp(jnp.where(causal, gaps, 0.0)), 0.0)
        att[:, cols] = jnp.dot(mixing.astype(BF16), v_ref[:, cols], preferred_element_type=F32)

    for load in inputs[4:]:
        load.wait()
    lane = lax.broadcasted_iota(jnp.int32, (tokens, 128), 1)
    expert_of = lax.div(lane, SLOTS)
    slot_of = lax.rem(lane, SLOTS)
    named = jnp.transpose(routes_ref[...].astype(F32)).astype(jnp.int32)
    shares = jnp.transpose(rw_ref[...])
    first_hit = named[:, 0:1] == expert_of
    second_hit = named[:, 1:2] == expert_of
    hit = jnp.where(first_hit | second_hit, 1.0, 0.0)
    strict = jnp.where(ti > tj, 1.0, 0.0).astype(BF16)
    before = jnp.dot(strict, hit.astype(BF16), preferred_element_type=F32)
    taken = (hit > 0.5) & (before.astype(jnp.int32) == slot_of) & (slot_of < CAP)
    onehot = jnp.where(taken, 1.0, 0.0)
    combine = jnp.where(first_hit, shares[:, 0:1], shares[:, 1:2]) * onehot
    dispatch = jnp.transpose(onehot)[0 : n_exp * SLOTS, :].astype(BF16)

    def let_go(i):
        pl.semaphore_signal(go_sem, inc=1, device_id={"seq": i}, device_id_type=MESH)

    for h in range(heads):
        cols = slice(h * hd, (h + 1) * hd)

        @pl.when(z > 0)
        def _():
            for p in range(PARTS):
                piece = slice(p * part_rows, (p + 1) * part_rows)
                hop(h, p).wait_recv()

                @pl.when(z < last)
                def _():
                    state_out[h, piece] = (
                        fading[:, h : h + 1] * state_in[h, piece].astype(F32)
                        + block_state[h, piece]
                    ).astype(BF16)
                    hop(h, p).start()

            lifted = (q_ref[:, cols].astype(F32) * lift[:, h : h + 1]).astype(BF16)
            att[:, cols] += jnp.dot(lifted, state_in[h], preferred_element_type=F32)

        if h == max(heads - 3, 0):

            @pl.when(z == last)
            def _():
                sweep(last, let_go)

    res = res_ref[...].astype(F32)
    attended = att[...]
    u = jax.nn.sigmoid(gate_ref[...].astype(F32)) * attended * again_ref[...]
    u_buf[...] = u
    parts = (attended * attended, res * u, u * u, res * res)
    table = jnp.zeros((tokens, 128), F32)
    for i, part in enumerate(parts):
        table = jnp.where(lane == i, jnp.sum(part, axis=1, keepdims=True), table)
    sums[me] = jnp.transpose(table)[0:8, :]

    def tell(i):
        to = lax.rem(me + 1 + i, peers)
        pltpu.make_async_remote_copy(
            src_ref=sums.at[me],
            dst_ref=sums.at[me],
            send_sem=sums_send,
            recv_sem=sums_recv,
            device_id={"exp": lax.div(to, n_rep), "rep": lax.rem(to, n_rep)},
            device_id_type=MESH,
        ).start()

    sweep(peers - 1, tell)
    many = sums.at[pl.ds(0, peers - 1)]
    pltpu.make_async_copy(many, many, sums_recv).wait()
    total = jnp.sum(sums[...], axis=0)
    s1 = lax.rsqrt(total[0:1, :] / width + EPSILON)
    moe = total[3:4, :] + s1 * (2.0 * total[1:2, :] + s1 * total[2:3, :])
    s2 = lax.rsqrt(jnp.maximum(moe, 0.0) / width + EPSILON)
    row8 = lax.broadcasted_iota(jnp.int32, (8, tokens), 0)
    scales = jnp.transpose(jnp.where(row8 == 0, s1, s2))
    hidden = res_ref[...].astype(F32) + scales[:, 0:1] * u_buf[...]
    u_buf[...] = hidden
    normed = (hidden * scales[:, 1:2] * mgain_ref[...]).astype(BF16)

    packed = jnp.dot(dispatch, normed, preferred_element_type=F32)
    for e in range(n_exp):
        pack[e] = packed[e * SLOTS : (e + 1) * SLOTS, :].astype(BF16)
    here = x * n_seq + z
    rows[r, here] = pack[x]

    def deal(e, to, source, target, send_sem, recv_sem):
        pltpu.make_async_remote_copy(
            src_ref=source,
            dst_ref=target,
            send_sem=send_sem,
            recv_sem=recv_sem,
            device_id={"exp": e, "seq": to},
            device_id_type=MESH,
        ).start()

    def deal_rows(e, to):
        used = pl.ds(0, CAP)
        deal(e, to, pack.at[e, used], rows.at[r, here, used], disp_send, disp_recv)

    def earlier(send):
        def one(i):
            @pl.when(i < z)
            def _():
                for e in range(n_exp):
                    send(e, i)

        sweep(n_seq, one)

    def level(send):
        for j in range(1, n_exp):
            send(lax.rem(x + j, n_exp), z)

    def later(send):
        def one(i):
            @pl.when(last - i > z)
            def _():
                for e in range(n_exp):
                    send(e, last - i)

        sweep(n_seq, one)

    earlier(deal_rows)
    level(deal_rows)

    @pl.when(z < last)
    def _():
        pl.semaphore_wait(go_sem, 1)

    later(deal_rows)
    arrived = rows.at[r, pl.ds(0, plane - 1), pl.ds(0, CAP)]
    pltpu.make_async_copy(arrived, arrived, disp_recv).wait()
    swap = pltpu.make_async_remote_copy(
        src_ref=rows.at[r],
        dst_ref=rows.at[r],
        send_sem=swap_send,
        recv_sem=swap_recv,
        device_id={"rep": other},
        device_id_type=MESH,
    )
    swap.start()
    for load in loads:
        load.wait()
    slots = n_seq * SLOTS

    def project(s):
        gate_part = up_part = 0.0
        for e in range(n_exp):
            chunk = rows[s, pl.ds(e * n_seq, n_seq)].astype(F32).reshape(slots, columns)
            chunk = chunk.astype(BF16)
            at = pl.ds(pl.multiple_of((e * n_rep + s) * columns, 128), columns)
            gate_part += nt_dot(wg[:, at], chunk)
            up_part += nt_dot(wu[:, at], chunk)
        return gate_part, up_part

    gate_val, up_val = project(r)
    swap.wait()
    gate_part, up_part = project(other)
    gate_val += gate_part
    up_val += up_part
    inner = gate_val / (1.0 + jnp.exp(-gate_val)) * up_val
    if hidden_rows == whole_rows:
        unit = lax.broadcasted_iota(jnp.int32, inner.shape, 0)
        inner = jnp.where(lax.div(unit, whole_rows // n_rep) == r, inner, 0.0)
    inner = jnp.transpose(inner).astype(BF16)

    def product(e, s):
        at = pl.multiple_of((e * n_rep + s) * columns, 128)
        return jnp.dot(inner, wd[:, pl.ds(at, columns)], preferred_element_type=F32)

    def half(e):
        return pltpu.make_async_remote_copy(
            src_ref=half_send.at[e],
            dst_ref=half_recv.at[e],
            send_sem=half_ssem.at[e],
            recv_sem=half_rsem.at[e],
            device_id={"rep": other},
            device_id_type=MESH,
        )

    for e in range(n_exp):
        half_send[e] = product(e, other).astype(BF16)
        half(e).start()

    here_back = x * n_seq + z
    for e in range(n_exp):
        own = product(e, r)
        half(e).wait_recv()
        whole = (own + half_recv[e].astype(F32)).reshape(n_seq, SLOTS, columns)
        fin[pl.ds(e * n_seq, n_seq)] = whole.astype(BF16)

    back[here_back] = fin[here_back]

    def hand_back(e, to):
        used = pl.ds(0, CAP)
        source = fin.at[e * n_seq + to, used]
        deal(e, to, source, back.at[here_back, used], back_send, back_recv)

    earlier(hand_back)
    later(hand_back)
    level(hand_back)
    returned = back.at[pl.ds(0, plane - 1), pl.ds(0, CAP)]
    pltpu.make_async_copy(returned, returned, back_recv).wait()
    coarse = combine.astype(BF16)
    fine = (combine - coarse.astype(F32)).astype(BF16)
    result = u_buf[...]
    for e in range(n_exp):
        rows_e = jnp.sum(back[pl.ds(e * n_seq, n_seq)].astype(F32), axis=0)
        slot = lax.broadcasted_iota(jnp.int32, rows_e.shape, 0)
        rows_e = jnp.where(slot < CAP, rows_e, 0.0).astype(BF16)
        lanes = slice(e * SLOTS, (e + 1) * SLOTS)
        result += jnp.dot(coarse[:, lanes], rows_e, preferred_element_type=F32)
        result += jnp.dot(fine[:, lanes], rows_e, preferred_element_type=F32)
    out_ref[...] = result.astype(BF16)

    for h in range(heads):

        @pl.when(z < last)
        def _():
            for p in range(PARTS):
                hop(h, p).wait_send()

    pltpu.make_async_copy(many, many, sums_send).wait()
    pltpu.make_async_copy(arrived, arrived, disp_send).wait()
    for e in range(n_exp):
        half(e).wait_send()
    pltpu.make_async_copy(returned, returned, back_send).wait()


def direct_kernel(
    n_seq,
    n_exp,
    n_rep,
    k_hbm,
    v_hbm,
    decay_hbm,
    q_hbm,
    routes_hbm,
    rw_hbm,
    res_hbm,
    gate_hbm,
    again_hbm,
    mgain_hbm,
    wg_hbm,
    wu_hbm,
    wd_hbm,
    out_ref,
    k_ref,
    v_ref,
    decay_ref,
    q_ref,
    routes_ref,
    rw_ref,
    res_ref,
    gate_ref,
    again_ref,
    mgain_ref,
    wg,
    wu,
    wd,
    state_in,
    state_out,
    own_state,
    block_state,
    lifted,
    att,
    u_buf,
    sums,
    first_sums,
    end_send,
    end_recv,
    q_send,
    q_recv,
    part_send,
    part_recv,
    tail_recv,
    extra_send,
    extra_recv,
    near,
    acc,
    fade,
    res_pack,
    res_rows,
    pack,
    rows,
    gate_early,
    up_early,
    half_send,
    half_recv,
    fin,
    back,
    in_sem,
    w_sem,
    go_sem,
    chain_send,
    chain_recv,
    sums_send,
    sums_recv,
    first_ssem,
    first_rsem,
    q_ssem,
    q_rsem,
    end_ssem,
    end_rsem,
    part_ssem,
    part_rsem,
    extra_ssem,
    extra_rsem,
    res_ssem,
    res_rsem,
    disp_send,
    disp_recv,
    swap_send,
    swap_recv,
    half_ssem,
    half_rsem,
    back_send,
    back_recv,
):
    z = lax.axis_index("seq")
    x = lax.axis_index("exp")
    r = lax.axis_index("rep")
    other = 1 - r
    tokens, columns = q_ref.shape
    heads = decay_ref.shape[0]
    hd = columns // heads
    part_rows = hd // PARTS
    hidden_rows = wg.shape[0]
    width = columns * n_exp * n_rep
    whole_rows = wg_hbm.shape[1]
    plane = n_exp * n_seq
    peers = n_exp * n_rep
    me = x * n_rep + r
    last = n_seq - 1
    middle = last // 2
    picked = n_exp * SLOTS
    used = pl.ds(0, CAP)
    here = x * n_seq + z

    def home(b):
        return b if b < last else middle

    inputs = {
        name: pltpu.make_async_copy(src, dst, in_sem.at[i])
        for i, (name, src, dst) in enumerate(
            (
                ("decay", decay_hbm, decay_ref),
                ("routes", routes_hbm, routes_ref),
                ("q", q_hbm, q_ref),
                ("k", k_hbm, k_ref),
                ("v", v_hbm, v_ref),
                ("res", res_hbm, res_ref),
                ("gate", gate_hbm, gate_ref),
                ("again", again_hbm, again_ref),
                ("mgain", mgain_hbm, mgain_ref),
                ("rw", rw_hbm, rw_ref),
            )
        )
    }
    for load in inputs.values():
        load.start()

    barrier = pltpu.get_barrier_semaphore()

    def greet(where):
        pl.semaphore_signal(barrier, inc=1, device_id=where, device_id_type=MESH)

    for i in range(n_seq):

        @pl.when((i != z) & ((i > 0) | (z == 1)))
        def _():
            greet({"seq": i})

    for i in range(peers - 1):
        to = lax.rem(me + 1 + i, peers)
        greet({"exp": lax.div(to, n_rep), "rep": lax.rem(to, n_rep)})

    first = pl.multiple_of(r * hidden_rows, 16) if hidden_rows != whole_rows else 0
    loads = [
        pltpu.make_async_copy(src.at[0, pl.ds(first, hidden_rows), :], dst, w_sem.at[i])
        for i, (src, dst) in enumerate(((wg_hbm, wg), (wu_hbm, wu), (wd_hbm, wd)))
    ]
    for load in loads:
        load.start()

    def remote(src, dst, send_sem, recv_sem, where):
        return pltpu.make_async_remote_copy(
            src_ref=src,
            dst_ref=dst,
            send_sem=send_sem,
            recv_sem=recv_sem,
            device_id=where,
            device_id_type=MESH,
        )

    inputs["decay"].wait()
    ti = lax.broadcasted_iota(jnp.int32, (tokens, tokens), 0)
    tj = lax.broadcasted_iota(jnp.int32, (tokens, tokens), 1)
    causal = ti >= tj
    upper = jnp.where(tj >= ti, 1.0, 0.0).astype(F32)
    cum_t = jnp.dot(
        decay_ref[...], upper, precision=lax.Precision.HIGHEST, preferred_element_type=F32
    )
    cum = jnp.transpose(cum_t)
    ending = cum[tokens - 1 : tokens, :]
    fade[...] = jnp.broadcast_to(jnp.exp(cum_t[:, tokens - 1 : tokens]), fade.shape)
    to_end = jnp.exp(ending - cum)
    lift = jnp.exp(cum)
    end_send[...] = jnp.zeros(end_send.shape, F32)
    end_send[:, 0:heads] = ending
    inputs["routes"].wait()
    lane = lax.broadcasted_iota(jnp.int32, (tokens, 128), 1)
    expert_of = lax.div(lane, SLOTS)
    slot_of = lax.rem(lane, SLOTS)
    named = jnp.transpose(routes_ref[...].astype(F32)).astype(jnp.int32)
    first_hit = named[:, 0:1] == expert_of
    second_hit = named[:, 1:2] == expert_of
    hit = jnp.where(first_hit | second_hit, 1.0, 0.0)
    strict = jnp.where(ti > tj, 1.0, 0.0).astype(BF16)
    before = jnp.dot(strict, hit.astype(BF16), preferred_element_type=F32)
    taken = (hit > 0.5) & (before.astype(jnp.int32) == slot_of) & (slot_of < CAP)
    onehot = jnp.where(taken, 1.0, 0.0)
    dispatch = jnp.transpose(onehot)[0:picked, :].astype(BF16)

    def pick(values):
        return jnp.dot(dispatch, values, preferred_element_type=F32)

    def put(ref, values):
        for e in range(n_exp):
            ref[e, :, 0:columns] = values[e * SLOTS : (e + 1) * SLOTS, :].astype(BF16)

    def take(ref):
        return ref[...].astype(F32)[:, :, 0:columns].reshape(picked, columns)

    inputs["q"].wait()
    for h in range(heads):
        cols = slice(h * hd, (h + 1) * hd)
        lifted[:, cols] = (q_ref[:, cols].astype(F32) * lift[:, h : h + 1]).astype(BF16)
    put(q_send, pick(lifted[...]))

    def keep_state():
        inputs["k"].wait()
        inputs["v"].wait()
        for h in range(heads):
            cols = slice(h * hd, (h + 1) * hd)
            faded = k_ref[:, cols].astype(F32) * to_end[:, h : h + 1]
            state = jnp.dot(
                jnp.transpose(faded).astype(BF16), v_ref[:, cols], preferred_element_type=F32
            )
            block_state[h] = state
            own_state[h] = state.astype(BF16)

    @pl.when(z < last - 1)
    def _():
        keep_state()

    pl.semaphore_wait(barrier, jnp.where(z == 0, 1, last) + peers - 1)

    def let_go():
        for i in range(1, n_exp):
            pl.semaphore_signal(
                go_sem,
                inc=1,
                device_id={"exp": lax.rem(x + i, n_exp)},
                device_id_type=MESH,
            )

    @pl.when(z > 0)
    def _():
        let_go()


    def ask(to):
        where = {"seq": to}
        return (
            remote(
                q_send.at[:, used], q_recv.at[z, :, used], q_ssem.at[to], q_rsem.at[z], where
            ),
            remote(end_send, end_recv.at[z], end_ssem.at[to], end_rsem.at[z], where),
        )

    for to in range(last):

        @pl.when(to < z)
        def _():
            for copy in ask(to):
                copy.start()

    @pl.when(z == last - 1)
    def _():
        keep_state()

    def hop(h, p, src):
        piece = pl.ds(p * part_rows, part_rows)
        return remote(
            src.at[h, piece],
            state_in.at[h, piece],
            chain_send.at[h, p],
            chain_recv.at[h, p],
            {"seq": z + 1},
        )

    def set_off(which):
        @pl.when((z == 0) & (z < last))
        def _():
            for h in which:
                for p in range(PARTS):
                    hop(h, p, own_state).start()

    lead = heads - heads // 4
    ahead = heads // 2
    set_off(range(ahead))

    @pl.when(z == last)
    def _():
        inputs["k"].wait()
        inputs["v"].wait()

    for h in range(heads):
        cols = slice(h * hd, (h + 1) * hd)
        scores = nt_dot(q_ref[:, cols], k_ref[:, cols])
        gaps = cum[:, h : h + 1] - cum_t[h : h + 1, :]
        mixing = jnp.where(causal, scores * jnp.exp(jnp.where(causal, gaps, 0.0)), 0.0)
        att[:, cols] = jnp.dot(mixing.astype(BF16), v_ref[:, cols], preferred_element_type=F32)

    for name in ("res", "gate", "again", "mgain", "rw"):
        inputs[name].wait()
    near_att = pick(att[...].astype(BF16))
    near_res = pick(res_ref[...])
    near_v = jax.nn.sigmoid(pick(gate_ref[...])) * again_ref[...]
    near[0] = near_att
    near[1] = near_v
    near[2] = near_res

    spot = lax.broadcasted_iota(jnp.int32, (picked, 128), 1)

    def peer_of(i):
        to = lax.rem(me + 1 + i, peers)
        return {"exp": lax.div(to, n_rep), "rep": lax.rem(to, n_rep)}

    def products(attended, gated, residual):
        u = gated * attended
        parts = (attended * attended, residual * u, u * u, residual * residual)
        return u, [jnp.sum(part, axis=1, keepdims=True) for part in parts]

    def first_tell(i):
        return remote(
            first_sums.at[me], first_sums.at[me], first_ssem, first_rsem, peer_of(i)
        )

    @pl.when(z == 0)
    def _():
        _, wholes = products(near_att, near_v, near_res)
        table = jnp.zeros((picked, 128), F32)
        for n, whole in enumerate(wholes):
            table = jnp.where(spot == n, whole, table)
        first_sums[me] = table
        for i in range(peers - 1):
            first_tell(i).start()

    def to_home(i):
        return remote(
            extra_send.at[i, :, used],
            extra_recv.at[i, :, used],
            extra_ssem.at[i],
            extra_rsem.at[i],
            {"seq": middle},
        )

    @pl.when(z > 0)
    def _():
        put(res_pack, near_res * mgain_ref[...])
        res_rows[r, here] = res_pack[x]

    if middle != last:

        @pl.when(z == last)
        def _():
            for i, value in enumerate((near_att, near_v, near_res)):
                put(extra_send.at[i], value)
                to_home(i).start()

    def own_line(send, order=None):
        for i in order or [n for k in range(n_seq) for n in (last - k, k)][:n_seq]:

            @pl.when(i != z)
            def _():
                send(x, i)

    def other_lines(send, order=None):
        for j in range(1, n_exp):
            for i in order or [n for k in range(n_seq) for n in (last - k, k)][:n_seq]:
                send(lax.rem(x + j, n_exp), i)

    def send_res(e, to):
        remote(
            res_pack.at[e, used],
            res_rows.at[r, here, used],
            res_ssem,
            res_rsem,
            {"exp": e, "seq": to},
        ).start()

    def keep(b, i):
        rows[r, x * n_seq + b] = pack[i, x]

    def spread(b, i):
        spot_of = x * n_seq + b

        def send(e, to):
            remote(
                pack.at[i, e, used],
                rows.at[r, spot_of, used],
                disp_send,
                disp_recv,
                {"exp": e, "seq": to},
            ).start()

        return send

    def hand_out(b, i, attended, gated, residual):
        u, wholes = products(attended, gated, residual)
        table = jnp.zeros((picked, 128), F32)
        for n, whole in enumerate(wholes):
            coarse = whole.astype(BF16).astype(F32)
            table = jnp.where(spot == n, coarse, table)
            table = jnp.where(spot == n + len(wholes), whole - coarse, table)
        put(pack.at[i], u * mgain_ref[...])
        for e in range(n_exp):
            pack[i, e, :, columns:] = table[e * SLOTS : (e + 1) * SLOTS, :].astype(BF16)
        keep(b, i)
        return spread(b, i)

    def norms(total):
        s1 = lax.rsqrt(total[0] / width + EPSILON)
        moe = total[3] + s1 * (2.0 * total[1] + s1 * total[2])
        return s1, lax.rsqrt(jnp.maximum(moe, 0.0) / width + EPSILON)

    @pl.when(z > 0)
    def _():
        own_line(send_res)
        pl.semaphore_wait(go_sem, n_exp - 1)
        other_lines(send_res)

    def offer(b):
        target = tail_recv if b == last else part_recv
        return remote(
            part_send.at[b, :, used],
            target.at[z, :, used],
            part_ssem.at[b],
            part_rsem.at[1 if b == last else 0, z],
            {"seq": home(b)},
        )

    def relay(h):
        for p in range(PARTS):
            piece = slice(p * part_rows, (p + 1) * part_rows)
            hop(h, p, state_out).wait_recv()
            state_out[h, piece] = (
                fade[h : h + 1, :] * state_in[h, piece].astype(F32) + block_state[h, piece]
            ).astype(BF16)
            hop(h, p, state_out).start()

    def relays(where, which):
        @pl.when(where)
        def _():
            for h in which:
                relay(h)

    chained = (z > 0) & (z < last)
    for b in range(1, n_seq):

        @pl.when(z < b)
        def _():
            ask_q = remote(q_send.at[:, used], q_recv.at[b, :, used], q_ssem.at[0], q_rsem.at[b], {"seq": 0})
            ask_e = remote(end_send, end_recv.at[b], end_ssem.at[0], end_rsem.at[b], {"seq": 0})
            ask_q.wait_recv()
            ask_e.wait_recv()
            between = jnp.zeros((1, 128), F32)
            for m in range(1, b):
                between += jnp.where(m > z, end_recv[m], 0.0)
            between = jnp.exp(between)
            asked = take(q_recv.at[b]).astype(BF16)
            given = [
                jnp.dot(
                    asked[:, h * hd : (h + 1) * hd], own_state[h], preferred_element_type=F32
                )
                * between[:, h : h + 1]
                for h in range(heads)
            ]
            given = jnp.concatenate(given, axis=1)
            put(part_send.at[b], given)

            @pl.when(z != home(b))
            def _():
                offer(b).start()

            if b == last:

                @pl.when(z == home(b))
                def _():
                    put(tail_recv.at[z], given)

    @pl.when(z == 0)
    def _():
        let_go()

    relays(chained & (z == 1), range(ahead))

    @pl.when(z == 0)
    def _():
        everyone = first_sums.at[pl.ds(0, peers - 1)]
        pltpu.make_async_copy(everyone, everyone, first_rsem).wait()
        total = jnp.sum(first_sums[...], axis=0)
        s1, s2 = norms([total[:, n : n + 1] for n in range(4)])
        normed = (near[2] + s1 * (near[0] * near[1])) * s2 * mgain_ref[...]
        put(pack.at[0], normed)
        keep(0, 0)
        own_line(spread(0, 0))

    set_off(range(ahead, lead))

    @pl.when(z == 0)
    def _():
        pl.semaphore_wait(go_sem, n_exp - 1)
        other_lines(spread(0, 0))

    set_off(range(lead, heads))

    def wait_part(which, source):
        buffer = tail_recv if which else part_recv
        remote(
            part_send.at[0, :, used],
            buffer.at[source, :, used],
            part_ssem.at[0],
            part_rsem.at[which, source],
            {"seq": 0},
        ).wait_recv()

    @pl.when((z > 0) & (z < last))
    def _():
        acc[...] = near[0]
        for source in range(last):

            @pl.when(source < z)
            def _():
                wait_part(0, source)
                acc[...] += take(part_recv.at[source])

        send = hand_out(z, 0, acc[...], near[1], near[2])
        own_line(send)
        other_lines(send)


    @pl.when(z == middle)
    def _():
        for i in range(3):
            to_home(i).wait_recv()
        whole = take(extra_recv.at[0])
        whole += take(tail_recv.at[middle])
        for source in range(last):
            if source != middle:
                wait_part(1, source)
                whole += take(tail_recv.at[source])
        send = hand_out(last, 1, whole, take(extra_recv.at[1]), take(extra_recv.at[2]))
        order = sorted(range(n_seq), key=lambda i: -abs(i - middle))
        own_line(send, order)
        other_lines(send, order)

    relays(chained & (z == 1), range(ahead, lead))

    slots = n_seq * SLOTS

    def project(table, s):
        gate_part = up_part = 0.0
        for e in range(n_exp):
            chunk = table[s, pl.ds(e * n_seq, n_seq)].astype(F32)[:, :, 0:columns]
            chunk = chunk.reshape(slots, columns).astype(BF16)
            at = pl.ds(pl.multiple_of((e * n_rep + s) * columns, 128), columns)
            gate_part += nt_dot(wg[:, at], chunk)
            up_part += nt_dot(wu[:, at], chunk)
        return gate_part, up_part

    def swap(table, i):
        return remote(
            table.at[r], table.at[r], swap_send.at[i], swap_recv.at[i], {"rep": other}
        )

    res_sent = res_rows.at[r, pl.ds(0, plane - 1), used]
    for n in range(2):

        @pl.when(jnp.where(z > 0, 1, 0) == n)
        def _():
            arrived = res_rows.at[r, pl.ds(0, plane - n_exp - n), used]
            pltpu.make_async_copy(arrived, arrived, res_rsem).wait()

    swap(res_rows, 0).start()
    for load in loads:
        load.wait()
    gate_val, up_val = project(res_rows, r)
    swap(res_rows, 0).wait()
    gate_part, up_part = project(res_rows, other)
    gate_early[...] = gate_val + gate_part
    up_early[...] = up_val + up_part

    relays(chained & (z == 1), range(lead, heads))
    relays(chained & (z > 1), range(ahead))

    mine = jnp.where(z < last, 1, 0) + jnp.where(z == middle, 1, 0)
    for n in range(3):

        @pl.when(mine == n)
        def _():
            arrived = rows.at[r, pl.ds(0, plane - n), used]
            pltpu.make_async_copy(arrived, arrived, disp_recv).wait()

    swap(rows, 1).start()
    gate_val, up_val = project(rows, r)
    relays(chained & (z > 1), range(ahead, lead))
    swap(rows, 1).wait()
    gate_part, up_part = project(rows, other)
    table = 0.0
    for s in range(n_rep):
        for e in range(n_exp):
            table += rows[s, pl.ds(e * n_seq, n_seq)].astype(F32)[:, :, columns:]
    table = jnp.transpose(table.reshape(slots, 128))
    total = table[0:4, :] + table[4:8, :]
    s1, s2 = norms([total[n : n + 1, :] for n in range(4)])
    whole = lax.broadcasted_iota(jnp.int32, (hidden_rows, slots), 1) < SLOTS
    gate_b, up_b = gate_val + gate_part, up_val + up_part
    gate_val = jnp.where(whole, gate_b, s2 * (gate_early[...] + s1 * gate_b))
    up_val = jnp.where(whole, up_b, s2 * (up_early[...] + s1 * up_b))
    inner = gate_val / (1.0 + jnp.exp(-gate_val)) * up_val
    if hidden_rows == whole_rows:
        unit = lax.broadcasted_iota(jnp.int32, inner.shape, 0)
        inner = jnp.where(lax.div(unit, whole_rows // n_rep) == r, inner, 0.0)
    inner = jnp.transpose(inner).astype(BF16)
    relays(chained & (z > 1), range(lead, heads))

    def product(e, s):
        at = pl.multiple_of((e * n_rep + s) * columns, 128)
        return jnp.dot(inner, wd[:, pl.ds(at, columns)], preferred_element_type=F32)

    def half(e):
        return remote(
            half_send.at[e], half_recv.at[e], half_ssem.at[e], half_rsem.at[e], {"rep": other}
        )

    for e in range(n_exp):
        half_send[e] = product(e, other).astype(BF16)
        half(e).start()

    for e in range(n_exp):
        own = product(e, r)
        half(e).wait_recv()
        whole = (own + half_recv[e].astype(F32)).reshape(n_seq, SLOTS, columns)
        fin[pl.ds(e * n_seq, n_seq)] = whole.astype(BF16)

    back[here] = fin[here]

    def hand_back(e, to):
        remote(
            fin.at[e * n_seq + to, used],
            back.at[here, used],
            back_send,
            back_recv,
            {"exp": e, "seq": to},
        ).start()

    other_lines(hand_back)
    own_line(hand_back)

    @pl.when(z == last)
    def _():
        for h in range(heads):
            for p in range(PARTS):
                hop(h, p, state_out).wait_recv()

    @pl.when(z > 0)
    def _():
        for h in range(heads):
            cols = slice(h * hd, (h + 1) * hd)
            att[:, cols] += jnp.dot(
                lifted[:, cols], state_in[h], preferred_element_type=F32
            )

    attended = att[...]
    square = jnp.sum(attended * attended, axis=1, keepdims=True)
    table = jnp.where(lane == 0, square, 0.0)
    sums[me] = jnp.transpose(table)[0:8, :]

    def tell(i):
        return remote(sums.at[me], sums.at[me], sums_send, sums_recv, peer_of(i))

    for i in range(peers - 1):
        tell(i).start()
    u_buf[...] = jax.nn.sigmoid(gate_ref[...].astype(F32)) * attended * again_ref[...]
    shares = jnp.transpose(rw_ref[...])
    combine = jnp.where(first_hit, shares[:, 0:1], shares[:, 1:2]) * onehot
    coarse = combine.astype(BF16)
    fine = (combine - coarse.astype(F32)).astype(BF16)

    for to in range(last):

        @pl.when(to < z)
        def _():
            for copy in ask(to):
                copy.wait_send()

    if middle != last:

        @pl.when(z == last)
        def _():
            for i in range(3):
                to_home(i).wait_send()

    for b in range(1, n_seq):

        @pl.when((z < b) & (z != home(b)))
        def _():
            offer(b).wait_send()

    @pl.when(z < last)
    def _():
        for h in range(heads):
            for p in range(PARTS):
                hop(h, p, state_out).wait_send()

    @pl.when(z > 0)
    def _():
        pltpu.make_async_copy(res_sent, res_sent, res_ssem).wait()

    @pl.when(z == 0)
    def _():
        everyone = first_sums.at[pl.ds(0, peers - 1)]
        pltpu.make_async_copy(everyone, everyone, first_ssem).wait()

    for n in range(1, 3):

        @pl.when(mine == n)
        def _():
            for _ in range(n):
                sent = rows.at[r, pl.ds(0, plane - 1), used]
                pltpu.make_async_copy(sent, sent, disp_send).wait()

    for e in range(n_exp):
        half(e).wait_send()

    many = sums.at[pl.ds(0, peers - 1)]
    pltpu.make_async_copy(many, many, sums_recv).wait()
    total = jnp.sum(sums[...], axis=0)
    scale = lax.rsqrt(total / width + EPSILON)
    scale = jnp.transpose(scale)[:, 0:1]
    u_buf[...] = res_ref[...].astype(F32) + scale * u_buf[...]
    pltpu.make_async_copy(many, many, sums_send).wait()

    returned = back.at[pl.ds(0, plane - 1), used]
    pltpu.make_async_copy(returned, returned, back_recv).wait()
    result = u_buf[...]
    for e in range(n_exp):
        rows_e = jnp.sum(back[pl.ds(e * n_seq, n_seq)].astype(F32), axis=0)
        slot = lax.broadcasted_iota(jnp.int32, rows_e.shape, 0)
        rows_e = jnp.where(slot < CAP, rows_e, 0.0).astype(BF16)
        lanes = slice(e * SLOTS, (e + 1) * SLOTS)
        result += jnp.dot(coarse[:, lanes], rows_e, preferred_element_type=F32)
        result += jnp.dot(fine[:, lanes], rows_e, preferred_element_type=F32)
    out_ref[...] = result.astype(BF16)
    pltpu.make_async_copy(returned, returned, back_send).wait()


def solution(mesh):
    n_seq, n_exp, n_rep = (mesh.shape[a] for a in ("seq", "exp", "rep"))

    def shards(
        queries,
        key_rows,
        value_rows,
        decay_log,
        residual,
        out_gate,
        attn_gain,
        moe_gain,
        routes,
        route_weights,
        w_gate,
        w_up,
        w_down,
    ):
        tokens, columns = queries.shape
        heads = decay_log.shape[1]
        hd = columns // heads
        _, whole_rows, width = w_gate.shape
        even = whole_rows % (16 * n_rep) == 0
        hidden_rows = whole_rows // n_rep if even else whole_rows
        plane = n_exp * n_seq
        slots = n_seq * SLOTS
        vmem = pl.BlockSpec(memory_space=pltpu.VMEM)
        hbm = pl.BlockSpec(memory_space=pltpu.HBM)
        dma = pltpu.SemaphoreType.DMA
        if 2 < n_seq <= SHORT:
            wide = columns + 128
            return pl.pallas_call(
                lambda *refs: direct_kernel(n_seq, n_exp, n_rep, *refs),
                name="layer",
                out_shape=pltpu.VMEM((tokens, columns), BF16),
                in_specs=[hbm] * 13,
                out_specs=vmem,
                scratch_shapes=[
                    pltpu.VMEM((tokens, columns), BF16),
                    pltpu.VMEM((tokens, columns), BF16),
                    pltpu.VMEM((heads, tokens), F32),
                    pltpu.VMEM((tokens, columns), BF16),
                    pltpu.VMEM((2, tokens), jnp.int32),
                    pltpu.VMEM((2, tokens), F32),
                    pltpu.VMEM((tokens, columns), BF16),
                    pltpu.VMEM((tokens, columns), BF16),
                    pltpu.VMEM((1, columns), F32),
                    pltpu.VMEM((1, columns), F32),
                    pltpu.VMEM((hidden_rows, width), BF16),
                    pltpu.VMEM((hidden_rows, width), BF16),
                    pltpu.VMEM((hidden_rows, width), BF16),
                    pltpu.VMEM((heads, hd, hd), BF16),
                    pltpu.VMEM((heads, hd, hd), BF16),
                    pltpu.VMEM((heads, hd, hd), BF16),
                    pltpu.VMEM((heads, hd, hd), F32),
                    pltpu.VMEM((tokens, columns), BF16),
                    pltpu.VMEM((tokens, columns), F32),
                    pltpu.VMEM((tokens, columns), F32),
                    pltpu.VMEM((n_exp * n_rep, 8, tokens), F32),
                    pltpu.VMEM((n_exp * n_rep, n_exp * SLOTS, 128), F32),
                    pltpu.VMEM((1, 128), F32),
                    pltpu.VMEM((n_seq, 1, 128), F32),
                    pltpu.VMEM((n_exp, SLOTS, columns), BF16),
                    pltpu.VMEM((n_seq, n_exp, SLOTS, columns), BF16),
                    pltpu.VMEM((n_seq, n_exp, SLOTS, columns), BF16),
                    pltpu.VMEM((n_seq, n_exp, SLOTS, columns), BF16),
                    pltpu.VMEM((n_seq, n_exp, SLOTS, columns), BF16),
                    pltpu.VMEM((3, n_exp, SLOTS, columns), BF16),
                    pltpu.VMEM((3, n_exp, SLOTS, columns), BF16),
                    pltpu.VMEM((3, n_exp * SLOTS, columns), F32),
                    pltpu.VMEM((n_exp * SLOTS, columns), F32),
                    pltpu.VMEM((heads, 128), F32),
                    pltpu.VMEM((n_exp, SLOTS, columns), BF16),
                    pltpu.VMEM((n_rep, plane, SLOTS, columns), BF16),
                    pltpu.VMEM((2, n_exp, SLOTS, wide), BF16),
                    pltpu.VMEM((n_rep, plane, SLOTS, wide), BF16),
                    pltpu.VMEM((hidden_rows, slots), F32),
                    pltpu.VMEM((hidden_rows, slots), F32),
                    pltpu.VMEM((n_exp, slots, columns), BF16),
                    pltpu.VMEM((n_exp, slots, columns), BF16),
                    pltpu.VMEM((plane, SLOTS, columns), BF16),
                    pltpu.VMEM((plane, SLOTS, columns), BF16),
                    dma((10,)),
                    dma((3,)),
                    pltpu.SemaphoreType.REGULAR,
                    dma((heads, PARTS)),
                    dma((heads, PARTS)),
                    dma,
                    dma,
                    dma,
                    dma,
                    dma((n_seq,)),
                    dma((n_seq,)),
                    dma((n_seq,)),
                    dma((n_seq,)),
                    dma((n_seq,)),
                    dma((2, n_seq)),
                    dma((3,)),
                    dma((3,)),
                    dma,
                    dma,
                    dma,
                    dma,
                    dma((2,)),
                    dma((2,)),
                    dma((n_exp,)),
                    dma((n_exp,)),
                    dma,
                    dma,
                ],
                compiler_params=pltpu.CompilerParams(
                    collective_id=0, has_side_effects=True, vmem_limit_bytes=63000000
                ),
            )(
                key_rows,
                value_rows,
                decay_log.T,
                queries,
                routes.T,
                route_weights.T,
                residual,
                out_gate,
                attn_gain.reshape(1, columns),
                moe_gain.reshape(1, columns),
                w_gate,
                w_up,
                w_down,
            )
        return pl.pallas_call(
            lambda *refs: chain_kernel(n_seq, n_exp, n_rep, *refs),
            name="layer",
            out_shape=pltpu.VMEM((tokens, columns), BF16),
            in_specs=[hbm] * 13,
            out_specs=vmem,
            scratch_shapes=[
                pltpu.VMEM((tokens, columns), BF16),
                pltpu.VMEM((tokens, columns), BF16),
                pltpu.VMEM((heads, tokens), F32),
                pltpu.VMEM((tokens, columns), BF16),
                pltpu.VMEM((2, tokens), jnp.int32),
                pltpu.VMEM((2, tokens), F32),
                pltpu.VMEM((tokens, columns), BF16),
                pltpu.VMEM((tokens, columns), BF16),
                pltpu.VMEM((1, columns), F32),
                pltpu.VMEM((1, columns), F32),
                pltpu.VMEM((hidden_rows, width), BF16),
                pltpu.VMEM((hidden_rows, width), BF16),
                pltpu.VMEM((hidden_rows, width), BF16),
                pltpu.VMEM((heads, hd, hd), BF16),
                pltpu.VMEM((heads, hd, hd), BF16),
                pltpu.VMEM((heads, hd, hd), F32),
                pltpu.VMEM((tokens, columns), F32),
                pltpu.VMEM((tokens, columns), F32),
                pltpu.VMEM((n_exp * n_rep, 8, tokens), F32),
                pltpu.VMEM((n_exp, SLOTS, columns), BF16),
                pltpu.VMEM((n_rep, plane, SLOTS, columns), BF16),
                pltpu.VMEM((n_exp, slots, columns), BF16),
                pltpu.VMEM((n_exp, slots, columns), BF16),
                pltpu.VMEM((plane, SLOTS, columns), BF16),
                pltpu.VMEM((plane, SLOTS, columns), BF16),
                dma((10,)),
                dma((3,)),
                pltpu.SemaphoreType.REGULAR,
                dma((heads, PARTS)),
                dma((heads, PARTS)),
                dma,
                dma,
                dma,
                dma,
                dma,
                dma,
                dma((n_exp,)),
                dma((n_exp,)),
                dma,
                dma,
            ],
            compiler_params=pltpu.CompilerParams(collective_id=0, has_side_effects=True, vmem_limit_bytes=63000000),
        )(
            key_rows,
            value_rows,
            decay_log.T,
            queries,
            routes.T,
            route_weights.T,
            residual,
            out_gate,
            attn_gain.reshape(1, columns),
            moe_gain.reshape(1, columns),
            w_gate,
            w_up,
            w_down,
        )

    block = P(("groups", "seq"), ("exp", "rep"))
    gain = P(("exp", "rep"))
    route = P(("groups", "seq"), None)
    weight = P("exp", "seq", None)
    return jax.shard_map(
        shards,
        mesh=mesh,
        in_specs=(block,) * 6 + (gain, gain, route, route) + (weight,) * 3,
        out_specs=block,
        check_vma=False,
    )
```

```python
import jax
import jax.numpy as jnp
from jax import lax
from jax.experimental import pallas as pl
from jax.experimental.pallas import tpu as pltpu
from jax.sharding import PartitionSpec as P

CAP = 6
SLOTS = 8
PARTS = 2
SHORT = 4
EPSILON = 1e-06
MESH = pl.DeviceIdType.MESH
F32 = jnp.float32
BF16 = jnp.bfloat16


def sweep(count, body):
    if count <= 16:
        for i in range(count):
            body(i)
    else:
        lax.fori_loop(0, count, lambda i, c: (body(i), c)[1], 0)


def nt_dot(a, b):
    return lax.dot_general(a, b, (((1,), (1,)), ((), ())), preferred_element_type=F32)


def chain_kernel(
    n_seq,
    n_exp,
    n_rep,
    k_hbm,
    v_hbm,
    decay_hbm,
    q_hbm,
    routes_hbm,
    rw_hbm,
    res_hbm,
    gate_hbm,
    again_hbm,
    mgain_hbm,
    wg_hbm,
    wu_hbm,
    wd_hbm,
    out_ref,
    k_ref,
    v_ref,
    decay_ref,
    q_ref,
    routes_ref,
    rw_ref,
    res_ref,
    gate_ref,
    again_ref,
    mgain_ref,
    wg,
    wu,
    wd,
    state_in,
    state_out,
    block_state,
    att,
    u_buf,
    sums,
    pack,
    rows,
    half_send,
    half_recv,
    fin,
    back,
    in_sem,
    w_sem,
    go_sem,
    chain_send,
    chain_recv,
    sums_send,
    sums_recv,
    disp_send,
    disp_recv,
    swap_send,
    swap_recv,
    half_ssem,
    half_rsem,
    back_send,
    back_recv,
):
    z = lax.axis_index("seq")
    x = lax.axis_index("exp")
    r = lax.axis_index("rep")
    other = 1 - r
    tokens, columns = q_ref.shape
    heads = decay_ref.shape[0]
    hd = columns // heads
    part_rows = hd // PARTS
    hidden_rows = wg.shape[0]
    width = columns * n_exp * n_rep
    whole_rows = wg_hbm.shape[1]

    inputs = [
        pltpu.make_async_copy(src, dst, in_sem.at[i])
        for i, (src, dst) in enumerate(
            (
                (k_hbm, k_ref),
                (v_hbm, v_ref),
                (decay_hbm, decay_ref),
                (q_hbm, q_ref),
                (routes_hbm, routes_ref),
                (rw_hbm, rw_ref),
                (res_hbm, res_ref),
                (gate_hbm, gate_ref),
                (again_hbm, again_ref),
                (mgain_hbm, mgain_ref),
            )
        )
    ]
    for load in inputs:
        load.start()
    first = pl.multiple_of(r * hidden_rows, 16) if hidden_rows != whole_rows else 0
    loads = [
        pltpu.make_async_copy(src.at[0, pl.ds(first, hidden_rows), :], dst, w_sem.at[i])
        for i, (src, dst) in enumerate(((wg_hbm, wg), (wu_hbm, wu), (wd_hbm, wd)))
    ]

    barrier = pltpu.get_barrier_semaphore()
    plane = n_exp * n_seq
    peers = n_exp * n_rep
    me = x * n_rep + r
    last = n_seq - 1

    def greet(where):
        pl.semaphore_signal(barrier, inc=1, device_id=where, device_id_type=MESH)

    @pl.when(z < last)
    def _():
        greet({"seq": z + 1})

    @pl.when(z > 0)
    def _():
        greet({"seq": z - 1})

    def greet_peer(i):
        to = lax.rem(me + 1 + i, peers)
        greet({"exp": lax.div(to, n_rep), "rep": lax.rem(to, n_rep)})

    sweep(peers - 1, greet_peer)
    for load in loads:
        load.start()
    for load in inputs[:3]:
        load.wait()

    ti = lax.broadcasted_iota(jnp.int32, (tokens, tokens), 0)
    tj = lax.broadcasted_iota(jnp.int32, (tokens, tokens), 1)
    causal = ti >= tj
    upper = jnp.where(tj >= ti, 1.0, 0.0).astype(F32)
    cum_t = jnp.dot(
        decay_ref[...], upper, precision=lax.Precision.HIGHEST, preferred_element_type=F32
    )
    cum = jnp.transpose(cum_t)
    ending = cum[tokens - 1 : tokens, :]
    fading = jnp.exp(ending)
    to_end = jnp.exp(ending - cum)
    lift = jnp.exp(cum)
    for h in range(heads):
        cols = slice(h * hd, (h + 1) * hd)
        faded = k_ref[:, cols].astype(F32) * to_end[:, h : h + 1]
        block_state[h] = jnp.dot(
            jnp.transpose(faded).astype(BF16), v_ref[:, cols], preferred_element_type=F32
        )

    ends = (z > 0).astype(jnp.int32) + (z < last).astype(jnp.int32)
    pl.semaphore_wait(barrier, peers - 1 + ends)

    def hop(h, p):
        piece = pl.ds(p * part_rows, part_rows)
        return pltpu.make_async_remote_copy(
            src_ref=state_out.at[h, piece],
            dst_ref=state_in.at[h, piece],
            send_sem=chain_send.at[h, p],
            recv_sem=chain_recv.at[h, p],
            device_id={"seq": z + 1},
            device_id_type=MESH,
        )

    @pl.when(z == 0)
    def _():
        for h in range(heads):
            state_out[h] = block_state[h].astype(BF16)
            for p in range(PARTS):
                hop(h, p).start()

    inputs[3].wait()

    for h in range(heads):
        cols = slice(h * hd, (h + 1) * hd)
        scores = nt_dot(q_ref[:, cols], k_ref[:, cols])
        gaps = cum[:, h : h + 1] - cum_t[h : h + 1, :]
        mixing = jnp.where(causal, scores * jnp.exp(jnp.where(causal, gaps, 0.0)), 0.0)
        att[:, cols] = jnp.dot(mixing.astype(BF16), v_ref[:, cols], preferred_element_type=F32)

    for load in inputs[4:]:
        load.wait()
    lane = lax.broadcasted_iota(jnp.int32, (tokens, 128), 1)
    expert_of = lax.div(lane, SLOTS)
    slot_of = lax.rem(lane, SLOTS)
    named = jnp.transpose(routes_ref[...].astype(F32)).astype(jnp.int32)
    shares = jnp.transpose(rw_ref[...])
    first_hit = named[:, 0:1] == expert_of
    second_hit = named[:, 1:2] == expert_of
    hit = jnp.where(first_hit | second_hit, 1.0, 0.0)
    strict = jnp.where(ti > tj, 1.0, 0.0).astype(BF16)
    before = jnp.dot(strict, hit.astype(BF16), preferred_element_type=F32)
    taken = (hit > 0.5) & (before.astype(jnp.int32) == slot_of) & (slot_of < CAP)
    onehot = jnp.where(taken, 1.0, 0.0)
    combine = jnp.where(first_hit, shares[:, 0:1], shares[:, 1:2]) * onehot
    dispatch = jnp.transpose(onehot)[0 : n_exp * SLOTS, :].astype(BF16)

    def let_go(i):
        pl.semaphore_signal(go_sem, inc=1, device_id={"seq": i}, device_id_type=MESH)

    for h in range(heads):
        cols = slice(h * hd, (h + 1) * hd)

        @pl.when(z > 0)
        def _():
            for p in range(PARTS):
                piece = slice(p * part_rows, (p + 1) * part_rows)
                hop(h, p).wait_recv()

                @pl.when(z < last)
                def _():
                    state_out[h, piece] = (
                        fading[:, h : h + 1] * state_in[h, piece].astype(F32)
                        + block_state[h, piece]
                    ).astype(BF16)
                    hop(h, p).start()

            lifted = (q_ref[:, cols].astype(F32) * lift[:, h : h + 1]).astype(BF16)
            att[:, cols] += jnp.dot(lifted, state_in[h], preferred_element_type=F32)

        if h == max(heads - 3, 0):

            @pl.when(z == last)
            def _():
                sweep(last, let_go)

    res = res_ref[...].astype(F32)
    attended = att[...]
    u = jax.nn.sigmoid(gate_ref[...].astype(F32)) * attended * again_ref[...]
    u_buf[...] = u
    parts = (attended * attended, res * u, u * u, res * res)
    table = jnp.zeros((tokens, 128), F32)
    for i, part in enumerate(parts):
        table = jnp.where(lane == i, jnp.sum(part, axis=1, keepdims=True), table)
    sums[me] = jnp.transpose(table)[0:8, :]

    def tell(i):
        to = lax.rem(me + 1 + i, peers)
        pltpu.make_async_remote_copy(
            src_ref=sums.at[me],
            dst_ref=sums.at[me],
            send_sem=sums_send,
            recv_sem=sums_recv,
            device_id={"exp": lax.div(to, n_rep), "rep": lax.rem(to, n_rep)},
            device_id_type=MESH,
        ).start()

    sweep(peers - 1, tell)
    many = sums.at[pl.ds(0, peers - 1)]
    pltpu.make_async_copy(many, many, sums_recv).wait()
    total = jnp.sum(sums[...], axis=0)
    s1 = lax.rsqrt(total[0:1, :] / width + EPSILON)
    moe = total[3:4, :] + s1 * (2.0 * total[1:2, :] + s1 * total[2:3, :])
    s2 = lax.rsqrt(jnp.maximum(moe, 0.0) / width + EPSILON)
    row8 = lax.broadcasted_iota(jnp.int32, (8, tokens), 0)
    scales = jnp.transpose(jnp.where(row8 == 0, s1, s2))
    hidden = res_ref[...].astype(F32) + scales[:, 0:1] * u_buf[...]
    u_buf[...] = hidden
    normed = (hidden * scales[:, 1:2] * mgain_ref[...]).astype(BF16)

    packed = jnp.dot(dispatch, normed, preferred_element_type=F32)
    for e in range(n_exp):
        pack[e] = packed[e * SLOTS : (e + 1) * SLOTS, :].astype(BF16)
    here = x * n_seq + z
    rows[r, here] = pack[x]

    def deal(e, to, source, target, send_sem, recv_sem):
        pltpu.make_async_remote_copy(
            src_ref=source,
            dst_ref=target,
            send_sem=send_sem,
            recv_sem=recv_sem,
            device_id={"exp": e, "seq": to},
            device_id_type=MESH,
        ).start()

    def deal_rows(e, to):
        used = pl.ds(0, CAP)
        deal(e, to, pack.at[e, used], rows.at[r, here, used], disp_send, disp_recv)

    def earlier(send):
        def one(i):
            @pl.when(i < z)
            def _():
                for e in range(n_exp):
                    send(e, i)

        sweep(n_seq, one)

    def level(send):
        for j in range(1, n_exp):
            send(lax.rem(x + j, n_exp), z)

    def later(send):
        def one(i):
            @pl.when(last - i > z)
            def _():
                for e in range(n_exp):
                    send(e, last - i)

        sweep(n_seq, one)

    earlier(deal_rows)
    level(deal_rows)

    @pl.when(z < last)
    def _():
        pl.semaphore_wait(go_sem, 1)

    later(deal_rows)
    arrived = rows.at[r, pl.ds(0, plane - 1), pl.ds(0, CAP)]
    pltpu.make_async_copy(arrived, arrived, disp_recv).wait()
    swap = pltpu.make_async_remote_copy(
        src_ref=rows.at[r],
        dst_ref=rows.at[r],
        send_sem=swap_send,
        recv_sem=swap_recv,
        device_id={"rep": other},
        device_id_type=MESH,
    )
    swap.start()
    for load in loads:
        load.wait()
    slots = n_seq * SLOTS

    def project(s):
        gate_part = up_part = 0.0
        for e in range(n_exp):
            chunk = rows[s, pl.ds(e * n_seq, n_seq)].astype(F32).reshape(slots, columns)
            chunk = chunk.astype(BF16)
            at = pl.ds(pl.multiple_of((e * n_rep + s) * columns, 128), columns)
            gate_part += nt_dot(wg[:, at], chunk)
            up_part += nt_dot(wu[:, at], chunk)
        return gate_part, up_part

    gate_val, up_val = project(r)
    swap.wait()
    gate_part, up_part = project(other)
    gate_val += gate_part
    up_val += up_part
    inner = gate_val / (1.0 + jnp.exp(-gate_val)) * up_val
    if hidden_rows == whole_rows:
        unit = lax.broadcasted_iota(jnp.int32, inner.shape, 0)
        inner = jnp.where(lax.div(unit, whole_rows // n_rep) == r, inner, 0.0)
    inner = jnp.transpose(inner).astype(BF16)

    def product(e, s):
        at = pl.multiple_of((e * n_rep + s) * columns, 128)
        return jnp.dot(inner, wd[:, pl.ds(at, columns)], preferred_element_type=F32)

    def half(e):
        return pltpu.make_async_remote_copy(
            src_ref=half_send.at[e],
            dst_ref=half_recv.at[e],
            send_sem=half_ssem.at[e],
            recv_sem=half_rsem.at[e],
            device_id={"rep": other},
            device_id_type=MESH,
        )

    for e in range(n_exp):
        half_send[e] = product(e, other).astype(BF16)
        half(e).start()

    here_back = x * n_seq + z
    for e in range(n_exp):
        own = product(e, r)
        half(e).wait_recv()
        whole = (own + half_recv[e].astype(F32)).reshape(n_seq, SLOTS, columns)
        fin[pl.ds(e * n_seq, n_seq)] = whole.astype(BF16)

    back[here_back] = fin[here_back]

    def hand_back(e, to):
        used = pl.ds(0, CAP)
        source = fin.at[e * n_seq + to, used]
        deal(e, to, source, back.at[here_back, used], back_send, back_recv)

    earlier(hand_back)
    later(hand_back)
    level(hand_back)
    returned = back.at[pl.ds(0, plane - 1), pl.ds(0, CAP)]
    pltpu.make_async_copy(returned, returned, back_recv).wait()
    coarse = combine.astype(BF16)
    fine = (combine - coarse.astype(F32)).astype(BF16)
    result = u_buf[...]
    for e in range(n_exp):
        rows_e = jnp.sum(back[pl.ds(e * n_seq, n_seq)].astype(F32), axis=0)
        slot = lax.broadcasted_iota(jnp.int32, rows_e.shape, 0)
        rows_e = jnp.where(slot < CAP, rows_e, 0.0).astype(BF16)
        lanes = slice(e * SLOTS, (e + 1) * SLOTS)
        result += jnp.dot(coarse[:, lanes], rows_e, preferred_element_type=F32)
        result += jnp.dot(fine[:, lanes], rows_e, preferred_element_type=F32)
    out_ref[...] = result.astype(BF16)

    for h in range(heads):

        @pl.when(z < last)
        def _():
            for p in range(PARTS):
                hop(h, p).wait_send()

    pltpu.make_async_copy(many, many, sums_send).wait()
    pltpu.make_async_copy(arrived, arrived, disp_send).wait()
    for e in range(n_exp):
        half(e).wait_send()
    pltpu.make_async_copy(returned, returned, back_send).wait()


def direct_kernel(
    n_seq,
    n_exp,
    n_rep,
    k_hbm,
    v_hbm,
    decay_hbm,
    q_hbm,
    routes_hbm,
    rw_hbm,
    res_hbm,
    gate_hbm,
    again_hbm,
    mgain_hbm,
    wg_hbm,
    wu_hbm,
    wd_hbm,
    out_ref,
    k_ref,
    v_ref,
    decay_ref,
    q_ref,
    routes_ref,
    rw_ref,
    res_ref,
    gate_ref,
    again_ref,
    mgain_ref,
    wg,
    wu,
    wd,
    state_in,
    state_out,
    own_state,
    block_state,
    lifted,
    att,
    u_buf,
    sums,
    first_sums,
    end_send,
    end_recv,
    q_send,
    q_recv,
    part_send,
    part_recv,
    tail_recv,
    extra_send,
    extra_recv,
    near,
    acc,
    fade,
    res_pack,
    res_rows,
    pack,
    rows,
    inner_head,
    inner_tail,
    fin,
    back,
    in_sem,
    w_sem,
    go_sem,
    chain_send,
    chain_recv,
    sums_send,
    sums_recv,
    first_ssem,
    first_rsem,
    q_ssem,
    q_rsem,
    end_ssem,
    end_rsem,
    part_ssem,
    part_rsem,
    extra_ssem,
    extra_rsem,
    res_ssem,
    res_rsem,
    disp_send,
    disp_recv,
    swap_send,
    swap_recv,
    inner_ssem,
    inner_rsem,
    back_send,
    back_recv,
):
    z = lax.axis_index("seq")
    x = lax.axis_index("exp")
    r = lax.axis_index("rep")
    other = 1 - r
    tokens, columns = q_ref.shape
    heads = decay_ref.shape[0]
    hd = columns // heads
    part_rows = hd // PARTS
    hidden_rows = wg.shape[0]
    width = columns * n_exp * n_rep
    cut = inner_head.shape[2]
    plane = n_exp * n_seq
    peers = n_exp * n_rep
    me = x * n_rep + r
    last = n_seq - 1
    middle = last // 2
    picked = n_exp * SLOTS
    used = pl.ds(0, CAP)
    here = x * n_seq + z

    def home(b):
        return b if b < last else middle

    inputs = {
        name: pltpu.make_async_copy(src, dst, in_sem.at[i])
        for i, (name, src, dst) in enumerate(
            (
                ("decay", decay_hbm, decay_ref),
                ("routes", routes_hbm, routes_ref),
                ("q", q_hbm, q_ref),
                ("k", k_hbm, k_ref),
                ("v", v_hbm, v_ref),
                ("res", res_hbm, res_ref),
                ("gate", gate_hbm, gate_ref),
                ("again", again_hbm, again_ref),
                ("mgain", mgain_hbm, mgain_ref),
                ("rw", rw_hbm, rw_ref),
            )
        )
    }
    for load in inputs.values():
        load.start()

    barrier = pltpu.get_barrier_semaphore()

    def greet(where):
        pl.semaphore_signal(barrier, inc=1, device_id=where, device_id_type=MESH)

    for i in range(n_seq):

        @pl.when((i != z) & ((i > 0) | (z == 1)))
        def _():
            greet({"seq": i})

    for i in range(peers - 1):
        to = lax.rem(me + 1 + i, peers)
        greet({"exp": lax.div(to, n_rep), "rep": lax.rem(to, n_rep)})

    first = pl.ds(pl.multiple_of(r * hidden_rows, 16), hidden_rows)
    loads = [
        pltpu.make_async_copy(src.at[0, first, :], dst, w_sem.at[i])
        for i, (src, dst) in enumerate(((wg_hbm, wg), (wu_hbm, wu)))
    ]
    for e in range(n_exp):
        at = pl.ds(pl.multiple_of((e * n_rep + r) * columns, 128), columns)
        loads.append(
            pltpu.make_async_copy(wd_hbm.at[0, :, at], wd.at[e], w_sem.at[len(loads)])
        )
    for load in loads:
        load.start()

    def remote(src, dst, send_sem, recv_sem, where):
        return pltpu.make_async_remote_copy(
            src_ref=src,
            dst_ref=dst,
            send_sem=send_sem,
            recv_sem=recv_sem,
            device_id=where,
            device_id_type=MESH,
        )

    inputs["decay"].wait()
    inputs["routes"].wait()
    ti = lax.broadcasted_iota(jnp.int32, (tokens, tokens), 0)
    tj = lax.broadcasted_iota(jnp.int32, (tokens, tokens), 1)
    causal = ti >= tj
    upper = jnp.where(tj >= ti, 1.0, 0.0).astype(F32)
    cum_t = jnp.dot(
        decay_ref[...], upper, precision=lax.Precision.HIGHEST, preferred_element_type=F32
    )
    cum = jnp.transpose(cum_t)
    ending = cum[tokens - 1 : tokens, :]
    fade[...] = jnp.broadcast_to(jnp.exp(cum_t[:, tokens - 1 : tokens]), fade.shape)
    to_end = jnp.exp(ending - cum)
    lift = jnp.exp(cum)
    end_send[...] = jnp.zeros(end_send.shape, F32)
    end_send[:, 0:heads] = ending
    lane = lax.broadcasted_iota(jnp.int32, (tokens, 128), 1)
    expert_of = lax.div(lane, SLOTS)
    slot_of = lax.rem(lane, SLOTS)
    named = jnp.transpose(routes_ref[...].astype(F32)).astype(jnp.int32)
    first_hit = named[:, 0:1] == expert_of
    second_hit = named[:, 1:2] == expert_of
    hit = jnp.where(first_hit | second_hit, 1.0, 0.0)
    strict = jnp.where(ti > tj, 1.0, 0.0).astype(BF16)
    before = jnp.dot(strict, hit.astype(BF16), preferred_element_type=F32)
    taken = (hit > 0.5) & (before.astype(jnp.int32) == slot_of) & (slot_of < CAP)
    onehot = jnp.where(taken, 1.0, 0.0)
    dispatch = jnp.transpose(onehot)[0:picked, :].astype(BF16)

    def pick(values):
        return jnp.dot(dispatch, values, preferred_element_type=F32)

    def put(ref, values):
        for e in range(n_exp):
            ref[e, :, 0:columns] = values[e * SLOTS : (e + 1) * SLOTS, :].astype(BF16)

    def take(ref):
        return ref[...].astype(F32)[:, :, 0:columns].reshape(picked, columns)

    inputs["q"].wait()
    for h in range(heads):
        cols = slice(h * hd, (h + 1) * hd)
        lifted[:, cols] = (q_ref[:, cols].astype(F32) * lift[:, h : h + 1]).astype(BF16)
    put(q_send, pick(lifted[...]))

    def keep_state():
        inputs["k"].wait()
        inputs["v"].wait()
        for h in range(heads):
            cols = slice(h * hd, (h + 1) * hd)
            faded = k_ref[:, cols].astype(F32) * to_end[:, h : h + 1]
            state = jnp.dot(
                jnp.transpose(faded).astype(BF16), v_ref[:, cols], preferred_element_type=F32
            )
            block_state[h] = state
            own_state[h] = state.astype(BF16)

    @pl.when(z < last - 1)
    def _():
        keep_state()

    pl.semaphore_wait(barrier, jnp.where(z == 0, 1, last) + peers - 1)

    def let_go():
        for i in range(1, n_exp):
            pl.semaphore_signal(
                go_sem,
                inc=1,
                device_id={"exp": lax.rem(x + i, n_exp)},
                device_id_type=MESH,
            )

    @pl.when(z > 0)
    def _():
        let_go()


    def ask(to):
        where = {"seq": to}
        return (
            remote(
                q_send.at[:, used], q_recv.at[z, :, used], q_ssem.at[to], q_rsem.at[z], where
            ),
            remote(end_send, end_recv.at[z], end_ssem.at[to], end_rsem.at[z], where),
        )

    def asks(which):
        for to in which:

            @pl.when(to < z)
            def _():
                for copy in ask(to):
                    copy.start()

    asks(range(1))

    @pl.when(z == last - 1)
    def _():
        keep_state()

    def hop(h, p, src):
        piece = pl.ds(p * part_rows, part_rows)
        return remote(
            src.at[h, piece],
            state_in.at[h, piece],
            chain_send.at[h, p],
            chain_recv.at[h, p],
            {"seq": z + 1},
        )

    def set_off(which):
        @pl.when((z == 0) & (z < last))
        def _():
            for h in which:
                for p in range(PARTS):
                    hop(h, p, own_state).start()

    quarter = heads // 4
    lead = heads - quarter
    set_off(range(lead))

    @pl.when(z == last)
    def _():
        inputs["k"].wait()
        inputs["v"].wait()

    asks(range(1, last))

    for h in range(heads):
        cols = slice(h * hd, (h + 1) * hd)
        scores = nt_dot(q_ref[:, cols], k_ref[:, cols])
        gaps = cum[:, h : h + 1] - cum_t[h : h + 1, :]
        mixing = jnp.where(causal, scores * jnp.exp(jnp.where(causal, gaps, 0.0)), 0.0)
        att[:, cols] = jnp.dot(mixing.astype(BF16), v_ref[:, cols], preferred_element_type=F32)

    for name in ("res", "gate", "again", "mgain", "rw"):
        inputs[name].wait()
    near_att = pick(att[...].astype(BF16))
    near_res = pick(res_ref[...])
    near_v = jax.nn.sigmoid(pick(gate_ref[...])) * again_ref[...]
    near[0] = near_att
    near[1] = near_v
    near[2] = near_res

    spot = lax.broadcasted_iota(jnp.int32, (picked, 128), 1)

    def peer_of(i):
        to = lax.rem(me + 1 + i, peers)
        return {"exp": lax.div(to, n_rep), "rep": lax.rem(to, n_rep)}

    def products(attended, gated, residual):
        u = gated * attended
        parts = (attended * attended, residual * u, u * u, residual * residual)
        return u, [jnp.sum(part, axis=1, keepdims=True) for part in parts]

    def first_tell(i):
        return remote(
            first_sums.at[me], first_sums.at[me], first_ssem, first_rsem, peer_of(i)
        )

    @pl.when(z == 0)
    def _():
        _, wholes = products(near_att, near_v, near_res)
        table = jnp.zeros((picked, 128), F32)
        for n, whole in enumerate(wholes):
            table = jnp.where(spot == n, whole, table)
        first_sums[me] = table
        for i in range(peers - 1):
            first_tell(i).start()

    def to_home(i):
        return remote(
            extra_send.at[i, :, used],
            extra_recv.at[i, :, used],
            extra_ssem.at[i],
            extra_rsem.at[i],
            {"seq": middle},
        )

    @pl.when(z > 0)
    def _():
        put(res_pack, near_res * mgain_ref[...])
        res_rows[r, here] = res_pack[x]

    if middle != last:

        @pl.when(z == last)
        def _():
            for i, value in enumerate((near_att, near_v, near_res)):
                put(extra_send.at[i], value)
                to_home(i).start()

    def own_line(send, order=None):
        for i in order or [n for k in range(n_seq) for n in (last - k, k)][:n_seq]:

            @pl.when(i != z)
            def _():
                send(x, i)

    def other_lines(send, order=None):
        for j in range(1, n_exp):
            for i in order or [n for k in range(n_seq) for n in (last - k, k)][:n_seq]:
                send(lax.rem(x + j, n_exp), i)

    def send_res(e, to):
        remote(
            res_pack.at[e, used],
            res_rows.at[r, here, used],
            res_ssem,
            res_rsem,
            {"exp": e, "seq": to},
        ).start()

    def keep(b, i):
        rows[r, x * n_seq + b] = pack[i, x]

    def spread(b, i):
        spot_of = x * n_seq + b

        def send(e, to):
            remote(
                pack.at[i, e, used],
                rows.at[r, spot_of, used],
                disp_send,
                disp_recv,
                {"exp": e, "seq": to},
            ).start()

        return send

    def hand_out(b, i, attended, gated, residual):
        u, wholes = products(attended, gated, residual)
        table = jnp.zeros((picked, 128), F32)
        for n, whole in enumerate(wholes):
            coarse = whole.astype(BF16).astype(F32)
            table = jnp.where(spot == n, coarse, table)
            table = jnp.where(spot == n + len(wholes), whole - coarse, table)
        put(pack.at[i], u * mgain_ref[...])
        for e in range(n_exp):
            pack[i, e, :, columns:] = table[e * SLOTS : (e + 1) * SLOTS, :].astype(BF16)
        keep(b, i)
        return spread(b, i)

    def norms(total):
        s1 = lax.rsqrt(total[0] / width + EPSILON)
        moe = total[3] + s1 * (2.0 * total[1] + s1 * total[2])
        return s1, lax.rsqrt(jnp.maximum(moe, 0.0) / width + EPSILON)

    def send_all_res():
        own_line(send_res)
        pl.semaphore_wait(go_sem, n_exp - 1)
        other_lines(send_res)

    @pl.when((z > 0) & (z != last - 1))
    def _():
        send_all_res()

    def offer(b):
        target = tail_recv if b == last else part_recv
        return remote(
            part_send.at[b, :, used],
            target.at[z, :, used],
            part_ssem.at[b],
            part_rsem.at[1 if b == last else 0, z],
            {"seq": home(b)},
        )

    def relay(h):
        for p in range(PARTS):
            piece = slice(p * part_rows, (p + 1) * part_rows)
            hop(h, p, state_out).wait_recv()
            state_out[h, piece] = (
                fade[h : h + 1, :] * state_in[h, piece].astype(F32) + block_state[h, piece]
            ).astype(BF16)
            hop(h, p, state_out).start()

    def relays(where, which):
        @pl.when(where)
        def _():
            for h in which:
                relay(h)

    chained = (z > 0) & (z < last)
    for b in range(1, n_seq):

        @pl.when(z < b)
        def _():
            ask_q = remote(q_send.at[:, used], q_recv.at[b, :, used], q_ssem.at[0], q_rsem.at[b], {"seq": 0})
            ask_e = remote(end_send, end_recv.at[b], end_ssem.at[0], end_rsem.at[b], {"seq": 0})
            ask_q.wait_recv()
            ask_e.wait_recv()
            between = jnp.zeros((1, 128), F32)
            for m in range(1, b):
                between += jnp.where(m > z, end_recv[m], 0.0)
            between = jnp.exp(between)
            asked = take(q_recv.at[b]).astype(BF16)
            given = [
                jnp.dot(
                    asked[:, h * hd : (h + 1) * hd], own_state[h], preferred_element_type=F32
                )
                * between[:, h : h + 1]
                for h in range(heads)
            ]
            given = jnp.concatenate(given, axis=1)
            put(part_send.at[b], given)

            @pl.when(z != home(b))
            def _():
                offer(b).start()

            if b == last:

                @pl.when(z == home(b))
                def _():
                    put(tail_recv.at[z], given)

    @pl.when(z == 0)
    def _():
        let_go()

    if last > 1:

        @pl.when(z == last - 1)
        def _():
            send_all_res()

    relays(chained & (z == 1), range(quarter))

    @pl.when(z == 0)
    def _():
        everyone = first_sums.at[pl.ds(0, peers - 1)]
        pltpu.make_async_copy(everyone, everyone, first_rsem).wait()
        total = jnp.sum(first_sums[...], axis=0)
        s1, s2 = norms([total[:, n : n + 1] for n in range(4)])
        normed = (near[2] + s1 * (near[0] * near[1])) * s2 * mgain_ref[...]
        put(pack.at[0], normed)
        keep(0, 0)
        own_line(spread(0, 0))

    @pl.when(z == 0)
    def _():
        pl.semaphore_wait(go_sem, n_exp - 1)
        other_lines(spread(0, 0))

    set_off(range(lead, heads))

    def wait_part(which, source):
        buffer = tail_recv if which else part_recv
        remote(
            part_send.at[0, :, used],
            buffer.at[source, :, used],
            part_ssem.at[0],
            part_rsem.at[which, source],
            {"seq": 0},
        ).wait_recv()

    @pl.when((z > 0) & (z < last))
    def _():
        acc[...] = near[0]
        for source in range(last):

            @pl.when(source < z)
            def _():
                wait_part(0, source)
                acc[...] += take(part_recv.at[source])

        send = hand_out(z, 0, acc[...], near[1], near[2])
        own_line(send)
        other_lines(send)


    @pl.when(z == middle)
    def _():
        for i in range(3):
            to_home(i).wait_recv()
        whole = take(extra_recv.at[0])
        whole += take(tail_recv.at[middle])
        for source in range(last):
            if source != middle:
                wait_part(1, source)
                whole += take(tail_recv.at[source])
        send = hand_out(last, 1, whole, take(extra_recv.at[1]), take(extra_recv.at[2]))
        order = sorted(range(n_seq), key=lambda i: -abs(i - middle))
        own_line(send, order)
        other_lines(send, order)

    slots = n_seq * SLOTS

    def pair(s, e):
        return jnp.concatenate(
            [
                table[s, pl.ds(e * n_seq, n_seq)]
                .astype(F32)[:, :, 0:columns]
                .reshape(slots, columns)
                .astype(BF16)
                for table in (rows, res_rows)
            ],
            axis=0,
        )

    def project(s, lines):
        gate_part = up_part = 0.0
        for e in range(n_exp):
            chunk = pair(s, e)
            at = pl.ds(pl.multiple_of((e * n_rep + s) * columns, 128), columns)
            gate_part += nt_dot(wg[lines, at], chunk)
            up_part += nt_dot(wu[lines, at], chunk)
        return gate_part, up_part

    def swap(table, i):
        return remote(
            table.at[r], table.at[r], swap_send.at[i], swap_recv.at[i], {"rep": other}
        )

    res_sent = res_rows.at[r, pl.ds(0, plane - 1), used]
    for n in range(2):

        @pl.when(jnp.where(z > 0, 1, 0) == n)
        def _():
            arrived = res_rows.at[r, pl.ds(0, plane - n_exp - n), used]
            pltpu.make_async_copy(arrived, arrived, res_rsem).wait()

    swap(res_rows, 0).start()
    relays(chained & (z == 1), range(quarter, heads))
    relays(chained & (z > 1), range(quarter))
    for load in loads:
        load.wait()

    mine = jnp.where(z < last, 1, 0) + jnp.where(z == middle, 1, 0)
    for n in range(3):

        @pl.when(mine == n)
        def _():
            arrived = rows.at[r, pl.ds(0, plane - n), used]
            pltpu.make_async_copy(arrived, arrived, disp_recv).wait()

    swap(rows, 1).start()
    gate_own, up_own = project(r, slice(0, hidden_rows))
    relays(chained & (z > 1), range(quarter, 2 * quarter))
    swap(res_rows, 0).wait()
    swap(rows, 1).wait()
    table = 0.0
    for s in range(n_rep):
        for e in range(n_exp):
            table += rows[s, pl.ds(e * n_seq, n_seq)].astype(F32)[:, :, columns:]
    table = table.reshape(slots, 128)
    s1, s2 = norms([table[:, n : n + 1] + table[:, n + 4 : n + 5] for n in range(4)])
    whole = lax.broadcasted_iota(jnp.int32, (slots, 1), 0) < SLOTS

    def scaled(values):
        values = jnp.transpose(values)
        fresh = values[0:slots, :]
        return jnp.where(whole, fresh, s2 * (values[slots:, :] + s1 * fresh))

    def share(i):
        part = (inner_head, inner_tail)[i]
        return remote(
            part.at[r], part.at[r], inner_ssem.at[i], inner_rsem.at[i], {"rep": other}
        )

    for i, lines in enumerate((slice(0, cut), slice(cut, hidden_rows))):
        gate_part, up_part = project(other, lines)
        gate_val = scaled(gate_own[lines] + gate_part)
        up_val = scaled(up_own[lines] + up_part)
        inner = gate_val / (1.0 + jnp.exp(-gate_val)) * up_val
        (inner_head, inner_tail)[i][r] = inner.astype(BF16)
        share(i).start()

    relays(chained & (z > 1), range(2 * quarter, lead))

    def product(e, s):
        start = s * hidden_rows
        head = pl.ds(pl.multiple_of(start, 16), cut)
        tail = pl.ds(pl.multiple_of(start + cut, 16), hidden_rows - cut)
        return jnp.dot(
            inner_head[s], wd[e, head, :], preferred_element_type=F32
        ) + jnp.dot(inner_tail[s], wd[e, tail, :], preferred_element_type=F32)

    halves = [product(e, r) for e in range(n_exp)]
    for i in range(2):
        share(i).wait_recv()
    for e in range(n_exp):
        both = (halves[e] + product(e, other)).reshape(n_seq, SLOTS, columns)
        fin[pl.ds(e * n_seq, n_seq)] = both.astype(BF16)

    relays(chained & (z > 1), range(lead, heads))

    back[here] = fin[here]

    def hand_back(e, to):
        remote(
            fin.at[e * n_seq + to, used],
            back.at[here, used],
            back_send,
            back_recv,
            {"exp": e, "seq": to},
        ).start()

    other_lines(hand_back)
    own_line(hand_back)


    @pl.when(z == last)
    def _():
        for h in range(heads):
            for p in range(PARTS):
                hop(h, p, state_out).wait_recv()

    @pl.when(z > 0)
    def _():
        for h in range(heads):
            cols = slice(h * hd, (h + 1) * hd)
            att[:, cols] += jnp.dot(
                lifted[:, cols], state_in[h], preferred_element_type=F32
            )

    attended = att[...]
    square = jnp.sum(attended * attended, axis=1, keepdims=True)
    table = jnp.where(lane == 0, square, 0.0)
    sums[me] = jnp.transpose(table)[0:8, :]

    def tell(i):
        return remote(sums.at[me], sums.at[me], sums_send, sums_recv, peer_of(i))

    for i in range(peers - 1):
        tell(i).start()
    u_buf[...] = jax.nn.sigmoid(gate_ref[...].astype(F32)) * attended * again_ref[...]
    shares = jnp.transpose(rw_ref[...])
    combine = jnp.where(first_hit, shares[:, 0:1], shares[:, 1:2]) * onehot
    coarse = combine.astype(BF16)
    fine = (combine - coarse.astype(F32)).astype(BF16)

    for to in range(last):

        @pl.when(to < z)
        def _():
            for copy in ask(to):
                copy.wait_send()

    if middle != last:

        @pl.when(z == last)
        def _():
            for i in range(3):
                to_home(i).wait_send()

    for b in range(1, n_seq):

        @pl.when((z < b) & (z != home(b)))
        def _():
            offer(b).wait_send()

    @pl.when(z < last)
    def _():
        for h in range(heads):
            for p in range(PARTS):
                hop(h, p, state_out).wait_send()

    @pl.when(z > 0)
    def _():
        pltpu.make_async_copy(res_sent, res_sent, res_ssem).wait()

    @pl.when(z == 0)
    def _():
        everyone = first_sums.at[pl.ds(0, peers - 1)]
        pltpu.make_async_copy(everyone, everyone, first_ssem).wait()

    for n in range(1, 3):

        @pl.when(mine == n)
        def _():
            for _ in range(n):
                sent = rows.at[r, pl.ds(0, plane - 1), used]
                pltpu.make_async_copy(sent, sent, disp_send).wait()

    for i in range(2):
        share(i).wait_send()

    many = sums.at[pl.ds(0, peers - 1)]
    pltpu.make_async_copy(many, many, sums_recv).wait()
    total = jnp.sum(sums[...], axis=0)
    scale = lax.rsqrt(total / width + EPSILON)
    scale = jnp.transpose(scale)[:, 0:1]
    u_buf[...] = res_ref[...].astype(F32) + scale * u_buf[...]
    pltpu.make_async_copy(many, many, sums_send).wait()

    returned = back.at[pl.ds(0, plane - 1), used]
    pltpu.make_async_copy(returned, returned, back_recv).wait()
    result = u_buf[...]
    for e in range(n_exp):
        rows_e = jnp.sum(back[pl.ds(e * n_seq, n_seq)].astype(F32), axis=0)
        slot = lax.broadcasted_iota(jnp.int32, rows_e.shape, 0)
        rows_e = jnp.where(slot < CAP, rows_e, 0.0).astype(BF16)
        lanes = slice(e * SLOTS, (e + 1) * SLOTS)
        result += jnp.dot(coarse[:, lanes], rows_e, preferred_element_type=F32)
        result += jnp.dot(fine[:, lanes], rows_e, preferred_element_type=F32)
    out_ref[...] = result.astype(BF16)
    pltpu.make_async_copy(returned, returned, back_send).wait()


def solution(mesh):
    n_seq, n_exp, n_rep = (mesh.shape[a] for a in ("seq", "exp", "rep"))

    def shards(
        queries,
        key_rows,
        value_rows,
        decay_log,
        residual,
        out_gate,
        attn_gain,
        moe_gain,
        routes,
        route_weights,
        w_gate,
        w_up,
        w_down,
    ):
        tokens, columns = queries.shape
        heads = decay_log.shape[1]
        hd = columns // heads
        _, whole_rows, width = w_gate.shape
        even = whole_rows % (16 * n_rep) == 0
        hidden_rows = whole_rows // n_rep if even else whole_rows
        plane = n_exp * n_seq
        slots = n_seq * SLOTS
        vmem = pl.BlockSpec(memory_space=pltpu.VMEM)
        hbm = pl.BlockSpec(memory_space=pltpu.HBM)
        dma = pltpu.SemaphoreType.DMA
        cut = hidden_rows // 256 * 128
        if 2 < n_seq <= SHORT and even and cut > 0:
            wide = columns + 128
            return pl.pallas_call(
                lambda *refs: direct_kernel(n_seq, n_exp, n_rep, *refs),
                name="layer",
                out_shape=pltpu.VMEM((tokens, columns), BF16),
                in_specs=[hbm] * 13,
                out_specs=vmem,
                scratch_shapes=[
                    pltpu.VMEM((tokens, columns), BF16),
                    pltpu.VMEM((tokens, columns), BF16),
                    pltpu.VMEM((heads, tokens), F32),
                    pltpu.VMEM((tokens, columns), BF16),
                    pltpu.VMEM((2, tokens), jnp.int32),
                    pltpu.VMEM((2, tokens), F32),
                    pltpu.VMEM((tokens, columns), BF16),
                    pltpu.VMEM((tokens, columns), BF16),
                    pltpu.VMEM((1, columns), F32),
                    pltpu.VMEM((1, columns), F32),
                    pltpu.VMEM((hidden_rows, width), BF16),
                    pltpu.VMEM((hidden_rows, width), BF16),
                    pltpu.VMEM((n_exp, whole_rows, columns), BF16),
                    pltpu.VMEM((heads, hd, hd), BF16),
                    pltpu.VMEM((heads, hd, hd), BF16),
                    pltpu.VMEM((heads, hd, hd), BF16),
                    pltpu.VMEM((heads, hd, hd), F32),
                    pltpu.VMEM((tokens, columns), BF16),
                    pltpu.VMEM((tokens, columns), F32),
                    pltpu.VMEM((tokens, columns), F32),
                    pltpu.VMEM((n_exp * n_rep, 8, tokens), F32),
                    pltpu.VMEM((n_exp * n_rep, n_exp * SLOTS, 128), F32),
                    pltpu.VMEM((1, 128), F32),
                    pltpu.VMEM((n_seq, 1, 128), F32),
                    pltpu.VMEM((n_exp, SLOTS, columns), BF16),
                    pltpu.VMEM((n_seq, n_exp, SLOTS, columns), BF16),
                    pltpu.VMEM((n_seq, n_exp, SLOTS, columns), BF16),
                    pltpu.VMEM((n_seq, n_exp, SLOTS, columns), BF16),
                    pltpu.VMEM((n_seq, n_exp, SLOTS, columns), BF16),
                    pltpu.VMEM((3, n_exp, SLOTS, columns), BF16),
                    pltpu.VMEM((3, n_exp, SLOTS, columns), BF16),
                    pltpu.VMEM((3, n_exp * SLOTS, columns), F32),
                    pltpu.VMEM((n_exp * SLOTS, columns), F32),
                    pltpu.VMEM((heads, 128), F32),
                    pltpu.VMEM((n_exp, SLOTS, columns), BF16),
                    pltpu.VMEM((n_rep, plane, SLOTS, columns), BF16),
                    pltpu.VMEM((2, n_exp, SLOTS, wide), BF16),
                    pltpu.VMEM((n_rep, plane, SLOTS, wide), BF16),
                    pltpu.VMEM((n_rep, slots, cut), BF16),
                    pltpu.VMEM((n_rep, slots, hidden_rows - cut), BF16),
                    pltpu.VMEM((plane, SLOTS, columns), BF16),
                    pltpu.VMEM((plane, SLOTS, columns), BF16),
                    dma((10,)),
                    dma((2 + n_exp,)),
                    pltpu.SemaphoreType.REGULAR,
                    dma((heads, PARTS)),
                    dma((heads, PARTS)),
                    dma,
                    dma,
                    dma,
                    dma,
                    dma((n_seq,)),
                    dma((n_seq,)),
                    dma((n_seq,)),
                    dma((n_seq,)),
                    dma((n_seq,)),
                    dma((2, n_seq)),
                    dma((3,)),
                    dma((3,)),
                    dma,
                    dma,
                    dma,
                    dma,
                    dma((2,)),
                    dma((2,)),
                    dma((2,)),
                    dma((2,)),
                    dma,
                    dma,
                ],
                compiler_params=pltpu.CompilerParams(
                    collective_id=0, has_side_effects=True, vmem_limit_bytes=63000000
                ),
            )(
                key_rows,
                value_rows,
                decay_log.T,
                queries,
                routes.T,
                route_weights.T,
                residual,
                out_gate,
                attn_gain.reshape(1, columns),
                moe_gain.reshape(1, columns),
                w_gate,
                w_up,
                w_down,
            )
        return pl.pallas_call(
            lambda *refs: chain_kernel(n_seq, n_exp, n_rep, *refs),
            name="layer",
            out_shape=pltpu.VMEM((tokens, columns), BF16),
            in_specs=[hbm] * 13,
            out_specs=vmem,
            scratch_shapes=[
                pltpu.VMEM((tokens, columns), BF16),
                pltpu.VMEM((tokens, columns), BF16),
                pltpu.VMEM((heads, tokens), F32),
                pltpu.VMEM((tokens, columns), BF16),
                pltpu.VMEM((2, tokens), jnp.int32),
                pltpu.VMEM((2, tokens), F32),
                pltpu.VMEM((tokens, columns), BF16),
                pltpu.VMEM((tokens, columns), BF16),
                pltpu.VMEM((1, columns), F32),
                pltpu.VMEM((1, columns), F32),
                pltpu.VMEM((hidden_rows, width), BF16),
                pltpu.VMEM((hidden_rows, width), BF16),
                pltpu.VMEM((hidden_rows, width), BF16),
                pltpu.VMEM((heads, hd, hd), BF16),
                pltpu.VMEM((heads, hd, hd), BF16),
                pltpu.VMEM((heads, hd, hd), F32),
                pltpu.VMEM((tokens, columns), F32),
                pltpu.VMEM((tokens, columns), F32),
                pltpu.VMEM((n_exp * n_rep, 8, tokens), F32),
                pltpu.VMEM((n_exp, SLOTS, columns), BF16),
                pltpu.VMEM((n_rep, plane, SLOTS, columns), BF16),
                pltpu.VMEM((n_exp, slots, columns), BF16),
                pltpu.VMEM((n_exp, slots, columns), BF16),
                pltpu.VMEM((plane, SLOTS, columns), BF16),
                pltpu.VMEM((plane, SLOTS, columns), BF16),
                dma((10,)),
                dma((3,)),
                pltpu.SemaphoreType.REGULAR,
                dma((heads, PARTS)),
                dma((heads, PARTS)),
                dma,
                dma,
                dma,
                dma,
                dma,
                dma,
                dma((n_exp,)),
                dma((n_exp,)),
                dma,
                dma,
            ],
            compiler_params=pltpu.CompilerParams(collective_id=0, has_side_effects=True, vmem_limit_bytes=63000000),
        )(
            key_rows,
            value_rows,
            decay_log.T,
            queries,
            routes.T,
            route_weights.T,
            residual,
            out_gate,
            attn_gain.reshape(1, columns),
            moe_gain.reshape(1, columns),
            w_gate,
            w_up,
            w_down,
        )

    block = P(("groups", "seq"), ("exp", "rep"))
    gain = P(("exp", "rep"))
    route = P(("groups", "seq"), None)
    weight = P("exp", "seq", None)
    return jax.shard_map(
        shards,
        mesh=mesh,
        in_specs=(block,) * 6 + (gain, gain, route, route) + (weight,) * 3,
        out_specs=block,
        check_vma=False,
    )
```

```python
import jax
import jax.numpy as jnp
from jax import lax
from jax.experimental import pallas as pl
from jax.experimental.pallas import tpu as pltpu
from jax.sharding import PartitionSpec as P

CAP = 6
SLOTS = 8
PARTS = 2
SHORT = 4
EPSILON = 1e-06
MESH = pl.DeviceIdType.MESH
F32 = jnp.float32
BF16 = jnp.bfloat16


def sweep(count, body):
    if count <= 16:
        for i in range(count):
            body(i)
    else:
        lax.fori_loop(0, count, lambda i, c: (body(i), c)[1], 0)


def nt_dot(a, b):
    return lax.dot_general(a, b, (((1,), (1,)), ((), ())), preferred_element_type=F32)


def chain_kernel(
    n_seq,
    n_exp,
    n_rep,
    k_hbm,
    v_hbm,
    decay_hbm,
    q_hbm,
    routes_hbm,
    rw_hbm,
    res_hbm,
    gate_hbm,
    again_hbm,
    mgain_hbm,
    wg_hbm,
    wu_hbm,
    wd_hbm,
    out_ref,
    k_ref,
    v_ref,
    decay_ref,
    q_ref,
    routes_ref,
    rw_ref,
    res_ref,
    gate_ref,
    again_ref,
    mgain_ref,
    wg,
    wu,
    wd,
    state_in,
    state_out,
    block_state,
    att,
    u_buf,
    sums,
    pack,
    rows,
    half_send,
    half_recv,
    fin,
    back,
    in_sem,
    w_sem,
    go_sem,
    chain_send,
    chain_recv,
    sums_send,
    sums_recv,
    disp_send,
    disp_recv,
    swap_send,
    swap_recv,
    half_ssem,
    half_rsem,
    back_send,
    back_recv,
):
    z = lax.axis_index("seq")
    x = lax.axis_index("exp")
    r = lax.axis_index("rep")
    other = 1 - r
    tokens, columns = q_ref.shape
    heads = decay_ref.shape[0]
    hd = columns // heads
    part_rows = hd // PARTS
    hidden_rows = wg.shape[0]
    width = columns * n_exp * n_rep
    whole_rows = wg_hbm.shape[1]

    inputs = [
        pltpu.make_async_copy(src, dst, in_sem.at[i])
        for i, (src, dst) in enumerate(
            (
                (k_hbm, k_ref),
                (v_hbm, v_ref),
                (decay_hbm, decay_ref),
                (q_hbm, q_ref),
                (routes_hbm, routes_ref),
                (rw_hbm, rw_ref),
                (res_hbm, res_ref),
                (gate_hbm, gate_ref),
                (again_hbm, again_ref),
                (mgain_hbm, mgain_ref),
            )
        )
    ]
    for load in inputs:
        load.start()
    first = pl.multiple_of(r * hidden_rows, 16) if hidden_rows != whole_rows else 0
    loads = [
        pltpu.make_async_copy(src.at[0, pl.ds(first, hidden_rows), :], dst, w_sem.at[i])
        for i, (src, dst) in enumerate(((wg_hbm, wg), (wu_hbm, wu), (wd_hbm, wd)))
    ]

    barrier = pltpu.get_barrier_semaphore()
    plane = n_exp * n_seq
    peers = n_exp * n_rep
    me = x * n_rep + r
    last = n_seq - 1

    def greet(where):
        pl.semaphore_signal(barrier, inc=1, device_id=where, device_id_type=MESH)

    @pl.when(z < last)
    def _():
        greet({"seq": z + 1})

    @pl.when(z > 0)
    def _():
        greet({"seq": z - 1})

    def greet_peer(i):
        to = lax.rem(me + 1 + i, peers)
        greet({"exp": lax.div(to, n_rep), "rep": lax.rem(to, n_rep)})

    sweep(peers - 1, greet_peer)
    for load in loads:
        load.start()
    for load in inputs[:3]:
        load.wait()

    ti = lax.broadcasted_iota(jnp.int32, (tokens, tokens), 0)
    tj = lax.broadcasted_iota(jnp.int32, (tokens, tokens), 1)
    causal = ti >= tj
    upper = jnp.where(tj >= ti, 1.0, 0.0).astype(F32)
    cum_t = jnp.dot(
        decay_ref[...], upper, precision=lax.Precision.HIGHEST, preferred_element_type=F32
    )
    cum = jnp.transpose(cum_t)
    ending = cum[tokens - 1 : tokens, :]
    fading = jnp.exp(ending)
    to_end = jnp.exp(ending - cum)
    lift = jnp.exp(cum)
    for h in range(heads):
        cols = slice(h * hd, (h + 1) * hd)
        faded = k_ref[:, cols].astype(F32) * to_end[:, h : h + 1]
        block_state[h] = jnp.dot(
            jnp.transpose(faded).astype(BF16), v_ref[:, cols], preferred_element_type=F32
        )

    ends = (z > 0).astype(jnp.int32) + (z < last).astype(jnp.int32)
    pl.semaphore_wait(barrier, peers - 1 + ends)

    def hop(h, p):
        piece = pl.ds(p * part_rows, part_rows)
        return pltpu.make_async_remote_copy(
            src_ref=state_out.at[h, piece],
            dst_ref=state_in.at[h, piece],
            send_sem=chain_send.at[h, p],
            recv_sem=chain_recv.at[h, p],
            device_id={"seq": z + 1},
            device_id_type=MESH,
        )

    @pl.when(z == 0)
    def _():
        for h in range(heads):
            state_out[h] = block_state[h].astype(BF16)
            for p in range(PARTS):
                hop(h, p).start()

    inputs[3].wait()

    for h in range(heads):
        cols = slice(h * hd, (h + 1) * hd)
        scores = nt_dot(q_ref[:, cols], k_ref[:, cols])
        gaps = cum[:, h : h + 1] - cum_t[h : h + 1, :]
        mixing = jnp.where(causal, scores * jnp.exp(jnp.where(causal, gaps, 0.0)), 0.0)
        att[:, cols] = jnp.dot(mixing.astype(BF16), v_ref[:, cols], preferred_element_type=F32)

    for load in inputs[4:]:
        load.wait()
    lane = lax.broadcasted_iota(jnp.int32, (tokens, 128), 1)
    expert_of = lax.div(lane, SLOTS)
    slot_of = lax.rem(lane, SLOTS)
    named = jnp.transpose(routes_ref[...].astype(F32)).astype(jnp.int32)
    shares = jnp.transpose(rw_ref[...])
    first_hit = named[:, 0:1] == expert_of
    second_hit = named[:, 1:2] == expert_of
    hit = jnp.where(first_hit | second_hit, 1.0, 0.0)
    strict = jnp.where(ti > tj, 1.0, 0.0).astype(BF16)
    before = jnp.dot(strict, hit.astype(BF16), preferred_element_type=F32)
    taken = (hit > 0.5) & (before.astype(jnp.int32) == slot_of) & (slot_of < CAP)
    onehot = jnp.where(taken, 1.0, 0.0)
    combine = jnp.where(first_hit, shares[:, 0:1], shares[:, 1:2]) * onehot
    dispatch = jnp.transpose(onehot)[0 : n_exp * SLOTS, :].astype(BF16)

    def let_go(i):
        pl.semaphore_signal(go_sem, inc=1, device_id={"seq": i}, device_id_type=MESH)

    for h in range(heads):
        cols = slice(h * hd, (h + 1) * hd)

        @pl.when(z > 0)
        def _():
            for p in range(PARTS):
                piece = slice(p * part_rows, (p + 1) * part_rows)
                hop(h, p).wait_recv()

                @pl.when(z < last)
                def _():
                    state_out[h, piece] = (
                        fading[:, h : h + 1] * state_in[h, piece].astype(F32)
                        + block_state[h, piece]
                    ).astype(BF16)
                    hop(h, p).start()

            lifted = (q_ref[:, cols].astype(F32) * lift[:, h : h + 1]).astype(BF16)
            att[:, cols] += jnp.dot(lifted, state_in[h], preferred_element_type=F32)

        if h == max(heads - 3, 0):

            @pl.when(z == last)
            def _():
                sweep(last, let_go)

    res = res_ref[...].astype(F32)
    attended = att[...]
    u = jax.nn.sigmoid(gate_ref[...].astype(F32)) * attended * again_ref[...]
    u_buf[...] = u
    parts = (attended * attended, res * u, u * u, res * res)
    table = jnp.zeros((tokens, 128), F32)
    for i, part in enumerate(parts):
        table = jnp.where(lane == i, jnp.sum(part, axis=1, keepdims=True), table)
    sums[me] = jnp.transpose(table)[0:8, :]

    def tell(i):
        to = lax.rem(me + 1 + i, peers)
        pltpu.make_async_remote_copy(
            src_ref=sums.at[me],
            dst_ref=sums.at[me],
            send_sem=sums_send,
            recv_sem=sums_recv,
            device_id={"exp": lax.div(to, n_rep), "rep": lax.rem(to, n_rep)},
            device_id_type=MESH,
        ).start()

    sweep(peers - 1, tell)
    many = sums.at[pl.ds(0, peers - 1)]
    pltpu.make_async_copy(many, many, sums_recv).wait()
    total = jnp.sum(sums[...], axis=0)
    s1 = lax.rsqrt(total[0:1, :] / width + EPSILON)
    moe = total[3:4, :] + s1 * (2.0 * total[1:2, :] + s1 * total[2:3, :])
    s2 = lax.rsqrt(jnp.maximum(moe, 0.0) / width + EPSILON)
    row8 = lax.broadcasted_iota(jnp.int32, (8, tokens), 0)
    scales = jnp.transpose(jnp.where(row8 == 0, s1, s2))
    hidden = res_ref[...].astype(F32) + scales[:, 0:1] * u_buf[...]
    u_buf[...] = hidden
    normed = (hidden * scales[:, 1:2] * mgain_ref[...]).astype(BF16)

    packed = jnp.dot(dispatch, normed, preferred_element_type=F32)
    for e in range(n_exp):
        pack[e] = packed[e * SLOTS : (e + 1) * SLOTS, :].astype(BF16)
    here = x * n_seq + z
    rows[r, here] = pack[x]

    def deal(e, to, source, target, send_sem, recv_sem):
        pltpu.make_async_remote_copy(
            src_ref=source,
            dst_ref=target,
            send_sem=send_sem,
            recv_sem=recv_sem,
            device_id={"exp": e, "seq": to},
            device_id_type=MESH,
        ).start()

    def deal_rows(e, to):
        used = pl.ds(0, CAP)
        deal(e, to, pack.at[e, used], rows.at[r, here, used], disp_send, disp_recv)

    def earlier(send):
        def one(i):
            @pl.when(i < z)
            def _():
                for e in range(n_exp):
                    send(e, i)

        sweep(n_seq, one)

    def level(send):
        for j in range(1, n_exp):
            send(lax.rem(x + j, n_exp), z)

    def later(send):
        def one(i):
            @pl.when(last - i > z)
            def _():
                for e in range(n_exp):
                    send(e, last - i)

        sweep(n_seq, one)

    earlier(deal_rows)
    level(deal_rows)

    @pl.when(z < last)
    def _():
        pl.semaphore_wait(go_sem, 1)

    later(deal_rows)
    arrived = rows.at[r, pl.ds(0, plane - 1), pl.ds(0, CAP)]
    pltpu.make_async_copy(arrived, arrived, disp_recv).wait()
    swap = pltpu.make_async_remote_copy(
        src_ref=rows.at[r],
        dst_ref=rows.at[r],
        send_sem=swap_send,
        recv_sem=swap_recv,
        device_id={"rep": other},
        device_id_type=MESH,
    )
    swap.start()
    for load in loads:
        load.wait()
    slots = n_seq * SLOTS

    def project(s):
        gate_part = up_part = 0.0
        for e in range(n_exp):
            chunk = rows[s, pl.ds(e * n_seq, n_seq)].astype(F32).reshape(slots, columns)
            chunk = chunk.astype(BF16)
            at = pl.ds(pl.multiple_of((e * n_rep + s) * columns, 128), columns)
            gate_part += nt_dot(wg[:, at], chunk)
            up_part += nt_dot(wu[:, at], chunk)
        return gate_part, up_part

    gate_val, up_val = project(r)
    swap.wait()
    gate_part, up_part = project(other)
    gate_val += gate_part
    up_val += up_part
    inner = gate_val / (1.0 + jnp.exp(-gate_val)) * up_val
    if hidden_rows == whole_rows:
        unit = lax.broadcasted_iota(jnp.int32, inner.shape, 0)
        inner = jnp.where(lax.div(unit, whole_rows // n_rep) == r, inner, 0.0)
    inner = jnp.transpose(inner).astype(BF16)

    def product(e, s):
        at = pl.multiple_of((e * n_rep + s) * columns, 128)
        return jnp.dot(inner, wd[:, pl.ds(at, columns)], preferred_element_type=F32)

    def half(e):
        return pltpu.make_async_remote_copy(
            src_ref=half_send.at[e],
            dst_ref=half_recv.at[e],
            send_sem=half_ssem.at[e],
            recv_sem=half_rsem.at[e],
            device_id={"rep": other},
            device_id_type=MESH,
        )

    for e in range(n_exp):
        half_send[e] = product(e, other).astype(BF16)
        half(e).start()

    here_back = x * n_seq + z
    for e in range(n_exp):
        own = product(e, r)
        half(e).wait_recv()
        whole = (own + half_recv[e].astype(F32)).reshape(n_seq, SLOTS, columns)
        fin[pl.ds(e * n_seq, n_seq)] = whole.astype(BF16)

    back[here_back] = fin[here_back]

    def hand_back(e, to):
        used = pl.ds(0, CAP)
        source = fin.at[e * n_seq + to, used]
        deal(e, to, source, back.at[here_back, used], back_send, back_recv)

    earlier(hand_back)
    later(hand_back)
    level(hand_back)
    returned = back.at[pl.ds(0, plane - 1), pl.ds(0, CAP)]
    pltpu.make_async_copy(returned, returned, back_recv).wait()
    coarse = combine.astype(BF16)
    fine = (combine - coarse.astype(F32)).astype(BF16)
    result = u_buf[...]
    for e in range(n_exp):
        rows_e = jnp.sum(back[pl.ds(e * n_seq, n_seq)].astype(F32), axis=0)
        slot = lax.broadcasted_iota(jnp.int32, rows_e.shape, 0)
        rows_e = jnp.where(slot < CAP, rows_e, 0.0).astype(BF16)
        lanes = slice(e * SLOTS, (e + 1) * SLOTS)
        result += jnp.dot(coarse[:, lanes], rows_e, preferred_element_type=F32)
        result += jnp.dot(fine[:, lanes], rows_e, preferred_element_type=F32)
    out_ref[...] = result.astype(BF16)

    for h in range(heads):

        @pl.when(z < last)
        def _():
            for p in range(PARTS):
                hop(h, p).wait_send()

    pltpu.make_async_copy(many, many, sums_send).wait()
    pltpu.make_async_copy(arrived, arrived, disp_send).wait()
    for e in range(n_exp):
        half(e).wait_send()
    pltpu.make_async_copy(returned, returned, back_send).wait()


def direct_kernel(
    n_seq,
    n_exp,
    n_rep,
    k_hbm,
    v_hbm,
    decay_hbm,
    q_hbm,
    routes_hbm,
    rw_hbm,
    res_hbm,
    gate_hbm,
    again_hbm,
    mgain_hbm,
    wg_hbm,
    wu_hbm,
    wd_hbm,
    out_ref,
    k_ref,
    v_ref,
    decay_ref,
    q_ref,
    routes_ref,
    rw_ref,
    res_ref,
    gate_ref,
    again_ref,
    mgain_ref,
    wg,
    wu,
    wd,
    state_in,
    state_out,
    own_state,
    block_state,
    lifted,
    att,
    u_buf,
    sums,
    first_sums,
    end_send,
    end_recv,
    q_send,
    q_recv,
    part_send,
    part_recv,
    tail_recv,
    extra_send,
    extra_recv,
    near,
    acc,
    fade,
    res_pack,
    res_rows,
    pack,
    rows,
    inner_head,
    inner_tail,
    fin,
    back,
    in_sem,
    w_sem,
    go_sem,
    chain_send,
    chain_recv,
    sums_send,
    sums_recv,
    first_ssem,
    first_rsem,
    q_ssem,
    q_rsem,
    end_ssem,
    end_rsem,
    part_ssem,
    part_rsem,
    extra_ssem,
    extra_rsem,
    res_ssem,
    res_rsem,
    disp_send,
    disp_recv,
    swap_send,
    swap_recv,
    inner_ssem,
    inner_rsem,
    back_send,
    back_recv,
):
    z = lax.axis_index("seq")
    x = lax.axis_index("exp")
    r = lax.axis_index("rep")
    other = 1 - r
    tokens, columns = q_ref.shape
    heads = decay_ref.shape[0]
    hd = columns // heads
    part_rows = hd // PARTS
    hidden_rows = wg.shape[0]
    width = columns * n_exp * n_rep
    cut = inner_head.shape[2]
    plane = n_exp * n_seq
    peers = n_exp * n_rep
    me = x * n_rep + r
    last = n_seq - 1
    middle = max(last - 1, 0)
    picked = n_exp * SLOTS
    used = pl.ds(0, CAP)
    here = x * n_seq + z

    def home(b):
        return b if b < last else middle

    inputs = {
        name: pltpu.make_async_copy(src, dst, in_sem.at[i])
        for i, (name, src, dst) in enumerate(
            (
                ("decay", decay_hbm, decay_ref),
                ("routes", routes_hbm, routes_ref),
                ("q", q_hbm, q_ref),
                ("k", k_hbm, k_ref),
                ("v", v_hbm, v_ref),
                ("res", res_hbm, res_ref),
                ("gate", gate_hbm, gate_ref),
                ("again", again_hbm, again_ref),
                ("mgain", mgain_hbm, mgain_ref),
                ("rw", rw_hbm, rw_ref),
            )
        )
    }
    for load in inputs.values():
        load.start()

    barrier = pltpu.get_barrier_semaphore()

    def greet(where):
        pl.semaphore_signal(barrier, inc=1, device_id=where, device_id_type=MESH)

    for i in range(n_seq):

        @pl.when((i != z) & ((i > 0) | (z == 1)))
        def _():
            greet({"seq": i})

    for i in range(peers - 1):
        to = lax.rem(me + 1 + i, peers)
        greet({"exp": lax.div(to, n_rep), "rep": lax.rem(to, n_rep)})

    first = pl.ds(pl.multiple_of(r * hidden_rows, 16), hidden_rows)
    loads = [
        pltpu.make_async_copy(src.at[0, first, :], dst, w_sem.at[i])
        for i, (src, dst) in enumerate(((wg_hbm, wg), (wu_hbm, wu)))
    ]
    for e in range(n_exp):
        at = pl.ds(pl.multiple_of((e * n_rep + r) * columns, 128), columns)
        loads.append(
            pltpu.make_async_copy(wd_hbm.at[0, :, at], wd.at[e], w_sem.at[len(loads)])
        )
    for load in loads:
        load.start()

    def remote(src, dst, send_sem, recv_sem, where):
        return pltpu.make_async_remote_copy(
            src_ref=src,
            dst_ref=dst,
            send_sem=send_sem,
            recv_sem=recv_sem,
            device_id=where,
            device_id_type=MESH,
        )

    inputs["decay"].wait()
    inputs["routes"].wait()
    ti = lax.broadcasted_iota(jnp.int32, (tokens, tokens), 0)
    tj = lax.broadcasted_iota(jnp.int32, (tokens, tokens), 1)
    causal = ti >= tj
    upper = jnp.where(tj >= ti, 1.0, 0.0).astype(F32)
    cum_t = jnp.dot(
        decay_ref[...], upper, precision=lax.Precision.HIGHEST, preferred_element_type=F32
    )
    cum = jnp.transpose(cum_t)
    ending = cum[tokens - 1 : tokens, :]
    fade[...] = jnp.broadcast_to(jnp.exp(cum_t[:, tokens - 1 : tokens]), fade.shape)
    to_end = jnp.exp(ending - cum)
    lift = jnp.exp(cum)
    end_send[...] = jnp.zeros(end_send.shape, F32)
    end_send[:, 0:heads] = ending
    lane = lax.broadcasted_iota(jnp.int32, (tokens, 128), 1)
    expert_of = lax.div(lane, SLOTS)
    slot_of = lax.rem(lane, SLOTS)
    named = jnp.transpose(routes_ref[...].astype(F32)).astype(jnp.int32)
    first_hit = named[:, 0:1] == expert_of
    second_hit = named[:, 1:2] == expert_of
    hit = jnp.where(first_hit | second_hit, 1.0, 0.0)
    strict = jnp.where(ti > tj, 1.0, 0.0).astype(BF16)
    before = jnp.dot(strict, hit.astype(BF16), preferred_element_type=F32)
    taken = (hit > 0.5) & (before.astype(jnp.int32) == slot_of) & (slot_of < CAP)
    onehot = jnp.where(taken, 1.0, 0.0)
    dispatch = jnp.transpose(onehot)[0:picked, :].astype(BF16)

    def pick(values):
        return jnp.dot(dispatch, values, preferred_element_type=F32)

    def put(ref, values):
        for e in range(n_exp):
            ref[e, :, 0:columns] = values[e * SLOTS : (e + 1) * SLOTS, :].astype(BF16)

    def take(ref):
        return ref[...].astype(F32)[:, :, 0:columns].reshape(picked, columns)

    inputs["q"].wait()
    for h in range(heads):
        cols = slice(h * hd, (h + 1) * hd)
        lifted[:, cols] = (q_ref[:, cols].astype(F32) * lift[:, h : h + 1]).astype(BF16)
    put(q_send, pick(lifted[...]))

    def keep_state():
        inputs["k"].wait()
        inputs["v"].wait()
        for h in range(heads):
            cols = slice(h * hd, (h + 1) * hd)
            faded = k_ref[:, cols].astype(F32) * to_end[:, h : h + 1]
            state = jnp.dot(
                jnp.transpose(faded).astype(BF16), v_ref[:, cols], preferred_element_type=F32
            )
            block_state[h] = state
            own_state[h] = state.astype(BF16)

    @pl.when(z < last - 1)
    def _():
        keep_state()

    pl.semaphore_wait(barrier, jnp.where(z == 0, 1, last) + peers - 1)

    def let_go():
        for i in range(1, n_exp):
            pl.semaphore_signal(
                go_sem,
                inc=1,
                device_id={"exp": lax.rem(x + i, n_exp)},
                device_id_type=MESH,
            )

    @pl.when(z > 0)
    def _():
        let_go()

    def ask(to):
        where = {"seq": to}
        return (
            remote(
                q_send.at[:, used], q_recv.at[z, :, used], q_ssem.at[to], q_rsem.at[z], where
            ),
            remote(end_send, end_recv.at[z], end_ssem.at[to], end_rsem.at[z], where),
        )

    def asks(which):
        for to in which:

            @pl.when(to < z)
            def _():
                for copy in ask(to):
                    copy.start()

    asks(range(1))

    @pl.when(z == last - 1)
    def _():
        keep_state()

    def hop(h, p, src):
        piece = pl.ds(p * part_rows, part_rows)
        return remote(
            src.at[h, piece],
            state_in.at[h, piece],
            chain_send.at[h, p],
            chain_recv.at[h, p],
            {"seq": z + 1},
        )

    def set_off(which):
        @pl.when((z == 0) & (z < last))
        def _():
            for h in which:
                for p in range(PARTS):
                    hop(h, p, own_state).start()

    quarter = heads // 4
    lead = heads - quarter
    set_off(range(lead))

    @pl.when(z == last)
    def _():
        inputs["k"].wait()
        inputs["v"].wait()

    asks(range(1, last))

    for h in range(heads):
        cols = slice(h * hd, (h + 1) * hd)
        scores = nt_dot(q_ref[:, cols], k_ref[:, cols])
        gaps = cum[:, h : h + 1] - cum_t[h : h + 1, :]
        mixing = jnp.where(causal, scores * jnp.exp(jnp.where(causal, gaps, 0.0)), 0.0)
        att[:, cols] = jnp.dot(mixing.astype(BF16), v_ref[:, cols], preferred_element_type=F32)

    for name in ("res", "gate", "again", "mgain", "rw"):
        inputs[name].wait()
    near_att = pick(att[...].astype(BF16))
    near_res = pick(res_ref[...])
    near_v = jax.nn.sigmoid(pick(gate_ref[...])) * again_ref[...]
    near[0] = near_att
    near[1] = near_v
    near[2] = near_res

    spot = lax.broadcasted_iota(jnp.int32, (picked, 128), 1)

    def peer_of(i):
        to = lax.rem(me + 1 + i, peers)
        return {"exp": lax.div(to, n_rep), "rep": lax.rem(to, n_rep)}

    def products(attended, gated, residual):
        u = gated * attended
        parts = (attended * attended, residual * u, u * u, residual * residual)
        return u, [jnp.sum(part, axis=1, keepdims=True) for part in parts]

    def first_tell(i):
        return remote(
            first_sums.at[me], first_sums.at[me], first_ssem, first_rsem, peer_of(i)
        )

    @pl.when(z == 0)
    def _():
        _, wholes = products(near_att, near_v, near_res)
        table = jnp.zeros((picked, 128), F32)
        for n, whole in enumerate(wholes):
            table = jnp.where(spot == n, whole, table)
        first_sums[me] = table
        for i in range(peers - 1):
            first_tell(i).start()

    def to_home(i):
        return remote(
            extra_send.at[i, :, used],
            extra_recv.at[i, :, used],
            extra_ssem.at[i],
            extra_rsem.at[i],
            {"seq": middle},
        )

    @pl.when(z > 0)
    def _():
        put(res_pack, near_res * mgain_ref[...])
        res_rows[r, here] = res_pack[x]

    if middle != last:

        @pl.when(z == last)
        def _():
            for i, value in enumerate((near_att, near_v, near_res)):
                put(extra_send.at[i], value)
                to_home(i).start()

    def own_line(send, order=None):
        for i in order or [n for k in range(n_seq) for n in (last - k, k)][:n_seq]:

            @pl.when(i != z)
            def _():
                send(x, i)

    def other_lines(send, order=None):
        for j in range(1, n_exp):
            for i in order or [n for k in range(n_seq) for n in (last - k, k)][:n_seq]:
                send(lax.rem(x + j, n_exp), i)

    def send_res(e, to):
        remote(
            res_pack.at[e, used],
            res_rows.at[r, here, used],
            res_ssem,
            res_rsem,
            {"exp": e, "seq": to},
        ).start()

    def keep(b, i):
        rows[r, x * n_seq + b] = pack[i, x]

    def spread(b, i):
        spot_of = x * n_seq + b

        def send(e, to):
            remote(
                pack.at[i, e, used],
                rows.at[r, spot_of, used],
                disp_send,
                disp_recv.at[b],
                {"exp": e, "seq": to},
            ).start()

        return send

    def hand_out(b, i, attended, gated, residual):
        u, wholes = products(attended, gated, residual)
        table = jnp.zeros((picked, 128), F32)
        for n, whole in enumerate(wholes):
            coarse = whole.astype(BF16).astype(F32)
            table = jnp.where(spot == n, coarse, table)
            table = jnp.where(spot == n + len(wholes), whole - coarse, table)
        put(pack.at[i], u * mgain_ref[...])
        for e in range(n_exp):
            pack[i, e, :, columns:] = table[e * SLOTS : (e + 1) * SLOTS, :].astype(BF16)
        keep(b, i)
        return spread(b, i)

    def norms(total):
        s1 = lax.rsqrt(total[0] / width + EPSILON)
        moe = total[3] + s1 * (2.0 * total[1] + s1 * total[2])
        return s1, lax.rsqrt(jnp.maximum(moe, 0.0) / width + EPSILON)

    def send_all_res():
        own_line(send_res)
        pl.semaphore_wait(go_sem, n_exp - 1)
        other_lines(send_res)

    @pl.when(z > 0)
    def _():
        send_all_res()

    def offer(b):
        target = tail_recv if b == last else part_recv
        return remote(
            part_send.at[b, :, used],
            target.at[z, :, used],
            part_ssem.at[b],
            part_rsem.at[1 if b == last else 0, z],
            {"seq": home(b)},
        )

    def relay(h):
        for p in range(PARTS):
            piece = slice(p * part_rows, (p + 1) * part_rows)
            hop(h, p, state_out).wait_recv()
            state_out[h, piece] = (
                fade[h : h + 1, :] * state_in[h, piece].astype(F32) + block_state[h, piece]
            ).astype(BF16)
            hop(h, p, state_out).start()

    def relays(where, which):
        @pl.when(where)
        def _():
            for h in which:
                relay(h)

    chained = (z > 0) & (z < last)
    for b in range(1, n_seq):

        @pl.when(z < b)
        def _():
            ask_q = remote(q_send.at[:, used], q_recv.at[b, :, used], q_ssem.at[0], q_rsem.at[b], {"seq": 0})
            ask_e = remote(end_send, end_recv.at[b], end_ssem.at[0], end_rsem.at[b], {"seq": 0})
            ask_q.wait_recv()
            ask_e.wait_recv()
            between = jnp.zeros((1, 128), F32)
            for m in range(1, b):
                between += jnp.where(m > z, end_recv[m], 0.0)
            between = jnp.exp(between)
            asked = take(q_recv.at[b]).astype(BF16)
            given = [
                jnp.dot(
                    asked[:, h * hd : (h + 1) * hd], own_state[h], preferred_element_type=F32
                )
                * between[:, h : h + 1]
                for h in range(heads)
            ]
            given = jnp.concatenate(given, axis=1)
            put(part_send.at[b], given)

            @pl.when(z != home(b))
            def _():
                offer(b).start()

            if b == last:

                @pl.when(z == home(b))
                def _():
                    put(tail_recv.at[z], given)

    @pl.when(z == 0)
    def _():
        let_go()

    relays(chained & (z == 1), range(quarter))

    @pl.when(z == 0)
    def _():
        everyone = first_sums.at[pl.ds(0, peers - 1)]
        pltpu.make_async_copy(everyone, everyone, first_rsem).wait()
        total = jnp.sum(first_sums[...], axis=0)
        s1, s2 = norms([total[:, n : n + 1] for n in range(4)])
        normed = (near[2] + s1 * (near[0] * near[1])) * s2 * mgain_ref[...]
        put(pack.at[0], normed)
        keep(0, 0)
        own_line(spread(0, 0))

    @pl.when(z == 0)
    def _():
        pl.semaphore_wait(go_sem, n_exp - 1)
        other_lines(spread(0, 0))

    set_off(range(lead, heads))

    def wait_part(which, source):
        buffer = tail_recv if which else part_recv
        remote(
            part_send.at[0, :, used],
            buffer.at[source, :, used],
            part_ssem.at[0],
            part_rsem.at[which, source],
            {"seq": 0},
        ).wait_recv()

    @pl.when((z > 0) & (z < last))
    def _():
        acc[...] = near[0]
        for source in range(last):

            @pl.when(source < z)
            def _():
                wait_part(0, source)
                acc[...] += take(part_recv.at[source])

        send = hand_out(z, 0, acc[...], near[1], near[2])
        own_line(send)
        other_lines(send)


    relays(chained & (z == 1), range(quarter, 2 * quarter))

    @pl.when(z == middle)
    def _():
        for i in range(3):
            to_home(i).wait_recv()
        whole = take(extra_recv.at[0])
        whole += take(tail_recv.at[middle])
        for source in range(last):
            if source != middle:
                wait_part(1, source)
                whole += take(tail_recv.at[source])
        send = hand_out(last, 1, whole, take(extra_recv.at[1]), take(extra_recv.at[2]))
        order = sorted(range(n_seq), key=lambda i: -abs(i - middle))
        own_line(send, order)
        other_lines(send, order)

    slots = n_seq * SLOTS

    def pair(s, e):
        return jnp.concatenate(
            [
                table[s, pl.ds(e * n_seq, n_seq)]
                .astype(F32)[:, :, 0:columns]
                .reshape(slots, columns)
                .astype(BF16)
                for table in (rows, res_rows)
            ],
            axis=0,
        )

    def project(s, lines):
        gate_part = up_part = 0.0
        for e in range(n_exp):
            chunk = pair(s, e)
            at = pl.ds(pl.multiple_of((e * n_rep + s) * columns, 128), columns)
            gate_part += nt_dot(wg[lines, at], chunk)
            up_part += nt_dot(wu[lines, at], chunk)
        return gate_part, up_part

    def swap(table, i):
        return remote(
            table.at[r], table.at[r], swap_send.at[i], swap_recv.at[i], {"rep": other}
        )

    res_sent = res_rows.at[r, pl.ds(0, plane - 1), used]
    for n in range(2):

        @pl.when(jnp.where(z > 0, 1, 0) == n)
        def _():
            arrived = res_rows.at[r, pl.ds(0, plane - n_exp - n), used]
            pltpu.make_async_copy(arrived, arrived, res_rsem).wait()

    swap(res_rows, 0).start()
    relays(chained & (z == 1), range(2 * quarter, heads))
    relays(chained & (z > 1), range(lead // 2))
    for load in loads:
        load.wait()

    mine = jnp.where(z < last, 1, 0) + jnp.where(z == middle, 1, 0)
    for b in range(n_seq):
        for own in range(2):

            @pl.when(jnp.where(z == home(b), 1, 0) == own)
            def _():
                if n_exp - own > 0:
                    arrived = rows.at[r, pl.ds(0, n_exp - own), used]
                    pltpu.make_async_copy(arrived, arrived, disp_recv.at[b]).wait()

    swap(rows, 1).start()
    gate_own, up_own = project(r, slice(0, hidden_rows))
    relays(chained & (z > 1), range(lead // 2, lead))
    swap(res_rows, 0).wait()
    swap(rows, 1).wait()
    table = 0.0
    for s in range(n_rep):
        for e in range(n_exp):
            table += rows[s, pl.ds(e * n_seq, n_seq)].astype(F32)[:, :, columns:]
    table = table.reshape(slots, 128)
    s1, s2 = norms([table[:, n : n + 1] + table[:, n + 4 : n + 5] for n in range(4)])
    whole = lax.broadcasted_iota(jnp.int32, (slots, 1), 0) < SLOTS

    def scaled(values):
        values = jnp.transpose(values)
        fresh = values[0:slots, :]
        return jnp.where(whole, fresh, s2 * (values[slots:, :] + s1 * fresh))

    def share(i):
        part = (inner_head, inner_tail)[i]
        return remote(
            part.at[r], part.at[r], inner_ssem.at[i], inner_rsem.at[i], {"rep": other}
        )

    for i, lines in enumerate((slice(0, cut), slice(cut, hidden_rows))):
        gate_part, up_part = project(other, lines)
        gate_val = scaled(gate_own[lines] + gate_part)
        up_val = scaled(up_own[lines] + up_part)
        inner = gate_val / (1.0 + jnp.exp(-gate_val)) * up_val
        (inner_head, inner_tail)[i][r] = inner.astype(BF16)
        share(i).start()

    relays(chained & (z > 1), range(lead, heads))

    def product(e, s, i):
        part = (inner_head, inner_tail)[i]
        lines = pl.ds(pl.multiple_of(s * hidden_rows + i * cut, 16), part.shape[2])
        return jnp.dot(part[s], wd[e, lines, :], preferred_element_type=F32)

    def hand_back(e, to):
        remote(
            fin.at[e * n_seq + to, used],
            back.at[here, used],
            back_send,
            back_recv,
            {"exp": e, "seq": to},
        ).start()

    turns = [lax.rem(x + j, n_exp) for j in range(1, n_exp + 1)]
    totals = [product(e, r, 0) + product(e, r, 1) for e in turns]
    share(0).wait_recv()
    totals = [total + product(e, other, 0) for total, e in zip(totals, turns)]
    share(1).wait_recv()
    for n, (total, e) in enumerate(zip(totals, turns)):
        whole = (total + product(e, other, 1)).reshape(n_seq, SLOTS, columns)
        fin[pl.ds(e * n_seq, n_seq)] = whole.astype(BF16)
        if n < n_exp - 1:
            for i in [n for k in range(n_seq) for n in (last - k, k)][:n_seq]:
                hand_back(e, i)

    back[here] = fin[here]
    own_line(hand_back)
    @pl.when(z == last)
    def _():
        for h in range(heads):
            for p in range(PARTS):
                hop(h, p, state_out).wait_recv()

    @pl.when(z > 0)
    def _():
        for h in range(heads):
            cols = slice(h * hd, (h + 1) * hd)
            att[:, cols] += jnp.dot(
                lifted[:, cols], state_in[h], preferred_element_type=F32
            )

    attended = att[...]
    square = jnp.sum(attended * attended, axis=1, keepdims=True)
    table = jnp.where(lane == 0, square, 0.0)
    sums[me] = jnp.transpose(table)[0:8, :]

    def tell(i):
        return remote(sums.at[me], sums.at[me], sums_send, sums_recv, peer_of(i))

    for i in range(peers - 1):
        tell(i).start()
    u_buf[...] = jax.nn.sigmoid(gate_ref[...].astype(F32)) * attended * again_ref[...]
    shares = jnp.transpose(rw_ref[...])
    combine = jnp.where(first_hit, shares[:, 0:1], shares[:, 1:2]) * onehot
    coarse = combine.astype(BF16)
    fine = (combine - coarse.astype(F32)).astype(BF16)

    for to in range(last):

        @pl.when(to < z)
        def _():
            for copy in ask(to):
                copy.wait_send()

    if middle != last:

        @pl.when(z == last)
        def _():
            for i in range(3):
                to_home(i).wait_send()

    for b in range(1, n_seq):

        @pl.when((z < b) & (z != home(b)))
        def _():
            offer(b).wait_send()

    @pl.when(z < last)
    def _():
        for h in range(heads):
            for p in range(PARTS):
                hop(h, p, state_out).wait_send()

    @pl.when(z > 0)
    def _():
        pltpu.make_async_copy(res_sent, res_sent, res_ssem).wait()

    @pl.when(z == 0)
    def _():
        everyone = first_sums.at[pl.ds(0, peers - 1)]
        pltpu.make_async_copy(everyone, everyone, first_ssem).wait()

    for n in range(1, 3):

        @pl.when(mine == n)
        def _():
            for _ in range(n):
                sent = rows.at[r, pl.ds(0, plane - 1), used]
                pltpu.make_async_copy(sent, sent, disp_send).wait()

    for i in range(2):
        share(i).wait_send()

    many = sums.at[pl.ds(0, peers - 1)]
    pltpu.make_async_copy(many, many, sums_recv).wait()
    total = jnp.sum(sums[...], axis=0)
    scale = lax.rsqrt(total / width + EPSILON)
    scale = jnp.transpose(scale)[:, 0:1]
    u_buf[...] = res_ref[...].astype(F32) + scale * u_buf[...]
    pltpu.make_async_copy(many, many, sums_send).wait()

    returned = back.at[pl.ds(0, plane - 1), used]
    pltpu.make_async_copy(returned, returned, back_recv).wait()
    result = u_buf[...]
    for e in range(n_exp):
        rows_e = jnp.sum(back[pl.ds(e * n_seq, n_seq)].astype(F32), axis=0)
        slot = lax.broadcasted_iota(jnp.int32, rows_e.shape, 0)
        rows_e = jnp.where(slot < CAP, rows_e, 0.0).astype(BF16)
        lanes = slice(e * SLOTS, (e + 1) * SLOTS)
        result += jnp.dot(coarse[:, lanes], rows_e, preferred_element_type=F32)
        result += jnp.dot(fine[:, lanes], rows_e, preferred_element_type=F32)
    out_ref[...] = result.astype(BF16)
    pltpu.make_async_copy(returned, returned, back_send).wait()


def solution(mesh):
    n_seq, n_exp, n_rep = (mesh.shape[a] for a in ("seq", "exp", "rep"))

    def shards(
        queries,
        key_rows,
        value_rows,
        decay_log,
        residual,
        out_gate,
        attn_gain,
        moe_gain,
        routes,
        route_weights,
        w_gate,
        w_up,
        w_down,
    ):
        tokens, columns = queries.shape
        heads = decay_log.shape[1]
        hd = columns // heads
        _, whole_rows, width = w_gate.shape
        even = whole_rows % (16 * n_rep) == 0
        hidden_rows = whole_rows // n_rep if even else whole_rows
        plane = n_exp * n_seq
        slots = n_seq * SLOTS
        vmem = pl.BlockSpec(memory_space=pltpu.VMEM)
        hbm = pl.BlockSpec(memory_space=pltpu.HBM)
        dma = pltpu.SemaphoreType.DMA
        cut = hidden_rows // 256 * 128
        if 2 < n_seq <= SHORT and even and cut > 0:
            wide = columns + 128
            return pl.pallas_call(
                lambda *refs: direct_kernel(n_seq, n_exp, n_rep, *refs),
                name="layer",
                out_shape=pltpu.VMEM((tokens, columns), BF16),
                in_specs=[hbm] * 13,
                out_specs=vmem,
                scratch_shapes=[
                    pltpu.VMEM((tokens, columns), BF16),
                    pltpu.VMEM((tokens, columns), BF16),
                    pltpu.VMEM((heads, tokens), F32),
                    pltpu.VMEM((tokens, columns), BF16),
                    pltpu.VMEM((2, tokens), jnp.int32),
                    pltpu.VMEM((2, tokens), F32),
                    pltpu.VMEM((tokens, columns), BF16),
                    pltpu.VMEM((tokens, columns), BF16),
                    pltpu.VMEM((1, columns), F32),
                    pltpu.VMEM((1, columns), F32),
                    pltpu.VMEM((hidden_rows, width), BF16),
                    pltpu.VMEM((hidden_rows, width), BF16),
                    pltpu.VMEM((n_exp, whole_rows, columns), BF16),
                    pltpu.VMEM((heads, hd, hd), BF16),
                    pltpu.VMEM((heads, hd, hd), BF16),
                    pltpu.VMEM((heads, hd, hd), BF16),
                    pltpu.VMEM((heads, hd, hd), F32),
                    pltpu.VMEM((tokens, columns), BF16),
                    pltpu.VMEM((tokens, columns), F32),
                    pltpu.VMEM((tokens, columns), F32),
                    pltpu.VMEM((n_exp * n_rep, 8, tokens), F32),
                    pltpu.VMEM((n_exp * n_rep, n_exp * SLOTS, 128), F32),
                    pltpu.VMEM((1, 128), F32),
                    pltpu.VMEM((n_seq, 1, 128), F32),
                    pltpu.VMEM((n_exp, SLOTS, columns), BF16),
                    pltpu.VMEM((n_seq, n_exp, SLOTS, columns), BF16),
                    pltpu.VMEM((n_seq, n_exp, SLOTS, columns), BF16),
                    pltpu.VMEM((n_seq, n_exp, SLOTS, columns), BF16),
                    pltpu.VMEM((n_seq, n_exp, SLOTS, columns), BF16),
                    pltpu.VMEM((3, n_exp, SLOTS, columns), BF16),
                    pltpu.VMEM((3, n_exp, SLOTS, columns), BF16),
                    pltpu.VMEM((3, n_exp * SLOTS, columns), F32),
                    pltpu.VMEM((n_exp * SLOTS, columns), F32),
                    pltpu.VMEM((heads, 128), F32),
                    pltpu.VMEM((n_exp, SLOTS, columns), BF16),
                    pltpu.VMEM((n_rep, plane, SLOTS, columns), BF16),
                    pltpu.VMEM((2, n_exp, SLOTS, wide), BF16),
                    pltpu.VMEM((n_rep, plane, SLOTS, wide), BF16),
                    pltpu.VMEM((n_rep, slots, cut), BF16),
                    pltpu.VMEM((n_rep, slots, hidden_rows - cut), BF16),
                    pltpu.VMEM((plane, SLOTS, columns), BF16),
                    pltpu.VMEM((plane, SLOTS, columns), BF16),
                    dma((10,)),
                    dma((2 + n_exp,)),
                    pltpu.SemaphoreType.REGULAR,
                    dma((heads, PARTS)),
                    dma((heads, PARTS)),
                    dma,
                    dma,
                    dma,
                    dma,
                    dma((n_seq,)),
                    dma((n_seq,)),
                    dma((n_seq,)),
                    dma((n_seq,)),
                    dma((n_seq,)),
                    dma((2, n_seq)),
                    dma((3,)),
                    dma((3,)),
                    dma,
                    dma,
                    dma,
                    dma((n_seq,)),
                    dma((2,)),
                    dma((2,)),
                    dma((2,)),
                    dma((2,)),
                    dma,
                    dma,
                ],
                compiler_params=pltpu.CompilerParams(
                    collective_id=0, has_side_effects=True, vmem_limit_bytes=63000000
                ),
            )(
                key_rows,
                value_rows,
                decay_log.T,
                queries,
                routes.T,
                route_weights.T,
                residual,
                out_gate,
                attn_gain.reshape(1, columns),
                moe_gain.reshape(1, columns),
                w_gate,
                w_up,
                w_down,
            )
        return pl.pallas_call(
            lambda *refs: chain_kernel(n_seq, n_exp, n_rep, *refs),
            name="layer",
            out_shape=pltpu.VMEM((tokens, columns), BF16),
            in_specs=[hbm] * 13,
            out_specs=vmem,
            scratch_shapes=[
                pltpu.VMEM((tokens, columns), BF16),
                pltpu.VMEM((tokens, columns), BF16),
                pltpu.VMEM((heads, tokens), F32),
                pltpu.VMEM((tokens, columns), BF16),
                pltpu.VMEM((2, tokens), jnp.int32),
                pltpu.VMEM((2, tokens), F32),
                pltpu.VMEM((tokens, columns), BF16),
                pltpu.VMEM((tokens, columns), BF16),
                pltpu.VMEM((1, columns), F32),
                pltpu.VMEM((1, columns), F32),
                pltpu.VMEM((hidden_rows, width), BF16),
                pltpu.VMEM((hidden_rows, width), BF16),
                pltpu.VMEM((hidden_rows, width), BF16),
                pltpu.VMEM((heads, hd, hd), BF16),
                pltpu.VMEM((heads, hd, hd), BF16),
                pltpu.VMEM((heads, hd, hd), F32),
                pltpu.VMEM((tokens, columns), F32),
                pltpu.VMEM((tokens, columns), F32),
                pltpu.VMEM((n_exp * n_rep, 8, tokens), F32),
                pltpu.VMEM((n_exp, SLOTS, columns), BF16),
                pltpu.VMEM((n_rep, plane, SLOTS, columns), BF16),
                pltpu.VMEM((n_exp, slots, columns), BF16),
                pltpu.VMEM((n_exp, slots, columns), BF16),
                pltpu.VMEM((plane, SLOTS, columns), BF16),
                pltpu.VMEM((plane, SLOTS, columns), BF16),
                dma((10,)),
                dma((3,)),
                pltpu.SemaphoreType.REGULAR,
                dma((heads, PARTS)),
                dma((heads, PARTS)),
                dma,
                dma,
                dma,
                dma,
                dma,
                dma,
                dma((n_exp,)),
                dma((n_exp,)),
                dma,
                dma,
            ],
            compiler_params=pltpu.CompilerParams(collective_id=0, has_side_effects=True, vmem_limit_bytes=63000000),
        )(
            key_rows,
            value_rows,
            decay_log.T,
            queries,
            routes.T,
            route_weights.T,
            residual,
            out_gate,
            attn_gain.reshape(1, columns),
            moe_gain.reshape(1, columns),
            w_gate,
            w_up,
            w_down,
        )

    block = P(("groups", "seq"), ("exp", "rep"))
    gain = P(("exp", "rep"))
    route = P(("groups", "seq"), None)
    weight = P("exp", "seq", None)
    return jax.shard_map(
        shards,
        mesh=mesh,
        in_specs=(block,) * 6 + (gain, gain, route, route) + (weight,) * 3,
        out_specs=block,
        check_vma=False,
    )
```

```python
import jax
import jax.numpy as jnp
from jax import lax
from jax.experimental import pallas as pl
from jax.experimental.pallas import tpu as pltpu
from jax.sharding import PartitionSpec as P

CAP = 6
SLOTS = 8
PARTS = 2
SHORT = 4
EPSILON = 1e-06
MESH = pl.DeviceIdType.MESH
F32 = jnp.float32
BF16 = jnp.bfloat16


def sweep(count, body):
    if count <= 16:
        for i in range(count):
            body(i)
    else:
        lax.fori_loop(0, count, lambda i, c: (body(i), c)[1], 0)


def nt_dot(a, b):
    return lax.dot_general(a, b, (((1,), (1,)), ((), ())), preferred_element_type=F32)


def chain_kernel(
    n_seq,
    n_exp,
    n_rep,
    k_hbm,
    v_hbm,
    decay_hbm,
    q_hbm,
    routes_hbm,
    rw_hbm,
    res_hbm,
    gate_hbm,
    again_hbm,
    mgain_hbm,
    wg_hbm,
    wu_hbm,
    wd_hbm,
    out_ref,
    k_ref,
    v_ref,
    decay_ref,
    q_ref,
    routes_ref,
    rw_ref,
    res_ref,
    gate_ref,
    again_ref,
    mgain_ref,
    wg,
    wu,
    wd,
    state_in,
    state_out,
    block_state,
    att,
    u_buf,
    sums,
    pack,
    rows,
    half_send,
    half_recv,
    fin,
    back,
    in_sem,
    w_sem,
    go_sem,
    chain_send,
    chain_recv,
    sums_send,
    sums_recv,
    disp_send,
    disp_recv,
    swap_send,
    swap_recv,
    half_ssem,
    half_rsem,
    back_send,
    back_recv,
):
    z = lax.axis_index("seq")
    x = lax.axis_index("exp")
    r = lax.axis_index("rep")
    other = 1 - r
    tokens, columns = q_ref.shape
    heads = decay_ref.shape[0]
    hd = columns // heads
    part_rows = hd // PARTS
    hidden_rows = wg.shape[0]
    width = columns * n_exp * n_rep
    whole_rows = wg_hbm.shape[1]

    inputs = [
        pltpu.make_async_copy(src, dst, in_sem.at[i])
        for i, (src, dst) in enumerate(
            (
                (k_hbm, k_ref),
                (v_hbm, v_ref),
                (decay_hbm, decay_ref),
                (q_hbm, q_ref),
                (routes_hbm, routes_ref),
                (rw_hbm, rw_ref),
                (res_hbm, res_ref),
                (gate_hbm, gate_ref),
                (again_hbm, again_ref),
                (mgain_hbm, mgain_ref),
            )
        )
    ]
    for load in inputs:
        load.start()
    first = pl.multiple_of(r * hidden_rows, 16) if hidden_rows != whole_rows else 0
    loads = [
        pltpu.make_async_copy(src.at[0, pl.ds(first, hidden_rows), :], dst, w_sem.at[i])
        for i, (src, dst) in enumerate(((wg_hbm, wg), (wu_hbm, wu), (wd_hbm, wd)))
    ]

    barrier = pltpu.get_barrier_semaphore()
    plane = n_exp * n_seq
    peers = n_exp * n_rep
    me = x * n_rep + r
    last = n_seq - 1

    def greet(where):
        pl.semaphore_signal(barrier, inc=1, device_id=where, device_id_type=MESH)

    @pl.when(z < last)
    def _():
        greet({"seq": z + 1})

    @pl.when(z > 0)
    def _():
        greet({"seq": z - 1})

    def greet_peer(i):
        to = lax.rem(me + 1 + i, peers)
        greet({"exp": lax.div(to, n_rep), "rep": lax.rem(to, n_rep)})

    sweep(peers - 1, greet_peer)
    for load in loads:
        load.start()
    for load in inputs[:3]:
        load.wait()

    ti = lax.broadcasted_iota(jnp.int32, (tokens, tokens), 0)
    tj = lax.broadcasted_iota(jnp.int32, (tokens, tokens), 1)
    causal = ti >= tj
    upper = jnp.where(tj >= ti, 1.0, 0.0).astype(F32)
    cum_t = jnp.dot(
        decay_ref[...], upper, precision=lax.Precision.HIGHEST, preferred_element_type=F32
    )
    cum = jnp.transpose(cum_t)
    ending = cum[tokens - 1 : tokens, :]
    fading = jnp.exp(ending)
    to_end = jnp.exp(ending - cum)
    lift = jnp.exp(cum)
    for h in range(heads):
        cols = slice(h * hd, (h + 1) * hd)
        faded = k_ref[:, cols].astype(F32) * to_end[:, h : h + 1]
        block_state[h] = jnp.dot(
            jnp.transpose(faded).astype(BF16), v_ref[:, cols], preferred_element_type=F32
        )

    ends = (z > 0).astype(jnp.int32) + (z < last).astype(jnp.int32)
    pl.semaphore_wait(barrier, peers - 1 + ends)

    def hop(h, p):
        piece = pl.ds(p * part_rows, part_rows)
        return pltpu.make_async_remote_copy(
            src_ref=state_out.at[h, piece],
            dst_ref=state_in.at[h, piece],
            send_sem=chain_send.at[h, p],
            recv_sem=chain_recv.at[h, p],
            device_id={"seq": z + 1},
            device_id_type=MESH,
        )

    @pl.when(z == 0)
    def _():
        for h in range(heads):
            state_out[h] = block_state[h].astype(BF16)
            for p in range(PARTS):
                hop(h, p).start()

    inputs[3].wait()

    for h in range(heads):
        cols = slice(h * hd, (h + 1) * hd)
        scores = nt_dot(q_ref[:, cols], k_ref[:, cols])
        gaps = cum[:, h : h + 1] - cum_t[h : h + 1, :]
        mixing = jnp.where(causal, scores * jnp.exp(jnp.where(causal, gaps, 0.0)), 0.0)
        att[:, cols] = jnp.dot(mixing.astype(BF16), v_ref[:, cols], preferred_element_type=F32)

    for load in inputs[4:]:
        load.wait()
    lane = lax.broadcasted_iota(jnp.int32, (tokens, 128), 1)
    expert_of = lax.div(lane, SLOTS)
    slot_of = lax.rem(lane, SLOTS)
    named = jnp.transpose(routes_ref[...].astype(F32)).astype(jnp.int32)
    shares = jnp.transpose(rw_ref[...])
    first_hit = named[:, 0:1] == expert_of
    second_hit = named[:, 1:2] == expert_of
    hit = jnp.where(first_hit | second_hit, 1.0, 0.0)
    strict = jnp.where(ti > tj, 1.0, 0.0).astype(BF16)
    before = jnp.dot(strict, hit.astype(BF16), preferred_element_type=F32)
    taken = (hit > 0.5) & (before.astype(jnp.int32) == slot_of) & (slot_of < CAP)
    onehot = jnp.where(taken, 1.0, 0.0)
    combine = jnp.where(first_hit, shares[:, 0:1], shares[:, 1:2]) * onehot
    dispatch = jnp.transpose(onehot)[0 : n_exp * SLOTS, :].astype(BF16)

    def let_go(i):
        pl.semaphore_signal(go_sem, inc=1, device_id={"seq": i}, device_id_type=MESH)

    for h in range(heads):
        cols = slice(h * hd, (h + 1) * hd)

        @pl.when(z > 0)
        def _():
            for p in range(PARTS):
                piece = slice(p * part_rows, (p + 1) * part_rows)
                hop(h, p).wait_recv()

                @pl.when(z < last)
                def _():
                    state_out[h, piece] = (
                        fading[:, h : h + 1] * state_in[h, piece].astype(F32)
                        + block_state[h, piece]
                    ).astype(BF16)
                    hop(h, p).start()

            lifted = (q_ref[:, cols].astype(F32) * lift[:, h : h + 1]).astype(BF16)
            att[:, cols] += jnp.dot(lifted, state_in[h], preferred_element_type=F32)

        if h == max(heads - 3, 0):

            @pl.when(z == last)
            def _():
                sweep(last, let_go)

    res = res_ref[...].astype(F32)
    attended = att[...]
    u = jax.nn.sigmoid(gate_ref[...].astype(F32)) * attended * again_ref[...]
    u_buf[...] = u
    parts = (attended * attended, res * u, u * u, res * res)
    table = jnp.zeros((tokens, 128), F32)
    for i, part in enumerate(parts):
        table = jnp.where(lane == i, jnp.sum(part, axis=1, keepdims=True), table)
    sums[me] = jnp.transpose(table)[0:8, :]

    def tell(i):
        to = lax.rem(me + 1 + i, peers)
        pltpu.make_async_remote_copy(
            src_ref=sums.at[me],
            dst_ref=sums.at[me],
            send_sem=sums_send,
            recv_sem=sums_recv,
            device_id={"exp": lax.div(to, n_rep), "rep": lax.rem(to, n_rep)},
            device_id_type=MESH,
        ).start()

    sweep(peers - 1, tell)
    many = sums.at[pl.ds(0, peers - 1)]
    pltpu.make_async_copy(many, many, sums_recv).wait()
    total = jnp.sum(sums[...], axis=0)
    s1 = lax.rsqrt(total[0:1, :] / width + EPSILON)
    moe = total[3:4, :] + s1 * (2.0 * total[1:2, :] + s1 * total[2:3, :])
    s2 = lax.rsqrt(jnp.maximum(moe, 0.0) / width + EPSILON)
    row8 = lax.broadcasted_iota(jnp.int32, (8, tokens), 0)
    scales = jnp.transpose(jnp.where(row8 == 0, s1, s2))
    hidden = res_ref[...].astype(F32) + scales[:, 0:1] * u_buf[...]
    u_buf[...] = hidden
    normed = (hidden * scales[:, 1:2] * mgain_ref[...]).astype(BF16)

    packed = jnp.dot(dispatch, normed, preferred_element_type=F32)
    for e in range(n_exp):
        pack[e] = packed[e * SLOTS : (e + 1) * SLOTS, :].astype(BF16)
    here = x * n_seq + z
    rows[r, here] = pack[x]

    def deal(e, to, source, target, send_sem, recv_sem):
        pltpu.make_async_remote_copy(
            src_ref=source,
            dst_ref=target,
            send_sem=send_sem,
            recv_sem=recv_sem,
            device_id={"exp": e, "seq": to},
            device_id_type=MESH,
        ).start()

    def deal_rows(e, to):
        used = pl.ds(0, CAP)
        deal(e, to, pack.at[e, used], rows.at[r, here, used], disp_send, disp_recv)

    def earlier(send):
        def one(i):
            @pl.when(i < z)
            def _():
                for e in range(n_exp):
                    send(e, i)

        sweep(n_seq, one)

    def level(send):
        for j in range(1, n_exp):
            send(lax.rem(x + j, n_exp), z)

    def later(send):
        def one(i):
            @pl.when(last - i > z)
            def _():
                for e in range(n_exp):
                    send(e, last - i)

        sweep(n_seq, one)

    earlier(deal_rows)
    level(deal_rows)

    @pl.when(z < last)
    def _():
        pl.semaphore_wait(go_sem, 1)

    later(deal_rows)
    arrived = rows.at[r, pl.ds(0, plane - 1), pl.ds(0, CAP)]
    pltpu.make_async_copy(arrived, arrived, disp_recv).wait()
    swap = pltpu.make_async_remote_copy(
        src_ref=rows.at[r],
        dst_ref=rows.at[r],
        send_sem=swap_send,
        recv_sem=swap_recv,
        device_id={"rep": other},
        device_id_type=MESH,
    )
    swap.start()
    for load in loads:
        load.wait()
    slots = n_seq * SLOTS

    def project(s):
        gate_part = up_part = 0.0
        for e in range(n_exp):
            chunk = rows[s, pl.ds(e * n_seq, n_seq)].astype(F32).reshape(slots, columns)
            chunk = chunk.astype(BF16)
            at = pl.ds(pl.multiple_of((e * n_rep + s) * columns, 128), columns)
            gate_part += nt_dot(wg[:, at], chunk)
            up_part += nt_dot(wu[:, at], chunk)
        return gate_part, up_part

    gate_val, up_val = project(r)
    swap.wait()
    gate_part, up_part = project(other)
    gate_val += gate_part
    up_val += up_part
    inner = gate_val / (1.0 + jnp.exp(-gate_val)) * up_val
    if hidden_rows == whole_rows:
        unit = lax.broadcasted_iota(jnp.int32, inner.shape, 0)
        inner = jnp.where(lax.div(unit, whole_rows // n_rep) == r, inner, 0.0)
    inner = jnp.transpose(inner).astype(BF16)

    def product(e, s):
        at = pl.multiple_of((e * n_rep + s) * columns, 128)
        return jnp.dot(inner, wd[:, pl.ds(at, columns)], preferred_element_type=F32)

    def half(e):
        return pltpu.make_async_remote_copy(
            src_ref=half_send.at[e],
            dst_ref=half_recv.at[e],
            send_sem=half_ssem.at[e],
            recv_sem=half_rsem.at[e],
            device_id={"rep": other},
            device_id_type=MESH,
        )

    for e in range(n_exp):
        half_send[e] = product(e, other).astype(BF16)
        half(e).start()

    here_back = x * n_seq + z
    for e in range(n_exp):
        own = product(e, r)
        half(e).wait_recv()
        whole = (own + half_recv[e].astype(F32)).reshape(n_seq, SLOTS, columns)
        fin[pl.ds(e * n_seq, n_seq)] = whole.astype(BF16)

    back[here_back] = fin[here_back]

    def hand_back(e, to):
        used = pl.ds(0, CAP)
        source = fin.at[e * n_seq + to, used]
        deal(e, to, source, back.at[here_back, used], back_send, back_recv)

    earlier(hand_back)
    later(hand_back)
    level(hand_back)
    returned = back.at[pl.ds(0, plane - 1), pl.ds(0, CAP)]
    pltpu.make_async_copy(returned, returned, back_recv).wait()
    coarse = combine.astype(BF16)
    fine = (combine - coarse.astype(F32)).astype(BF16)
    result = u_buf[...]
    for e in range(n_exp):
        rows_e = jnp.sum(back[pl.ds(e * n_seq, n_seq)].astype(F32), axis=0)
        slot = lax.broadcasted_iota(jnp.int32, rows_e.shape, 0)
        rows_e = jnp.where(slot < CAP, rows_e, 0.0).astype(BF16)
        lanes = slice(e * SLOTS, (e + 1) * SLOTS)
        result += jnp.dot(coarse[:, lanes], rows_e, preferred_element_type=F32)
        result += jnp.dot(fine[:, lanes], rows_e, preferred_element_type=F32)
    out_ref[...] = result.astype(BF16)

    for h in range(heads):

        @pl.when(z < last)
        def _():
            for p in range(PARTS):
                hop(h, p).wait_send()

    pltpu.make_async_copy(many, many, sums_send).wait()
    pltpu.make_async_copy(arrived, arrived, disp_send).wait()
    for e in range(n_exp):
        half(e).wait_send()
    pltpu.make_async_copy(returned, returned, back_send).wait()


def direct_kernel(
    n_seq,
    n_exp,
    n_rep,
    k_hbm,
    v_hbm,
    decay_hbm,
    q_hbm,
    routes_hbm,
    rw_hbm,
    res_hbm,
    gate_hbm,
    again_hbm,
    mgain_hbm,
    wg_hbm,
    wu_hbm,
    wd_hbm,
    out_ref,
    k_ref,
    v_ref,
    decay_ref,
    q_ref,
    routes_ref,
    rw_ref,
    res_ref,
    gate_ref,
    again_ref,
    mgain_ref,
    wg,
    wu,
    wd,
    state_in,
    state_out,
    own_state,
    block_state,
    lifted,
    att,
    u_buf,
    sums,
    first_sums,
    end_send,
    end_recv,
    q_send,
    q_recv,
    part_send,
    part_recv,
    tail_recv,
    extra_send,
    extra_recv,
    near,
    acc,
    fade,
    res_pack,
    res_rows,
    pack,
    rows,
    inner_head,
    inner_tail,
    fin,
    back,
    in_sem,
    w_sem,
    go_sem,
    chain_send,
    chain_recv,
    sums_send,
    sums_recv,
    first_ssem,
    first_rsem,
    q_ssem,
    q_rsem,
    end_ssem,
    end_rsem,
    part_ssem,
    part_rsem,
    extra_ssem,
    extra_rsem,
    res_ssem,
    res_rsem,
    disp_send,
    disp_recv,
    swap_send,
    swap_recv,
    inner_ssem,
    inner_rsem,
    back_send,
    back_recv,
):
    z = lax.axis_index("seq")
    x = lax.axis_index("exp")
    r = lax.axis_index("rep")
    other = 1 - r
    tokens, columns = q_ref.shape
    heads = decay_ref.shape[0]
    hd = columns // heads
    part_rows = hd // PARTS
    hidden_rows = wg.shape[0]
    width = columns * n_exp * n_rep
    cut = inner_head.shape[2]
    plane = n_exp * n_seq
    peers = n_exp * n_rep
    me = x * n_rep + r
    last = n_seq - 1
    middle = max(last - 1, 0)
    picked = n_exp * SLOTS
    used = pl.ds(0, CAP)
    here = x * n_seq + z

    def home(b):
        return b if b < last else middle

    inputs = {
        name: pltpu.make_async_copy(src, dst, in_sem.at[i])
        for i, (name, src, dst) in enumerate(
            (
                ("decay", decay_hbm, decay_ref),
                ("routes", routes_hbm, routes_ref),
                ("q", q_hbm, q_ref),
                ("k", k_hbm, k_ref),
                ("v", v_hbm, v_ref),
                ("res", res_hbm, res_ref),
                ("gate", gate_hbm, gate_ref),
                ("again", again_hbm, again_ref),
                ("mgain", mgain_hbm, mgain_ref),
                ("rw", rw_hbm, rw_ref),
            )
        )
    }
    for load in inputs.values():
        load.start()

    barrier = pltpu.get_barrier_semaphore()

    def greet(where):
        pl.semaphore_signal(barrier, inc=1, device_id=where, device_id_type=MESH)

    for i in range(n_seq):

        @pl.when((i != z) & ((i > 0) | (z == 1)))
        def _():
            greet({"seq": i})

    for i in range(peers - 1):
        to = lax.rem(me + 1 + i, peers)
        greet({"exp": lax.div(to, n_rep), "rep": lax.rem(to, n_rep)})

    first = pl.ds(pl.multiple_of(r * hidden_rows, 16), hidden_rows)
    loads = [
        pltpu.make_async_copy(src.at[0, first, :], dst, w_sem.at[i])
        for i, (src, dst) in enumerate(((wg_hbm, wg), (wu_hbm, wu)))
    ]
    for e in range(n_exp):
        at = pl.ds(pl.multiple_of((e * n_rep + r) * columns, 128), columns)
        loads.append(
            pltpu.make_async_copy(wd_hbm.at[0, :, at], wd.at[e], w_sem.at[len(loads)])
        )
    for load in loads:
        load.start()

    def remote(src, dst, send_sem, recv_sem, where):
        return pltpu.make_async_remote_copy(
            src_ref=src,
            dst_ref=dst,
            send_sem=send_sem,
            recv_sem=recv_sem,
            device_id=where,
            device_id_type=MESH,
        )

    inputs["decay"].wait()
    inputs["routes"].wait()
    ti = lax.broadcasted_iota(jnp.int32, (tokens, tokens), 0)
    tj = lax.broadcasted_iota(jnp.int32, (tokens, tokens), 1)
    causal = ti >= tj
    upper = jnp.where(tj >= ti, 1.0, 0.0).astype(F32)
    cum_t = jnp.dot(
        decay_ref[...], upper, precision=lax.Precision.HIGHEST, preferred_element_type=F32
    )
    cum = jnp.transpose(cum_t)
    ending = cum[tokens - 1 : tokens, :]
    fade[...] = jnp.broadcast_to(jnp.exp(cum_t[:, tokens - 1 : tokens]), fade.shape)
    to_end = jnp.exp(ending - cum)
    lift = jnp.exp(cum)
    end_send[...] = jnp.zeros(end_send.shape, F32)
    end_send[:, 0:heads] = ending
    lane = lax.broadcasted_iota(jnp.int32, (tokens, 128), 1)
    expert_of = lax.div(lane, SLOTS)
    slot_of = lax.rem(lane, SLOTS)
    named = jnp.transpose(routes_ref[...].astype(F32)).astype(jnp.int32)
    first_hit = named[:, 0:1] == expert_of
    second_hit = named[:, 1:2] == expert_of
    hit = jnp.where(first_hit | second_hit, 1.0, 0.0)
    strict = jnp.where(ti > tj, 1.0, 0.0).astype(BF16)
    before = jnp.dot(strict, hit.astype(BF16), preferred_element_type=F32)
    taken = (hit > 0.5) & (before.astype(jnp.int32) == slot_of) & (slot_of < CAP)
    onehot = jnp.where(taken, 1.0, 0.0)
    dispatch = jnp.transpose(onehot)[0:picked, :].astype(BF16)

    def pick(values):
        return jnp.dot(dispatch, values, preferred_element_type=F32)

    def put(ref, values):
        for e in range(n_exp):
            ref[e, :, 0:columns] = values[e * SLOTS : (e + 1) * SLOTS, :].astype(BF16)

    def take(ref):
        return ref[...].astype(F32)[:, :, 0:columns].reshape(picked, columns)

    inputs["q"].wait()
    for h in range(heads):
        cols = slice(h * hd, (h + 1) * hd)
        lifted[:, cols] = (q_ref[:, cols].astype(F32) * lift[:, h : h + 1]).astype(BF16)
    put(q_send, pick(lifted[...]))

    def keep_state():
        inputs["k"].wait()
        inputs["v"].wait()
        for h in range(heads):
            cols = slice(h * hd, (h + 1) * hd)
            faded = k_ref[:, cols].astype(F32) * to_end[:, h : h + 1]
            state = jnp.dot(
                jnp.transpose(faded).astype(BF16), v_ref[:, cols], preferred_element_type=F32
            )
            block_state[h] = state
            own_state[h] = state.astype(BF16)

    @pl.when(z < last - 1)
    def _():
        keep_state()

    pl.semaphore_wait(barrier, jnp.where(z == 0, 1, last) + peers - 1)

    def let_go():
        for i in range(1, n_exp):
            pl.semaphore_signal(
                go_sem,
                inc=1,
                device_id={"exp": lax.rem(x + i, n_exp)},
                device_id_type=MESH,
            )

    @pl.when(z > 0)
    def _():
        let_go()

    def ask(to):
        where = {"seq": to}
        return (
            remote(
                q_send.at[:, used], q_recv.at[z, :, used], q_ssem.at[to], q_rsem.at[z], where
            ),
            remote(end_send, end_recv.at[z], end_ssem.at[to], end_rsem.at[z], where),
        )

    def asks(which):
        for to in which:

            @pl.when(to < z)
            def _():
                for copy in ask(to):
                    copy.start()

    asks(range(1))

    @pl.when(z == last - 1)
    def _():
        keep_state()

    def hop(h, p, src):
        piece = pl.ds(p * part_rows, part_rows)
        return remote(
            src.at[h, piece],
            state_in.at[h, piece],
            chain_send.at[h, p],
            chain_recv.at[h, p],
            {"seq": z + 1},
        )

    def set_off(which):
        @pl.when((z == 0) & (z < last))
        def _():
            for h in which:
                for p in range(PARTS):
                    hop(h, p, own_state).start()

    quarter = heads // 4
    lead = heads - quarter
    set_off(range(lead))

    @pl.when(z == last)
    def _():
        inputs["k"].wait()
        inputs["v"].wait()

    asks(range(1, last))

    for h in range(heads):
        cols = slice(h * hd, (h + 1) * hd)
        scores = nt_dot(q_ref[:, cols], k_ref[:, cols])
        gaps = cum[:, h : h + 1] - cum_t[h : h + 1, :]
        mixing = jnp.where(causal, scores * jnp.exp(jnp.where(causal, gaps, 0.0)), 0.0)
        att[:, cols] = jnp.dot(mixing.astype(BF16), v_ref[:, cols], preferred_element_type=F32)

    for name in ("res", "gate", "again", "mgain", "rw"):
        inputs[name].wait()
    near_att = pick(att[...].astype(BF16))
    near_res = pick(res_ref[...])
    near_v = jax.nn.sigmoid(pick(gate_ref[...])) * again_ref[...]
    near[0] = near_att
    near[1] = near_v
    near[2] = near_res

    spot = lax.broadcasted_iota(jnp.int32, (picked, 128), 1)

    def peer_of(i):
        to = lax.rem(me + 1 + i, peers)
        return {"exp": lax.div(to, n_rep), "rep": lax.rem(to, n_rep)}

    def products(attended, gated, residual):
        u = gated * attended
        parts = (attended * attended, residual * u, u * u, residual * residual)
        return u, [jnp.sum(part, axis=1, keepdims=True) for part in parts]

    def first_tell(i):
        return remote(
            first_sums.at[me], first_sums.at[me], first_ssem, first_rsem, peer_of(i)
        )

    @pl.when(z == 0)
    def _():
        _, wholes = products(near_att, near_v, near_res)
        table = jnp.zeros((picked, 128), F32)
        for n, whole in enumerate(wholes):
            table = jnp.where(spot == n, whole, table)
        first_sums[me] = table
        for i in range(peers - 1):
            first_tell(i).start()

    def to_home(i):
        return remote(
            extra_send.at[i, :, used],
            extra_recv.at[i, :, used],
            extra_ssem.at[i],
            extra_rsem.at[i],
            {"seq": middle},
        )

    @pl.when(z > 0)
    def _():
        put(res_pack, near_res * mgain_ref[...])
        res_rows[r, here] = res_pack[x]

    if middle != last:

        @pl.when(z == last)
        def _():
            for i, value in enumerate((near_att, near_v, near_res)):
                put(extra_send.at[i], value)
                to_home(i).start()

    def own_line(send, order=None):
        for i in order or [n for k in range(n_seq) for n in (last - k, k)][:n_seq]:

            @pl.when(i != z)
            def _():
                send(x, i)

    def other_lines(send, order=None):
        for j in range(1, n_exp):
            for i in order or [n for k in range(n_seq) for n in (last - k, k)][:n_seq]:
                send(lax.rem(x + j, n_exp), i)

    def send_res(e, to):
        remote(
            res_pack.at[e, used],
            res_rows.at[r, here, used],
            res_ssem,
            res_rsem,
            {"exp": e, "seq": to},
        ).start()

    def keep(b, i):
        rows[r, x * n_seq + b] = pack[i, x]

    def spread(b, i):
        spot_of = x * n_seq + b

        def send(e, to):
            remote(
                pack.at[i, e, used],
                rows.at[r, spot_of, used],
                disp_send,
                disp_recv.at[b],
                {"exp": e, "seq": to},
            ).start()

        return send

    def hand_out(b, i, attended, gated, residual):
        u, wholes = products(attended, gated, residual)
        table = jnp.zeros((picked, 128), F32)
        for n, whole in enumerate(wholes):
            coarse = whole.astype(BF16).astype(F32)
            table = jnp.where(spot == n, coarse, table)
            table = jnp.where(spot == n + len(wholes), whole - coarse, table)
        put(pack.at[i], u * mgain_ref[...])
        for e in range(n_exp):
            pack[i, e, :, columns:] = table[e * SLOTS : (e + 1) * SLOTS, :].astype(BF16)
        keep(b, i)
        return spread(b, i)

    def norms(total):
        s1 = lax.rsqrt(total[0] / width + EPSILON)
        moe = total[3] + s1 * (2.0 * total[1] + s1 * total[2])
        return s1, lax.rsqrt(jnp.maximum(moe, 0.0) / width + EPSILON)

    def send_all_res():
        own_line(send_res)
        pl.semaphore_wait(go_sem, n_exp - 1)
        other_lines(send_res)

    @pl.when(z > 0)
    def _():
        send_all_res()

    def offer(b):
        target = tail_recv if b == last else part_recv
        return remote(
            part_send.at[b, :, used],
            target.at[z, :, used],
            part_ssem.at[b],
            part_rsem.at[1 if b == last else 0, z],
            {"seq": home(b)},
        )

    def relay(h):
        for p in range(PARTS):
            piece = slice(p * part_rows, (p + 1) * part_rows)
            hop(h, p, state_out).wait_recv()
            state_out[h, piece] = (
                fade[h : h + 1, :] * state_in[h, piece].astype(F32) + block_state[h, piece]
            ).astype(BF16)
            hop(h, p, state_out).start()

    def relays(where, which):
        @pl.when(where)
        def _():
            for h in which:
                relay(h)

    chained = (z > 0) & (z < last)
    for b in range(1, n_seq):

        @pl.when(z < b)
        def _():
            ask_q = remote(q_send.at[:, used], q_recv.at[b, :, used], q_ssem.at[0], q_rsem.at[b], {"seq": 0})
            ask_e = remote(end_send, end_recv.at[b], end_ssem.at[0], end_rsem.at[b], {"seq": 0})
            ask_q.wait_recv()
            ask_e.wait_recv()
            between = jnp.zeros((1, 128), F32)
            for m in range(1, b):
                between += jnp.where(m > z, end_recv[m], 0.0)
            between = jnp.exp(between)
            asked = take(q_recv.at[b]).astype(BF16)
            given = [
                jnp.dot(
                    asked[:, h * hd : (h + 1) * hd], own_state[h], preferred_element_type=F32
                )
                * between[:, h : h + 1]
                for h in range(heads)
            ]
            given = jnp.concatenate(given, axis=1)
            put(part_send.at[b], given)

            @pl.when(z != home(b))
            def _():
                offer(b).start()

            if b == last:

                @pl.when(z == home(b))
                def _():
                    put(tail_recv.at[z], given)

    @pl.when(z == 0)
    def _():
        let_go()

    relays(chained & (z == 1), range(quarter))

    @pl.when(z == 0)
    def _():
        everyone = first_sums.at[pl.ds(0, peers - 1)]
        pltpu.make_async_copy(everyone, everyone, first_rsem).wait()
        total = jnp.sum(first_sums[...], axis=0)
        s1, s2 = norms([total[:, n : n + 1] for n in range(4)])
        normed = (near[2] + s1 * (near[0] * near[1])) * s2 * mgain_ref[...]
        put(pack.at[0], normed)
        keep(0, 0)
        own_line(spread(0, 0))

    @pl.when(z == 0)
    def _():
        pl.semaphore_wait(go_sem, n_exp - 1)
        other_lines(spread(0, 0))

    set_off(range(lead, heads))

    def wait_part(which, source):
        buffer = tail_recv if which else part_recv
        remote(
            part_send.at[0, :, used],
            buffer.at[source, :, used],
            part_ssem.at[0],
            part_rsem.at[which, source],
            {"seq": 0},
        ).wait_recv()

    @pl.when((z > 0) & (z < last))
    def _():
        acc[...] = near[0]
        for source in range(last):

            @pl.when(source < z)
            def _():
                wait_part(0, source)
                acc[...] += take(part_recv.at[source])

        send = hand_out(z, 0, acc[...], near[1], near[2])
        own_line(send)
        other_lines(send)


    relays(chained & (z == 1), range(quarter, 2 * quarter))

    @pl.when(z == middle)
    def _():
        for i in range(3):
            to_home(i).wait_recv()
        whole = take(extra_recv.at[0])
        whole += take(tail_recv.at[middle])
        for source in range(last):
            if source != middle:
                wait_part(1, source)
                whole += take(tail_recv.at[source])
        send = hand_out(last, 1, whole, take(extra_recv.at[1]), take(extra_recv.at[2]))
        order = sorted(range(n_seq), key=lambda i: -abs(i - middle))
        own_line(send, order)
        other_lines(send, order)

    slots = n_seq * SLOTS

    def pair(s, e):
        return jnp.concatenate(
            [
                table[s, pl.ds(e * n_seq, n_seq)]
                .astype(F32)[:, :, 0:columns]
                .reshape(slots, columns)
                .astype(BF16)
                for table in (rows, res_rows)
            ],
            axis=0,
        )

    def project(s, lines):
        gate_part = up_part = 0.0
        for e in range(n_exp):
            chunk = pair(s, e)
            at = pl.ds(pl.multiple_of((e * n_rep + s) * columns, 128), columns)
            gate_part += nt_dot(wg[lines, at], chunk)
            up_part += nt_dot(wu[lines, at], chunk)
        return gate_part, up_part

    def swap(table, i):
        return remote(
            table.at[r], table.at[r], swap_send.at[i], swap_recv.at[i], {"rep": other}
        )

    res_sent = res_rows.at[r, pl.ds(0, plane - 1), used]
    for n in range(2):

        @pl.when(jnp.where(z > 0, 1, 0) == n)
        def _():
            arrived = res_rows.at[r, pl.ds(0, plane - n_exp - n), used]
            pltpu.make_async_copy(arrived, arrived, res_rsem).wait()

    swap(res_rows, 0).start()
    relays(chained & (z == 1), range(2 * quarter, heads))
    relays(chained & (z > 1), range(quarter))
    for load in loads:
        load.wait()

    mine = jnp.where(z < last, 1, 0) + jnp.where(z == middle, 1, 0)
    for b in range(n_seq):
        for own in range(2):

            @pl.when(jnp.where(z == home(b), 1, 0) == own)
            def _():
                if n_exp - own > 0:
                    arrived = rows.at[r, pl.ds(0, n_exp - own), used]
                    pltpu.make_async_copy(arrived, arrived, disp_recv.at[b]).wait()

    swap(rows, 1).start()
    gate_own, up_own = project(r, slice(0, hidden_rows))
    relays(chained & (z > 1), range(quarter, lead - 1))
    swap(res_rows, 0).wait()
    swap(rows, 1).wait()
    table = 0.0
    for s in range(n_rep):
        for e in range(n_exp):
            table += rows[s, pl.ds(e * n_seq, n_seq)].astype(F32)[:, :, columns:]
    table = table.reshape(slots, 128)
    s1, s2 = norms([table[:, n : n + 1] + table[:, n + 4 : n + 5] for n in range(4)])
    whole = lax.broadcasted_iota(jnp.int32, (slots, 1), 0) < SLOTS

    def scaled(values):
        values = jnp.transpose(values)
        fresh = values[0:slots, :]
        return jnp.where(whole, fresh, s2 * (values[slots:, :] + s1 * fresh))

    def share(i):
        part = (inner_head, inner_tail)[i]
        return remote(
            part.at[r], part.at[r], inner_ssem.at[i], inner_rsem.at[i], {"rep": other}
        )

    for i, lines in enumerate((slice(0, cut), slice(cut, hidden_rows))):
        gate_part, up_part = project(other, lines)
        gate_val = scaled(gate_own[lines] + gate_part)
        up_val = scaled(up_own[lines] + up_part)
        inner = gate_val / (1.0 + jnp.exp(-gate_val)) * up_val
        (inner_head, inner_tail)[i][r] = inner.astype(BF16)
        share(i).start()

    relays(chained & (z > 1), range(lead - 1, heads))

    def product(e, s, i):
        part = (inner_head, inner_tail)[i]
        lines = pl.ds(pl.multiple_of(s * hidden_rows + i * cut, 16), part.shape[2])
        return jnp.dot(part[s], wd[e, lines, :], preferred_element_type=F32)

    def hand_back(e, to):
        remote(
            fin.at[e * n_seq + to, used],
            back.at[here, used],
            back_send,
            back_recv.at[here],
            {"exp": e, "seq": to},
        ).start()

    turns = [lax.rem(x + j, n_exp) for j in range(1, n_exp + 1)]
    totals = [product(e, r, 0) + product(e, r, 1) for e in turns]
    share(0).wait_recv()
    totals = [total + product(e, other, 0) for total, e in zip(totals, turns)]
    share(1).wait_recv()
    for n, (total, e) in enumerate(zip(totals, turns)):
        whole = (total + product(e, other, 1)).reshape(n_seq, SLOTS, columns)
        fin[pl.ds(e * n_seq, n_seq)] = whole.astype(BF16)
        if n < n_exp - 1:
            for i in range(n_seq):
                hand_back(e, i)

    back[here] = fin[here]
    own_line(hand_back, range(n_seq))
    @pl.when(z == last)
    def _():
        for h in range(heads):
            for p in range(PARTS):
                hop(h, p, state_out).wait_recv()

    @pl.when(z > 0)
    def _():
        for h in range(heads):
            cols = slice(h * hd, (h + 1) * hd)
            att[:, cols] += jnp.dot(
                lifted[:, cols], state_in[h], preferred_element_type=F32
            )

    attended = att[...]
    square = jnp.sum(attended * attended, axis=1, keepdims=True)
    table = jnp.where(lane == 0, square, 0.0)
    sums[me] = jnp.transpose(table)[0:8, :]

    def tell(i):
        return remote(sums.at[me], sums.at[me], sums_send, sums_recv, peer_of(i))

    for i in range(peers - 1):
        tell(i).start()
    u_buf[...] = jax.nn.sigmoid(gate_ref[...].astype(F32)) * attended * again_ref[...]
    shares = jnp.transpose(rw_ref[...])
    combine = jnp.where(first_hit, shares[:, 0:1], shares[:, 1:2]) * onehot
    coarse = combine.astype(BF16)
    fine = (combine - coarse.astype(F32)).astype(BF16)

    for to in range(last):

        @pl.when(to < z)
        def _():
            for copy in ask(to):
                copy.wait_send()

    if middle != last:

        @pl.when(z == last)
        def _():
            for i in range(3):
                to_home(i).wait_send()

    for b in range(1, n_seq):

        @pl.when((z < b) & (z != home(b)))
        def _():
            offer(b).wait_send()

    @pl.when(z < last)
    def _():
        for h in range(heads):
            for p in range(PARTS):
                hop(h, p, state_out).wait_send()

    @pl.when(z > 0)
    def _():
        pltpu.make_async_copy(res_sent, res_sent, res_ssem).wait()

    @pl.when(z == 0)
    def _():
        everyone = first_sums.at[pl.ds(0, peers - 1)]
        pltpu.make_async_copy(everyone, everyone, first_ssem).wait()

    for n in range(1, 3):

        @pl.when(mine == n)
        def _():
            for _ in range(n):
                sent = rows.at[r, pl.ds(0, plane - 1), used]
                pltpu.make_async_copy(sent, sent, disp_send).wait()

    for i in range(2):
        share(i).wait_send()

    many = sums.at[pl.ds(0, peers - 1)]
    pltpu.make_async_copy(many, many, sums_recv).wait()
    total = jnp.sum(sums[...], axis=0)
    scale = lax.rsqrt(total / width + EPSILON)
    scale = jnp.transpose(scale)[:, 0:1]
    u_buf[...] = res_ref[...].astype(F32) + scale * u_buf[...]
    pltpu.make_async_copy(many, many, sums_send).wait()

    returned = back.at[pl.ds(0, plane - 1), used]
    for spot_of in [e * n_seq + n for n in range(n_seq) for e in range(n_exp)]:

        @pl.when(spot_of != here)
        def _():
            one = back.at[spot_of, used]
            pltpu.make_async_copy(one, one, back_recv.at[spot_of]).wait()

    result = u_buf[...]
    for e in range(n_exp):
        rows_e = jnp.sum(back[pl.ds(e * n_seq, n_seq)].astype(F32), axis=0)
        slot = lax.broadcasted_iota(jnp.int32, rows_e.shape, 0)
        rows_e = jnp.where(slot < CAP, rows_e, 0.0).astype(BF16)
        lanes = slice(e * SLOTS, (e + 1) * SLOTS)
        result += jnp.dot(coarse[:, lanes], rows_e, preferred_element_type=F32)
        result += jnp.dot(fine[:, lanes], rows_e, preferred_element_type=F32)
    out_ref[...] = result.astype(BF16)
    pltpu.make_async_copy(returned, returned, back_send).wait()


def solution(mesh):
    n_seq, n_exp, n_rep = (mesh.shape[a] for a in ("seq", "exp", "rep"))

    def shards(
        queries,
        key_rows,
        value_rows,
        decay_log,
        residual,
        out_gate,
        attn_gain,
        moe_gain,
        routes,
        route_weights,
        w_gate,
        w_up,
        w_down,
    ):
        tokens, columns = queries.shape
        heads = decay_log.shape[1]
        hd = columns // heads
        _, whole_rows, width = w_gate.shape
        even = whole_rows % (16 * n_rep) == 0
        hidden_rows = whole_rows // n_rep if even else whole_rows
        plane = n_exp * n_seq
        slots = n_seq * SLOTS
        vmem = pl.BlockSpec(memory_space=pltpu.VMEM)
        hbm = pl.BlockSpec(memory_space=pltpu.HBM)
        dma = pltpu.SemaphoreType.DMA
        cut = hidden_rows // 256 * 128
        if 2 < n_seq <= SHORT and even and cut > 0:
            wide = columns + 128
            return pl.pallas_call(
                lambda *refs: direct_kernel(n_seq, n_exp, n_rep, *refs),
                name="layer",
                out_shape=pltpu.VMEM((tokens, columns), BF16),
                in_specs=[hbm] * 13,
                out_specs=vmem,
                scratch_shapes=[
                    pltpu.VMEM((tokens, columns), BF16),
                    pltpu.VMEM((tokens, columns), BF16),
                    pltpu.VMEM((heads, tokens), F32),
                    pltpu.VMEM((tokens, columns), BF16),
                    pltpu.VMEM((2, tokens), jnp.int32),
                    pltpu.VMEM((2, tokens), F32),
                    pltpu.VMEM((tokens, columns), BF16),
                    pltpu.VMEM((tokens, columns), BF16),
                    pltpu.VMEM((1, columns), F32),
                    pltpu.VMEM((1, columns), F32),
                    pltpu.VMEM((hidden_rows, width), BF16),
                    pltpu.VMEM((hidden_rows, width), BF16),
                    pltpu.VMEM((n_exp, whole_rows, columns), BF16),
                    pltpu.VMEM((heads, hd, hd), BF16),
                    pltpu.VMEM((heads, hd, hd), BF16),
                    pltpu.VMEM((heads, hd, hd), BF16),
                    pltpu.VMEM((heads, hd, hd), F32),
                    pltpu.VMEM((tokens, columns), BF16),
                    pltpu.VMEM((tokens, columns), F32),
                    pltpu.VMEM((tokens, columns), F32),
                    pltpu.VMEM((n_exp * n_rep, 8, tokens), F32),
                    pltpu.VMEM((n_exp * n_rep, n_exp * SLOTS, 128), F32),
                    pltpu.VMEM((1, 128), F32),
                    pltpu.VMEM((n_seq, 1, 128), F32),
                    pltpu.VMEM((n_exp, SLOTS, columns), BF16),
                    pltpu.VMEM((n_seq, n_exp, SLOTS, columns), BF16),
                    pltpu.VMEM((n_seq, n_exp, SLOTS, columns), BF16),
                    pltpu.VMEM((n_seq, n_exp, SLOTS, columns), BF16),
                    pltpu.VMEM((n_seq, n_exp, SLOTS, columns), BF16),
                    pltpu.VMEM((3, n_exp, SLOTS, columns), BF16),
                    pltpu.VMEM((3, n_exp, SLOTS, columns), BF16),
                    pltpu.VMEM((3, n_exp * SLOTS, columns), F32),
                    pltpu.VMEM((n_exp * SLOTS, columns), F32),
                    pltpu.VMEM((heads, 128), F32),
                    pltpu.VMEM((n_exp, SLOTS, columns), BF16),
                    pltpu.VMEM((n_rep, plane, SLOTS, columns), BF16),
                    pltpu.VMEM((2, n_exp, SLOTS, wide), BF16),
                    pltpu.VMEM((n_rep, plane, SLOTS, wide), BF16),
                    pltpu.VMEM((n_rep, slots, cut), BF16),
                    pltpu.VMEM((n_rep, slots, hidden_rows - cut), BF16),
                    pltpu.VMEM((plane, SLOTS, columns), BF16),
                    pltpu.VMEM((plane, SLOTS, columns), BF16),
                    dma((10,)),
                    dma((2 + n_exp,)),
                    pltpu.SemaphoreType.REGULAR,
                    dma((heads, PARTS)),
                    dma((heads, PARTS)),
                    dma,
                    dma,
                    dma,
                    dma,
                    dma((n_seq,)),
                    dma((n_seq,)),
                    dma((n_seq,)),
                    dma((n_seq,)),
                    dma((n_seq,)),
                    dma((2, n_seq)),
                    dma((3,)),
                    dma((3,)),
                    dma,
                    dma,
                    dma,
                    dma((n_seq,)),
                    dma((2,)),
                    dma((2,)),
                    dma((2,)),
                    dma((2,)),
                    dma,
                    dma((plane,)),
                ],
                compiler_params=pltpu.CompilerParams(
                    collective_id=0, has_side_effects=True, vmem_limit_bytes=63000000
                ),
            )(
                key_rows,
                value_rows,
                decay_log.T,
                queries,
                routes.T,
                route_weights.T,
                residual,
                out_gate,
                attn_gain.reshape(1, columns),
                moe_gain.reshape(1, columns),
                w_gate,
                w_up,
                w_down,
            )
        return pl.pallas_call(
            lambda *refs: chain_kernel(n_seq, n_exp, n_rep, *refs),
            name="layer",
            out_shape=pltpu.VMEM((tokens, columns), BF16),
            in_specs=[hbm] * 13,
            out_specs=vmem,
            scratch_shapes=[
                pltpu.VMEM((tokens, columns), BF16),
                pltpu.VMEM((tokens, columns), BF16),
                pltpu.VMEM((heads, tokens), F32),
                pltpu.VMEM((tokens, columns), BF16),
                pltpu.VMEM((2, tokens), jnp.int32),
                pltpu.VMEM((2, tokens), F32),
                pltpu.VMEM((tokens, columns), BF16),
                pltpu.VMEM((tokens, columns), BF16),
                pltpu.VMEM((1, columns), F32),
                pltpu.VMEM((1, columns), F32),
                pltpu.VMEM((hidden_rows, width), BF16),
                pltpu.VMEM((hidden_rows, width), BF16),
                pltpu.VMEM((hidden_rows, width), BF16),
                pltpu.VMEM((heads, hd, hd), BF16),
                pltpu.VMEM((heads, hd, hd), BF16),
                pltpu.VMEM((heads, hd, hd), F32),
                pltpu.VMEM((tokens, columns), F32),
                pltpu.VMEM((tokens, columns), F32),
                pltpu.VMEM((n_exp * n_rep, 8, tokens), F32),
                pltpu.VMEM((n_exp, SLOTS, columns), BF16),
                pltpu.VMEM((n_rep, plane, SLOTS, columns), BF16),
                pltpu.VMEM((n_exp, slots, columns), BF16),
                pltpu.VMEM((n_exp, slots, columns), BF16),
                pltpu.VMEM((plane, SLOTS, columns), BF16),
                pltpu.VMEM((plane, SLOTS, columns), BF16),
                dma((10,)),
                dma((3,)),
                pltpu.SemaphoreType.REGULAR,
                dma((heads, PARTS)),
                dma((heads, PARTS)),
                dma,
                dma,
                dma,
                dma,
                dma,
                dma,
                dma((n_exp,)),
                dma((n_exp,)),
                dma,
                dma,
            ],
            compiler_params=pltpu.CompilerParams(collective_id=0, has_side_effects=True, vmem_limit_bytes=63000000),
        )(
            key_rows,
            value_rows,
            decay_log.T,
            queries,
            routes.T,
            route_weights.T,
            residual,
            out_gate,
            attn_gain.reshape(1, columns),
            moe_gain.reshape(1, columns),
            w_gate,
            w_up,
            w_down,
        )

    block = P(("groups", "seq"), ("exp", "rep"))
    gain = P(("exp", "rep"))
    route = P(("groups", "seq"), None)
    weight = P("exp", "seq", None)
    return jax.shard_map(
        shards,
        mesh=mesh,
        in_specs=(block,) * 6 + (gain, gain, route, route) + (weight,) * 3,
        out_specs=block,
        check_vma=False,
    )
```

```python
import jax
import jax.numpy as jnp
from jax import lax
from jax.experimental import pallas as pl
from jax.experimental.pallas import tpu as pltpu
from jax.sharding import PartitionSpec as P

CAP = 6
SLOTS = 8
PARTS = 2
SHORT = 4
EPSILON = 1e-06
MESH = pl.DeviceIdType.MESH
F32 = jnp.float32
BF16 = jnp.bfloat16


def sweep(count, body):
    if count <= 16:
        for i in range(count):
            body(i)
    else:
        lax.fori_loop(0, count, lambda i, c: (body(i), c)[1], 0)


def nt_dot(a, b):
    return lax.dot_general(a, b, (((1,), (1,)), ((), ())), preferred_element_type=F32)


def chain_kernel(
    n_seq,
    n_exp,
    n_rep,
    k_hbm,
    v_hbm,
    decay_hbm,
    q_hbm,
    routes_hbm,
    rw_hbm,
    res_hbm,
    gate_hbm,
    again_hbm,
    mgain_hbm,
    wg_hbm,
    wu_hbm,
    wd_hbm,
    out_ref,
    k_ref,
    v_ref,
    decay_ref,
    q_ref,
    routes_ref,
    rw_ref,
    res_ref,
    gate_ref,
    again_ref,
    mgain_ref,
    wg,
    wu,
    wd,
    state_in,
    state_out,
    block_state,
    att,
    u_buf,
    sums,
    pack,
    rows,
    half_send,
    half_recv,
    fin,
    back,
    in_sem,
    w_sem,
    go_sem,
    chain_send,
    chain_recv,
    sums_send,
    sums_recv,
    disp_send,
    disp_recv,
    swap_send,
    swap_recv,
    half_ssem,
    half_rsem,
    back_send,
    back_recv,
):
    z = lax.axis_index("seq")
    x = lax.axis_index("exp")
    r = lax.axis_index("rep")
    other = 1 - r
    tokens, columns = q_ref.shape
    heads = decay_ref.shape[0]
    hd = columns // heads
    part_rows = hd // PARTS
    hidden_rows = wg.shape[0]
    width = columns * n_exp * n_rep
    whole_rows = wg_hbm.shape[1]

    inputs = [
        pltpu.make_async_copy(src, dst, in_sem.at[i])
        for i, (src, dst) in enumerate(
            (
                (k_hbm, k_ref),
                (v_hbm, v_ref),
                (decay_hbm, decay_ref),
                (q_hbm, q_ref),
                (routes_hbm, routes_ref),
                (rw_hbm, rw_ref),
                (res_hbm, res_ref),
                (gate_hbm, gate_ref),
                (again_hbm, again_ref),
                (mgain_hbm, mgain_ref),
            )
        )
    ]
    for load in inputs:
        load.start()
    first = pl.multiple_of(r * hidden_rows, 16) if hidden_rows != whole_rows else 0
    loads = [
        pltpu.make_async_copy(src.at[0, pl.ds(first, hidden_rows), :], dst, w_sem.at[i])
        for i, (src, dst) in enumerate(((wg_hbm, wg), (wu_hbm, wu), (wd_hbm, wd)))
    ]

    barrier = pltpu.get_barrier_semaphore()
    plane = n_exp * n_seq
    peers = n_exp * n_rep
    me = x * n_rep + r
    last = n_seq - 1

    def greet(where):
        pl.semaphore_signal(barrier, inc=1, device_id=where, device_id_type=MESH)

    @pl.when(z < last)
    def _():
        greet({"seq": z + 1})

    @pl.when(z > 0)
    def _():
        greet({"seq": z - 1})

    def greet_peer(i):
        to = lax.rem(me + 1 + i, peers)
        greet({"exp": lax.div(to, n_rep), "rep": lax.rem(to, n_rep)})

    sweep(peers - 1, greet_peer)
    for load in loads:
        load.start()
    for load in inputs[:3]:
        load.wait()

    ti = lax.broadcasted_iota(jnp.int32, (tokens, tokens), 0)
    tj = lax.broadcasted_iota(jnp.int32, (tokens, tokens), 1)
    causal = ti >= tj
    upper = jnp.where(tj >= ti, 1.0, 0.0).astype(F32)
    cum_t = jnp.dot(
        decay_ref[...], upper, precision=lax.Precision.HIGHEST, preferred_element_type=F32
    )
    cum = jnp.transpose(cum_t)
    ending = cum[tokens - 1 : tokens, :]
    fading = jnp.exp(ending)
    to_end = jnp.exp(ending - cum)
    lift = jnp.exp(cum)
    for h in range(heads):
        cols = slice(h * hd, (h + 1) * hd)
        faded = k_ref[:, cols].astype(F32) * to_end[:, h : h + 1]
        block_state[h] = jnp.dot(
            jnp.transpose(faded).astype(BF16), v_ref[:, cols], preferred_element_type=F32
        )

    ends = (z > 0).astype(jnp.int32) + (z < last).astype(jnp.int32)
    pl.semaphore_wait(barrier, peers - 1 + ends)

    def hop(h, p):
        piece = pl.ds(p * part_rows, part_rows)
        return pltpu.make_async_remote_copy(
            src_ref=state_out.at[h, piece],
            dst_ref=state_in.at[h, piece],
            send_sem=chain_send.at[h, p],
            recv_sem=chain_recv.at[h, p],
            device_id={"seq": z + 1},
            device_id_type=MESH,
        )

    @pl.when(z == 0)
    def _():
        for h in range(heads):
            state_out[h] = block_state[h].astype(BF16)
            for p in range(PARTS):
                hop(h, p).start()

    inputs[3].wait()

    for h in range(heads):
        cols = slice(h * hd, (h + 1) * hd)
        scores = nt_dot(q_ref[:, cols], k_ref[:, cols])
        gaps = cum[:, h : h + 1] - cum_t[h : h + 1, :]
        mixing = jnp.where(causal, scores * jnp.exp(jnp.where(causal, gaps, 0.0)), 0.0)
        att[:, cols] = jnp.dot(mixing.astype(BF16), v_ref[:, cols], preferred_element_type=F32)

    for load in inputs[4:]:
        load.wait()
    lane = lax.broadcasted_iota(jnp.int32, (tokens, 128), 1)
    expert_of = lax.div(lane, SLOTS)
    slot_of = lax.rem(lane, SLOTS)
    named = jnp.transpose(routes_ref[...].astype(F32)).astype(jnp.int32)
    shares = jnp.transpose(rw_ref[...])
    first_hit = named[:, 0:1] == expert_of
    second_hit = named[:, 1:2] == expert_of
    hit = jnp.where(first_hit | second_hit, 1.0, 0.0)
    strict = jnp.where(ti > tj, 1.0, 0.0).astype(BF16)
    before = jnp.dot(strict, hit.astype(BF16), preferred_element_type=F32)
    taken = (hit > 0.5) & (before.astype(jnp.int32) == slot_of) & (slot_of < CAP)
    onehot = jnp.where(taken, 1.0, 0.0)
    combine = jnp.where(first_hit, shares[:, 0:1], shares[:, 1:2]) * onehot
    dispatch = jnp.transpose(onehot)[0 : n_exp * SLOTS, :].astype(BF16)

    def let_go(i):
        pl.semaphore_signal(go_sem, inc=1, device_id={"seq": i}, device_id_type=MESH)

    for h in range(heads):
        cols = slice(h * hd, (h + 1) * hd)

        @pl.when(z > 0)
        def _():
            for p in range(PARTS):
                piece = slice(p * part_rows, (p + 1) * part_rows)
                hop(h, p).wait_recv()

                @pl.when(z < last)
                def _():
                    state_out[h, piece] = (
                        fading[:, h : h + 1] * state_in[h, piece].astype(F32)
                        + block_state[h, piece]
                    ).astype(BF16)
                    hop(h, p).start()

            lifted = (q_ref[:, cols].astype(F32) * lift[:, h : h + 1]).astype(BF16)
            att[:, cols] += jnp.dot(lifted, state_in[h], preferred_element_type=F32)

        if h == max(heads - 3, 0):

            @pl.when(z == last)
            def _():
                sweep(last, let_go)

    res = res_ref[...].astype(F32)
    attended = att[...]
    u = jax.nn.sigmoid(gate_ref[...].astype(F32)) * attended * again_ref[...]
    u_buf[...] = u
    parts = (attended * attended, res * u, u * u, res * res)
    table = jnp.zeros((tokens, 128), F32)
    for i, part in enumerate(parts):
        table = jnp.where(lane == i, jnp.sum(part, axis=1, keepdims=True), table)
    sums[me] = jnp.transpose(table)[0:8, :]

    def tell(i):
        to = lax.rem(me + 1 + i, peers)
        pltpu.make_async_remote_copy(
            src_ref=sums.at[me],
            dst_ref=sums.at[me],
            send_sem=sums_send,
            recv_sem=sums_recv,
            device_id={"exp": lax.div(to, n_rep), "rep": lax.rem(to, n_rep)},
            device_id_type=MESH,
        ).start()

    sweep(peers - 1, tell)
    many = sums.at[pl.ds(0, peers - 1)]
    pltpu.make_async_copy(many, many, sums_recv).wait()
    total = jnp.sum(sums[...], axis=0)
    s1 = lax.rsqrt(total[0:1, :] / width + EPSILON)
    moe = total[3:4, :] + s1 * (2.0 * total[1:2, :] + s1 * total[2:3, :])
    s2 = lax.rsqrt(jnp.maximum(moe, 0.0) / width + EPSILON)
    row8 = lax.broadcasted_iota(jnp.int32, (8, tokens), 0)
    scales = jnp.transpose(jnp.where(row8 == 0, s1, s2))
    hidden = res_ref[...].astype(F32) + scales[:, 0:1] * u_buf[...]
    u_buf[...] = hidden
    normed = (hidden * scales[:, 1:2] * mgain_ref[...]).astype(BF16)

    packed = jnp.dot(dispatch, normed, preferred_element_type=F32)
    for e in range(n_exp):
        pack[e] = packed[e * SLOTS : (e + 1) * SLOTS, :].astype(BF16)
    here = x * n_seq + z
    rows[r, here] = pack[x]

    def deal(e, to, source, target, send_sem, recv_sem):
        pltpu.make_async_remote_copy(
            src_ref=source,
            dst_ref=target,
            send_sem=send_sem,
            recv_sem=recv_sem,
            device_id={"exp": e, "seq": to},
            device_id_type=MESH,
        ).start()

    def deal_rows(e, to):
        used = pl.ds(0, CAP)
        deal(e, to, pack.at[e, used], rows.at[r, here, used], disp_send, disp_recv)

    def earlier(send):
        def one(i):
            @pl.when(i < z)
            def _():
                for e in range(n_exp):
                    send(e, i)

        sweep(n_seq, one)

    def level(send):
        for j in range(1, n_exp):
            send(lax.rem(x + j, n_exp), z)

    def later(send):
        def one(i):
            @pl.when(last - i > z)
            def _():
                for e in range(n_exp):
                    send(e, last - i)

        sweep(n_seq, one)

    earlier(deal_rows)
    level(deal_rows)

    @pl.when(z < last)
    def _():
        pl.semaphore_wait(go_sem, 1)

    later(deal_rows)
    arrived = rows.at[r, pl.ds(0, plane - 1), pl.ds(0, CAP)]
    pltpu.make_async_copy(arrived, arrived, disp_recv).wait()
    swap = pltpu.make_async_remote_copy(
        src_ref=rows.at[r],
        dst_ref=rows.at[r],
        send_sem=swap_send,
        recv_sem=swap_recv,
        device_id={"rep": other},
        device_id_type=MESH,
    )
    swap.start()
    for load in loads:
        load.wait()
    slots = n_seq * SLOTS

    def project(s):
        gate_part = up_part = 0.0
        for e in range(n_exp):
            chunk = rows[s, pl.ds(e * n_seq, n_seq)].astype(F32).reshape(slots, columns)
            chunk = chunk.astype(BF16)
            at = pl.ds(pl.multiple_of((e * n_rep + s) * columns, 128), columns)
            gate_part += nt_dot(wg[:, at], chunk)
            up_part += nt_dot(wu[:, at], chunk)
        return gate_part, up_part

    gate_val, up_val = project(r)
    swap.wait()
    gate_part, up_part = project(other)
    gate_val += gate_part
    up_val += up_part
    inner = gate_val / (1.0 + jnp.exp(-gate_val)) * up_val
    if hidden_rows == whole_rows:
        unit = lax.broadcasted_iota(jnp.int32, inner.shape, 0)
        inner = jnp.where(lax.div(unit, whole_rows // n_rep) == r, inner, 0.0)
    inner = jnp.transpose(inner).astype(BF16)

    def product(e, s):
        at = pl.multiple_of((e * n_rep + s) * columns, 128)
        return jnp.dot(inner, wd[:, pl.ds(at, columns)], preferred_element_type=F32)

    def half(e):
        return pltpu.make_async_remote_copy(
            src_ref=half_send.at[e],
            dst_ref=half_recv.at[e],
            send_sem=half_ssem.at[e],
            recv_sem=half_rsem.at[e],
            device_id={"rep": other},
            device_id_type=MESH,
        )

    for e in range(n_exp):
        half_send[e] = product(e, other).astype(BF16)
        half(e).start()

    here_back = x * n_seq + z
    for e in range(n_exp):
        own = product(e, r)
        half(e).wait_recv()
        whole = (own + half_recv[e].astype(F32)).reshape(n_seq, SLOTS, columns)
        fin[pl.ds(e * n_seq, n_seq)] = whole.astype(BF16)

    back[here_back] = fin[here_back]

    def hand_back(e, to):
        used = pl.ds(0, CAP)
        source = fin.at[e * n_seq + to, used]
        deal(e, to, source, back.at[here_back, used], back_send, back_recv)

    earlier(hand_back)
    later(hand_back)
    level(hand_back)
    returned = back.at[pl.ds(0, plane - 1), pl.ds(0, CAP)]
    pltpu.make_async_copy(returned, returned, back_recv).wait()
    coarse = combine.astype(BF16)
    fine = (combine - coarse.astype(F32)).astype(BF16)
    result = u_buf[...]
    for e in range(n_exp):
        rows_e = jnp.sum(back[pl.ds(e * n_seq, n_seq)].astype(F32), axis=0)
        slot = lax.broadcasted_iota(jnp.int32, rows_e.shape, 0)
        rows_e = jnp.where(slot < CAP, rows_e, 0.0).astype(BF16)
        lanes = slice(e * SLOTS, (e + 1) * SLOTS)
        result += jnp.dot(coarse[:, lanes], rows_e, preferred_element_type=F32)
        result += jnp.dot(fine[:, lanes], rows_e, preferred_element_type=F32)
    out_ref[...] = result.astype(BF16)

    for h in range(heads):

        @pl.when(z < last)
        def _():
            for p in range(PARTS):
                hop(h, p).wait_send()

    pltpu.make_async_copy(many, many, sums_send).wait()
    pltpu.make_async_copy(arrived, arrived, disp_send).wait()
    for e in range(n_exp):
        half(e).wait_send()
    pltpu.make_async_copy(returned, returned, back_send).wait()


def direct_kernel(
    n_seq,
    n_exp,
    n_rep,
    k_hbm,
    v_hbm,
    decay_hbm,
    q_hbm,
    routes_hbm,
    rw_hbm,
    res_hbm,
    gate_hbm,
    again_hbm,
    mgain_hbm,
    wg_hbm,
    wu_hbm,
    wd_hbm,
    out_ref,
    k_ref,
    v_ref,
    decay_ref,
    q_ref,
    routes_ref,
    rw_ref,
    res_ref,
    gate_ref,
    again_ref,
    mgain_ref,
    wg,
    wu,
    wd,
    state_in,
    state_out,
    own_state,
    block_state,
    lifted,
    att,
    u_buf,
    sums,
    first_sums,
    end_send,
    end_recv,
    q_send,
    q_recv,
    part_send,
    part_recv,
    tail_recv,
    extra_send,
    extra_recv,
    near,
    acc,
    fade,
    res_pack,
    res_rows,
    pack,
    rows,
    inner_head,
    inner_tail,
    fin,
    back,
    in_sem,
    w_sem,
    go_sem,
    chain_send,
    chain_recv,
    sums_send,
    sums_recv,
    first_ssem,
    first_rsem,
    q_ssem,
    q_rsem,
    end_ssem,
    end_rsem,
    part_ssem,
    part_rsem,
    extra_ssem,
    extra_rsem,
    res_ssem,
    res_rsem,
    disp_send,
    disp_recv,
    swap_send,
    swap_recv,
    inner_ssem,
    inner_rsem,
    back_send,
    back_recv,
):
    z = lax.axis_index("seq")
    x = lax.axis_index("exp")
    r = lax.axis_index("rep")
    other = 1 - r
    tokens, columns = q_ref.shape
    heads = decay_ref.shape[0]
    hd = columns // heads
    part_rows = hd // PARTS
    hidden_rows = wg.shape[0]
    width = columns * n_exp * n_rep
    cut = inner_head.shape[2]
    plane = n_exp * n_seq
    peers = n_exp * n_rep
    me = x * n_rep + r
    last = n_seq - 1
    middle = max(last - 1, 0)
    picked = n_exp * SLOTS
    used = pl.ds(0, CAP)
    here = x * n_seq + z

    def home(b):
        return b if b < last else middle

    inputs = {
        name: pltpu.make_async_copy(src, dst, in_sem.at[i])
        for i, (name, src, dst) in enumerate(
            (
                ("decay", decay_hbm, decay_ref),
                ("routes", routes_hbm, routes_ref),
                ("q", q_hbm, q_ref),
                ("k", k_hbm, k_ref),
                ("v", v_hbm, v_ref),
                ("res", res_hbm, res_ref),
                ("gate", gate_hbm, gate_ref),
                ("again", again_hbm, again_ref),
                ("mgain", mgain_hbm, mgain_ref),
                ("rw", rw_hbm, rw_ref),
            )
        )
    }
    for load in inputs.values():
        load.start()

    barrier = pltpu.get_barrier_semaphore()

    def greet(where):
        pl.semaphore_signal(barrier, inc=1, device_id=where, device_id_type=MESH)

    for i in range(n_seq):

        @pl.when((i != z) & ((i > 0) | (z == 1)))
        def _():
            greet({"seq": i})

    for i in range(peers - 1):
        to = lax.rem(me + 1 + i, peers)
        greet({"exp": lax.div(to, n_rep), "rep": lax.rem(to, n_rep)})

    first = pl.ds(pl.multiple_of(r * hidden_rows, 16), hidden_rows)
    loads = [
        pltpu.make_async_copy(src.at[0, first, :], dst, w_sem.at[i])
        for i, (src, dst) in enumerate(((wg_hbm, wg), (wu_hbm, wu)))
    ]
    for e in range(n_exp):
        at = pl.ds(pl.multiple_of((e * n_rep + r) * columns, 128), columns)
        loads.append(
            pltpu.make_async_copy(wd_hbm.at[0, :, at], wd.at[e], w_sem.at[len(loads)])
        )
    for load in loads:
        load.start()

    def remote(src, dst, send_sem, recv_sem, where):
        return pltpu.make_async_remote_copy(
            src_ref=src,
            dst_ref=dst,
            send_sem=send_sem,
            recv_sem=recv_sem,
            device_id=where,
            device_id_type=MESH,
        )

    inputs["decay"].wait()
    inputs["routes"].wait()
    ti = lax.broadcasted_iota(jnp.int32, (tokens, tokens), 0)
    tj = lax.broadcasted_iota(jnp.int32, (tokens, tokens), 1)
    causal = ti >= tj
    upper = jnp.where(tj >= ti, 1.0, 0.0).astype(F32)
    cum_t = jnp.dot(
        decay_ref[...], upper, precision=lax.Precision.HIGHEST, preferred_element_type=F32
    )
    cum = jnp.transpose(cum_t)
    ending = cum[tokens - 1 : tokens, :]
    fade[...] = jnp.broadcast_to(jnp.exp(cum_t[:, tokens - 1 : tokens]), fade.shape)
    to_end = jnp.exp(ending - cum)
    lift = jnp.exp(cum)
    end_send[...] = jnp.zeros(end_send.shape, F32)
    end_send[:, 0:heads] = ending
    lane = lax.broadcasted_iota(jnp.int32, (tokens, 128), 1)
    expert_of = lax.div(lane, SLOTS)
    slot_of = lax.rem(lane, SLOTS)
    named = jnp.transpose(routes_ref[...].astype(F32)).astype(jnp.int32)
    first_hit = named[:, 0:1] == expert_of
    second_hit = named[:, 1:2] == expert_of
    hit = jnp.where(first_hit | second_hit, 1.0, 0.0)
    strict = jnp.where(ti > tj, 1.0, 0.0).astype(BF16)
    before = jnp.dot(strict, hit.astype(BF16), preferred_element_type=F32)
    taken = (hit > 0.5) & (before.astype(jnp.int32) == slot_of) & (slot_of < CAP)
    onehot = jnp.where(taken, 1.0, 0.0)
    dispatch = jnp.transpose(onehot)[0:picked, :].astype(BF16)

    def pick(values):
        return jnp.dot(dispatch, values, preferred_element_type=F32)

    def put(ref, values):
        for e in range(n_exp):
            ref[e, :, 0:columns] = values[e * SLOTS : (e + 1) * SLOTS, :].astype(BF16)

    def take(ref):
        return ref[...].astype(F32)[:, :, 0:columns].reshape(picked, columns)

    inputs["q"].wait()
    for h in range(heads):
        cols = slice(h * hd, (h + 1) * hd)
        lifted[:, cols] = (q_ref[:, cols].astype(F32) * lift[:, h : h + 1]).astype(BF16)
    put(q_send, pick(lifted[...]))

    def keep_state():
        inputs["k"].wait()
        inputs["v"].wait()
        for h in range(heads):
            cols = slice(h * hd, (h + 1) * hd)
            faded = k_ref[:, cols].astype(F32) * to_end[:, h : h + 1]
            state = jnp.dot(
                jnp.transpose(faded).astype(BF16), v_ref[:, cols], preferred_element_type=F32
            )
            block_state[h] = state
            own_state[h] = state.astype(BF16)

    @pl.when(z < last - 1)
    def _():
        keep_state()

    pl.semaphore_wait(barrier, jnp.where(z == 0, 1, last) + peers - 1)

    def let_go():
        for i in range(1, n_exp):
            pl.semaphore_signal(
                go_sem,
                inc=1,
                device_id={"exp": lax.rem(x + i, n_exp)},
                device_id_type=MESH,
            )

    @pl.when(z > 0)
    def _():
        let_go()

    def ask(to):
        where = {"seq": to}
        return (
            remote(
                q_send.at[:, used], q_recv.at[z, :, used], q_ssem.at[to], q_rsem.at[z], where
            ),
            remote(end_send, end_recv.at[z], end_ssem.at[to], end_rsem.at[z], where),
        )

    def asks(which):
        for to in which:

            @pl.when(to < z)
            def _():
                for copy in ask(to):
                    copy.start()

    asks(range(1))

    @pl.when(z == last - 1)
    def _():
        keep_state()

    def hop(h, p, src):
        piece = pl.ds(p * part_rows, part_rows)
        return remote(
            src.at[h, piece],
            state_in.at[h, piece],
            chain_send.at[h, p],
            chain_recv.at[h, p],
            {"seq": z + 1},
        )

    def set_off(which):
        @pl.when((z == 0) & (z < last))
        def _():
            for h in which:
                for p in range(PARTS):
                    hop(h, p, own_state).start()

    quarter = heads // 4
    lead = heads - quarter
    set_off(range(lead))

    @pl.when(z == last)
    def _():
        inputs["k"].wait()
        inputs["v"].wait()

    asks(range(1, last))

    for h in range(heads):
        cols = slice(h * hd, (h + 1) * hd)
        scores = nt_dot(q_ref[:, cols], k_ref[:, cols])
        gaps = cum[:, h : h + 1] - cum_t[h : h + 1, :]
        mixing = jnp.where(causal, scores * jnp.exp(jnp.where(causal, gaps, 0.0)), 0.0)
        att[:, cols] = jnp.dot(mixing.astype(BF16), v_ref[:, cols], preferred_element_type=F32)

    for name in ("res", "gate", "again", "mgain", "rw"):
        inputs[name].wait()
    near_att = pick(att[...].astype(BF16))
    near_res = pick(res_ref[...])
    near_v = jax.nn.sigmoid(pick(gate_ref[...])) * again_ref[...]
    near[0] = near_att
    near[1] = near_v
    near[2] = near_res

    spot = lax.broadcasted_iota(jnp.int32, (picked, 128), 1)

    def peer_of(i):
        to = lax.rem(me + 1 + i, peers)
        return {"exp": lax.div(to, n_rep), "rep": lax.rem(to, n_rep)}

    def products(attended, gated, residual):
        u = gated * attended
        parts = (attended * attended, residual * u, u * u, residual * residual)
        return u, [jnp.sum(part, axis=1, keepdims=True) for part in parts]

    def first_tell(i):
        return remote(
            first_sums.at[me], first_sums.at[me], first_ssem, first_rsem, peer_of(i)
        )

    @pl.when(z == 0)
    def _():
        _, wholes = products(near_att, near_v, near_res)
        table = jnp.zeros((picked, 128), F32)
        for n, whole in enumerate(wholes):
            table = jnp.where(spot == n, whole, table)
        first_sums[me] = table
        for i in range(peers - 1):
            first_tell(i).start()

    def to_home(i):
        return remote(
            extra_send.at[i, :, used],
            extra_recv.at[i, :, used],
            extra_ssem.at[i],
            extra_rsem.at[i],
            {"seq": middle},
        )

    @pl.when(z > 0)
    def _():
        put(res_pack, near_res * mgain_ref[...])
        res_rows[r, here] = res_pack[x]

    if middle != last:

        @pl.when(z == last)
        def _():
            for i, value in enumerate((near_att, near_v, near_res)):
                put(extra_send.at[i], value)
                to_home(i).start()

    def own_line(send, order=None):
        for i in order or [n for k in range(n_seq) for n in (last - k, k)][:n_seq]:

            @pl.when(i != z)
            def _():
                send(x, i)

    def other_lines(send, order=None):
        for j in range(1, n_exp):
            for i in order or [n for k in range(n_seq) for n in (last - k, k)][:n_seq]:
                send(lax.rem(x + j, n_exp), i)

    def send_res(e, to):
        remote(
            res_pack.at[e, used],
            res_rows.at[r, here, used],
            res_ssem,
            res_rsem,
            {"exp": e, "seq": to},
        ).start()

    def keep(b, i):
        rows[r, x * n_seq + b] = pack[i, x]

    def spread(b, i):
        spot_of = x * n_seq + b

        def send(e, to):
            remote(
                pack.at[i, e, used],
                rows.at[r, spot_of, used],
                disp_send,
                disp_recv.at[b],
                {"exp": e, "seq": to},
            ).start()

        return send

    def hand_out(b, i, attended, gated, residual):
        u, wholes = products(attended, gated, residual)
        table = jnp.zeros((picked, 128), F32)
        for n, whole in enumerate(wholes):
            coarse = whole.astype(BF16).astype(F32)
            table = jnp.where(spot == n, coarse, table)
            table = jnp.where(spot == n + len(wholes), whole - coarse, table)
        put(pack.at[i], u * mgain_ref[...])
        for e in range(n_exp):
            pack[i, e, :, columns:] = table[e * SLOTS : (e + 1) * SLOTS, :].astype(BF16)
        keep(b, i)
        return spread(b, i)

    def norms(total):
        s1 = lax.rsqrt(total[0] / width + EPSILON)
        moe = total[3] + s1 * (2.0 * total[1] + s1 * total[2])
        return s1, lax.rsqrt(jnp.maximum(moe, 0.0) / width + EPSILON)

    def send_all_res():
        own_line(send_res)
        pl.semaphore_wait(go_sem, n_exp - 1)
        other_lines(send_res)

    @pl.when(z > 0)
    def _():
        send_all_res()

    def offer(b):
        target = tail_recv if b == last else part_recv
        return remote(
            part_send.at[b, :, used],
            target.at[z, :, used],
            part_ssem.at[b],
            part_rsem.at[1 if b == last else 0, z],
            {"seq": home(b)},
        )

    def relay(h):
        for p in range(PARTS):
            piece = slice(p * part_rows, (p + 1) * part_rows)
            hop(h, p, state_out).wait_recv()
            state_out[h, piece] = (
                fade[h : h + 1, :] * state_in[h, piece].astype(F32) + block_state[h, piece]
            ).astype(BF16)
            hop(h, p, state_out).start()

    def relays(where, which):
        @pl.when(where)
        def _():
            for h in which:
                relay(h)

    chained = (z > 0) & (z < last)
    for b in range(1, n_seq):

        @pl.when(z < b)
        def _():
            ask_q = remote(q_send.at[:, used], q_recv.at[b, :, used], q_ssem.at[0], q_rsem.at[b], {"seq": 0})
            ask_e = remote(end_send, end_recv.at[b], end_ssem.at[0], end_rsem.at[b], {"seq": 0})
            ask_q.wait_recv()
            ask_e.wait_recv()
            between = jnp.zeros((1, 128), F32)
            for m in range(1, b):
                between += jnp.where(m > z, end_recv[m], 0.0)
            between = jnp.exp(between)
            asked = take(q_recv.at[b]).astype(BF16)
            given = [
                jnp.dot(
                    asked[:, h * hd : (h + 1) * hd], own_state[h], preferred_element_type=F32
                )
                * between[:, h : h + 1]
                for h in range(heads)
            ]
            given = jnp.concatenate(given, axis=1)
            put(part_send.at[b], given)

            @pl.when(z != home(b))
            def _():
                offer(b).start()

            if b == last:

                @pl.when(z == home(b))
                def _():
                    put(tail_recv.at[z], given)

    @pl.when(z == 0)
    def _():
        let_go()

    relays(chained & (z == 1), range(quarter))

    @pl.when(z == 0)
    def _():
        everyone = first_sums.at[pl.ds(0, peers - 1)]
        pltpu.make_async_copy(everyone, everyone, first_rsem).wait()
        total = jnp.sum(first_sums[...], axis=0)
        s1, s2 = norms([total[:, n : n + 1] for n in range(4)])
        normed = (near[2] + s1 * (near[0] * near[1])) * s2 * mgain_ref[...]
        put(pack.at[0], normed)
        keep(0, 0)
        own_line(spread(0, 0))

    @pl.when(z == 0)
    def _():
        pl.semaphore_wait(go_sem, n_exp - 1)
        other_lines(spread(0, 0))

    set_off(range(lead, heads))

    def wait_part(which, source):
        buffer = tail_recv if which else part_recv
        remote(
            part_send.at[0, :, used],
            buffer.at[source, :, used],
            part_ssem.at[0],
            part_rsem.at[which, source],
            {"seq": 0},
        ).wait_recv()

    @pl.when((z > 0) & (z < last))
    def _():
        acc[...] = near[0]
        for source in range(last):

            @pl.when(source < z)
            def _():
                wait_part(0, source)
                acc[...] += take(part_recv.at[source])

        send = hand_out(z, 0, acc[...], near[1], near[2])
        own_line(send)
        other_lines(send)


    @pl.when(z == middle)
    def _():
        for i in range(3):
            to_home(i).wait_recv()
        whole = take(extra_recv.at[0])
        whole += take(tail_recv.at[middle])
        for source in range(last):
            if source != middle:
                wait_part(1, source)
                whole += take(tail_recv.at[source])
        send = hand_out(last, 1, whole, take(extra_recv.at[1]), take(extra_recv.at[2]))
        order = sorted(range(n_seq), key=lambda i: -abs(i - middle))
        own_line(send, order)
        other_lines(send, order)

    slots = n_seq * SLOTS

    def pair(s, e):
        return jnp.concatenate(
            [
                table[s, pl.ds(e * n_seq, n_seq)]
                .astype(F32)[:, :, 0:columns]
                .reshape(slots, columns)
                .astype(BF16)
                for table in (rows, res_rows)
            ],
            axis=0,
        )

    def project(s, lines):
        gate_part = up_part = 0.0
        for e in range(n_exp):
            chunk = pair(s, e)
            at = pl.ds(pl.multiple_of((e * n_rep + s) * columns, 128), columns)
            gate_part += nt_dot(wg[lines, at], chunk)
            up_part += nt_dot(wu[lines, at], chunk)
        return gate_part, up_part

    def swap(table, i):
        return remote(
            table.at[r], table.at[r], swap_send.at[i], swap_recv.at[i], {"rep": other}
        )

    res_sent = res_rows.at[r, pl.ds(0, plane - 1), used]
    for n in range(2):

        @pl.when(jnp.where(z > 0, 1, 0) == n)
        def _():
            arrived = res_rows.at[r, pl.ds(0, plane - n_exp - n), used]
            pltpu.make_async_copy(arrived, arrived, res_rsem).wait()

    swap(res_rows, 0).start()
    relays(chained & (z == 1), range(quarter, heads))
    relays(chained & (z > 1), range(quarter))
    for load in loads:
        load.wait()

    mine = jnp.where(z < last, 1, 0) + jnp.where(z == middle, 1, 0)
    for b in range(n_seq):
        for own in range(2):

            @pl.when(jnp.where(z == home(b), 1, 0) == own)
            def _():
                if n_exp - own > 0:
                    arrived = rows.at[r, pl.ds(0, n_exp - own), used]
                    pltpu.make_async_copy(arrived, arrived, disp_recv.at[b]).wait()

    swap(rows, 1).start()
    gate_own, up_own = project(r, slice(0, hidden_rows))
    relays(chained & (z > 1), range(quarter, lead - 1))
    swap(res_rows, 0).wait()
    swap(rows, 1).wait()
    table = 0.0
    for s in range(n_rep):
        for e in range(n_exp):
            table += rows[s, pl.ds(e * n_seq, n_seq)].astype(F32)[:, :, columns:]
    table = table.reshape(slots, 128)
    s1, s2 = norms([table[:, n : n + 1] + table[:, n + 4 : n + 5] for n in range(4)])
    whole = lax.broadcasted_iota(jnp.int32, (slots, 1), 0) < SLOTS

    def scaled(values):
        values = jnp.transpose(values)
        fresh = values[0:slots, :]
        return jnp.where(whole, fresh, s2 * (values[slots:, :] + s1 * fresh))

    def share(i):
        part = (inner_head, inner_tail)[i]
        return remote(
            part.at[r], part.at[r], inner_ssem.at[i], inner_rsem.at[i], {"rep": other}
        )

    for i, lines in enumerate((slice(0, cut), slice(cut, hidden_rows))):
        gate_part, up_part = project(other, lines)
        gate_val = scaled(gate_own[lines] + gate_part)
        up_val = scaled(up_own[lines] + up_part)
        inner = gate_val / (1.0 + jnp.exp(-gate_val)) * up_val
        (inner_head, inner_tail)[i][r] = inner.astype(BF16)
        share(i).start()

    relays(chained & (z > 1), range(lead - 1, heads))

    def product(e, s, i):
        part = (inner_head, inner_tail)[i]
        lines = pl.ds(pl.multiple_of(s * hidden_rows + i * cut, 16), part.shape[2])
        return jnp.dot(part[s], wd[e, lines, :], preferred_element_type=F32)

    def hand_back(e, to):
        remote(
            fin.at[e * n_seq + to, used],
            back.at[here, used],
            back_send,
            back_recv.at[here],
            {"exp": e, "seq": to},
        ).start()

    turns = [lax.rem(x + j, n_exp) for j in range(1, n_exp + 1)]
    totals = [product(e, r, 0) + product(e, r, 1) for e in turns]
    share(0).wait_recv()
    totals = [total + product(e, other, 0) for total, e in zip(totals, turns)]
    share(1).wait_recv()
    for n, (total, e) in enumerate(zip(totals, turns)):
        whole = (total + product(e, other, 1)).reshape(n_seq, SLOTS, columns)
        fin[pl.ds(e * n_seq, n_seq)] = whole.astype(BF16)
        if n < n_exp - 1:
            for i in range(n_seq):
                hand_back(e, i)

    back[here] = fin[here]
    own_line(hand_back, range(n_seq))
    @pl.when(z == last)
    def _():
        for h in range(heads):
            for p in range(PARTS):
                hop(h, p, state_out).wait_recv()

    @pl.when(z > 0)
    def _():
        for h in range(heads):
            cols = slice(h * hd, (h + 1) * hd)
            att[:, cols] += jnp.dot(
                lifted[:, cols], state_in[h], preferred_element_type=F32
            )

    attended = att[...]
    square = jnp.sum(attended * attended, axis=1, keepdims=True)
    table = jnp.where(lane == 0, square, 0.0)
    sums[me] = jnp.transpose(table)[0:8, :]

    def tell(i):
        return remote(sums.at[me], sums.at[me], sums_send, sums_recv, peer_of(i))

    for i in range(peers - 1):
        tell(i).start()
    u_buf[...] = jax.nn.sigmoid(gate_ref[...].astype(F32)) * attended * again_ref[...]
    shares = jnp.transpose(rw_ref[...])
    combine = jnp.where(first_hit, shares[:, 0:1], shares[:, 1:2]) * onehot
    coarse = combine.astype(BF16)
    fine = (combine - coarse.astype(F32)).astype(BF16)

    for to in range(last):

        @pl.when(to < z)
        def _():
            for copy in ask(to):
                copy.wait_send()

    if middle != last:

        @pl.when(z == last)
        def _():
            for i in range(3):
                to_home(i).wait_send()

    for b in range(1, n_seq):

        @pl.when((z < b) & (z != home(b)))
        def _():
            offer(b).wait_send()

    @pl.when(z < last)
    def _():
        for h in range(heads):
            for p in range(PARTS):
                hop(h, p, state_out).wait_send()

    @pl.when(z > 0)
    def _():
        pltpu.make_async_copy(res_sent, res_sent, res_ssem).wait()

    @pl.when(z == 0)
    def _():
        everyone = first_sums.at[pl.ds(0, peers - 1)]
        pltpu.make_async_copy(everyone, everyone, first_ssem).wait()

    for n in range(1, 3):

        @pl.when(mine == n)
        def _():
            for _ in range(n):
                sent = rows.at[r, pl.ds(0, plane - 1), used]
                pltpu.make_async_copy(sent, sent, disp_send).wait()

    for i in range(2):
        share(i).wait_send()

    many = sums.at[pl.ds(0, peers - 1)]
    pltpu.make_async_copy(many, many, sums_recv).wait()
    total = jnp.sum(sums[...], axis=0)
    scale = lax.rsqrt(total / width + EPSILON)
    scale = jnp.transpose(scale)[:, 0:1]
    u_buf[...] = res_ref[...].astype(F32) + scale * u_buf[...]
    pltpu.make_async_copy(many, many, sums_send).wait()

    returned = back.at[pl.ds(0, plane - 1), used]
    for spot_of in [e * n_seq + n for n in range(n_seq) for e in range(n_exp)]:

        @pl.when(spot_of != here)
        def _():
            one = back.at[spot_of, used]
            pltpu.make_async_copy(one, one, back_recv.at[spot_of]).wait()

    slot = lax.rem(lax.broadcasted_iota(jnp.int32, (picked, columns), 0), SLOTS)
    owed = jnp.concatenate(
        [
            jnp.sum(back[pl.ds(e * n_seq, n_seq)].astype(F32), axis=0)
            for e in range(n_exp)
        ],
        axis=0,
    )
    owed = jnp.where(slot < CAP, owed, 0.0).astype(BF16)
    result = u_buf[...]
    for part in (coarse, fine):
        result += jnp.dot(part[:, 0:picked], owed, preferred_element_type=F32)
    out_ref[...] = result.astype(BF16)
    pltpu.make_async_copy(returned, returned, back_send).wait()


def solution(mesh):
    n_seq, n_exp, n_rep = (mesh.shape[a] for a in ("seq", "exp", "rep"))

    def shards(
        queries,
        key_rows,
        value_rows,
        decay_log,
        residual,
        out_gate,
        attn_gain,
        moe_gain,
        routes,
        route_weights,
        w_gate,
        w_up,
        w_down,
    ):
        tokens, columns = queries.shape
        heads = decay_log.shape[1]
        hd = columns // heads
        _, whole_rows, width = w_gate.shape
        even = whole_rows % (16 * n_rep) == 0
        hidden_rows = whole_rows // n_rep if even else whole_rows
        plane = n_exp * n_seq
        slots = n_seq * SLOTS
        vmem = pl.BlockSpec(memory_space=pltpu.VMEM)
        hbm = pl.BlockSpec(memory_space=pltpu.HBM)
        dma = pltpu.SemaphoreType.DMA
        cut = hidden_rows // 192 * 128
        if 2 < n_seq <= SHORT and even and cut > 0:
            wide = columns + 128
            return pl.pallas_call(
                lambda *refs: direct_kernel(n_seq, n_exp, n_rep, *refs),
                name="layer",
                out_shape=pltpu.VMEM((tokens, columns), BF16),
                in_specs=[hbm] * 13,
                out_specs=vmem,
                scratch_shapes=[
                    pltpu.VMEM((tokens, columns), BF16),
                    pltpu.VMEM((tokens, columns), BF16),
                    pltpu.VMEM((heads, tokens), F32),
                    pltpu.VMEM((tokens, columns), BF16),
                    pltpu.VMEM((2, tokens), jnp.int32),
                    pltpu.VMEM((2, tokens), F32),
                    pltpu.VMEM((tokens, columns), BF16),
                    pltpu.VMEM((tokens, columns), BF16),
                    pltpu.VMEM((1, columns), F32),
                    pltpu.VMEM((1, columns), F32),
                    pltpu.VMEM((hidden_rows, width), BF16),
                    pltpu.VMEM((hidden_rows, width), BF16),
                    pltpu.VMEM((n_exp, whole_rows, columns), BF16),
                    pltpu.VMEM((heads, hd, hd), BF16),
                    pltpu.VMEM((heads, hd, hd), BF16),
                    pltpu.VMEM((heads, hd, hd), BF16),
                    pltpu.VMEM((heads, hd, hd), F32),
                    pltpu.VMEM((tokens, columns), BF16),
                    pltpu.VMEM((tokens, columns), F32),
                    pltpu.VMEM((tokens, columns), F32),
                    pltpu.VMEM((n_exp * n_rep, 8, tokens), F32),
                    pltpu.VMEM((n_exp * n_rep, n_exp * SLOTS, 128), F32),
                    pltpu.VMEM((1, 128), F32),
                    pltpu.VMEM((n_seq, 1, 128), F32),
                    pltpu.VMEM((n_exp, SLOTS, columns), BF16),
                    pltpu.VMEM((n_seq, n_exp, SLOTS, columns), BF16),
                    pltpu.VMEM((n_seq, n_exp, SLOTS, columns), BF16),
                    pltpu.VMEM((n_seq, n_exp, SLOTS, columns), BF16),
                    pltpu.VMEM((n_seq, n_exp, SLOTS, columns), BF16),
                    pltpu.VMEM((3, n_exp, SLOTS, columns), BF16),
                    pltpu.VMEM((3, n_exp, SLOTS, columns), BF16),
                    pltpu.VMEM((3, n_exp * SLOTS, columns), F32),
                    pltpu.VMEM((n_exp * SLOTS, columns), F32),
                    pltpu.VMEM((heads, 128), F32),
                    pltpu.VMEM((n_exp, SLOTS, columns), BF16),
                    pltpu.VMEM((n_rep, plane, SLOTS, columns), BF16),
                    pltpu.VMEM((2, n_exp, SLOTS, wide), BF16),
                    pltpu.VMEM((n_rep, plane, SLOTS, wide), BF16),
                    pltpu.VMEM((n_rep, slots, cut), BF16),
                    pltpu.VMEM((n_rep, slots, hidden_rows - cut), BF16),
                    pltpu.VMEM((plane, SLOTS, columns), BF16),
                    pltpu.VMEM((plane, SLOTS, columns), BF16),
                    dma((10,)),
                    dma((2 + n_exp,)),
                    pltpu.SemaphoreType.REGULAR,
                    dma((heads, PARTS)),
                    dma((heads, PARTS)),
                    dma,
                    dma,
                    dma,
                    dma,
                    dma((n_seq,)),
                    dma((n_seq,)),
                    dma((n_seq,)),
                    dma((n_seq,)),
                    dma((n_seq,)),
                    dma((2, n_seq)),
                    dma((3,)),
                    dma((3,)),
                    dma,
                    dma,
                    dma,
                    dma((n_seq,)),
                    dma((2,)),
                    dma((2,)),
                    dma((2,)),
                    dma((2,)),
                    dma,
                    dma((plane,)),
                ],
                compiler_params=pltpu.CompilerParams(
                    collective_id=0, has_side_effects=True, vmem_limit_bytes=63000000
                ),
            )(
                key_rows,
                value_rows,
                decay_log.T,
                queries,
                routes.T,
                route_weights.T,
                residual,
                out_gate,
                attn_gain.reshape(1, columns),
                moe_gain.reshape(1, columns),
                w_gate,
                w_up,
                w_down,
            )
        return pl.pallas_call(
            lambda *refs: chain_kernel(n_seq, n_exp, n_rep, *refs),
            name="layer",
            out_shape=pltpu.VMEM((tokens, columns), BF16),
            in_specs=[hbm] * 13,
            out_specs=vmem,
            scratch_shapes=[
                pltpu.VMEM((tokens, columns), BF16),
                pltpu.VMEM((tokens, columns), BF16),
                pltpu.VMEM((heads, tokens), F32),
                pltpu.VMEM((tokens, columns), BF16),
                pltpu.VMEM((2, tokens), jnp.int32),
                pltpu.VMEM((2, tokens), F32),
                pltpu.VMEM((tokens, columns), BF16),
                pltpu.VMEM((tokens, columns), BF16),
                pltpu.VMEM((1, columns), F32),
                pltpu.VMEM((1, columns), F32),
                pltpu.VMEM((hidden_rows, width), BF16),
                pltpu.VMEM((hidden_rows, width), BF16),
                pltpu.VMEM((hidden_rows, width), BF16),
                pltpu.VMEM((heads, hd, hd), BF16),
                pltpu.VMEM((heads, hd, hd), BF16),
                pltpu.VMEM((heads, hd, hd), F32),
                pltpu.VMEM((tokens, columns), F32),
                pltpu.VMEM((tokens, columns), F32),
                pltpu.VMEM((n_exp * n_rep, 8, tokens), F32),
                pltpu.VMEM((n_exp, SLOTS, columns), BF16),
                pltpu.VMEM((n_rep, plane, SLOTS, columns), BF16),
                pltpu.VMEM((n_exp, slots, columns), BF16),
                pltpu.VMEM((n_exp, slots, columns), BF16),
                pltpu.VMEM((plane, SLOTS, columns), BF16),
                pltpu.VMEM((plane, SLOTS, columns), BF16),
                dma((10,)),
                dma((3,)),
                pltpu.SemaphoreType.REGULAR,
                dma((heads, PARTS)),
                dma((heads, PARTS)),
                dma,
                dma,
                dma,
                dma,
                dma,
                dma,
                dma((n_exp,)),
                dma((n_exp,)),
                dma,
                dma,
            ],
            compiler_params=pltpu.CompilerParams(collective_id=0, has_side_effects=True, vmem_limit_bytes=63000000),
        )(
            key_rows,
            value_rows,
            decay_log.T,
            queries,
            routes.T,
            route_weights.T,
            residual,
            out_gate,
            attn_gain.reshape(1, columns),
            moe_gain.reshape(1, columns),
            w_gate,
            w_up,
            w_down,
        )

    block = P(("groups", "seq"), ("exp", "rep"))
    gain = P(("exp", "rep"))
    route = P(("groups", "seq"), None)
    weight = P("exp", "seq", None)
    return jax.shard_map(
        shards,
        mesh=mesh,
        in_specs=(block,) * 6 + (gain, gain, route, route) + (weight,) * 3,
        out_specs=block,
        check_vma=False,
    )
```

```python
import jax
import jax.numpy as jnp
from jax import lax
from jax.experimental import pallas as pl
from jax.experimental.pallas import tpu as pltpu
from jax.sharding import PartitionSpec as P

CAP = 6
SLOTS = 8
PARTS = 2
SHORT = 4
EPSILON = 1e-06
MESH = pl.DeviceIdType.MESH
F32 = jnp.float32
BF16 = jnp.bfloat16


def sweep(count, body):
    if count <= 16:
        for i in range(count):
            body(i)
    else:
        lax.fori_loop(0, count, lambda i, c: (body(i), c)[1], 0)


def nt_dot(a, b):
    return lax.dot_general(a, b, (((1,), (1,)), ((), ())), preferred_element_type=F32)


def chain_kernel(
    n_seq,
    n_exp,
    n_rep,
    k_hbm,
    v_hbm,
    decay_hbm,
    q_hbm,
    routes_hbm,
    rw_hbm,
    res_hbm,
    gate_hbm,
    again_hbm,
    mgain_hbm,
    wg_hbm,
    wu_hbm,
    wd_hbm,
    out_ref,
    k_ref,
    v_ref,
    decay_ref,
    q_ref,
    routes_ref,
    rw_ref,
    res_ref,
    gate_ref,
    again_ref,
    mgain_ref,
    wg,
    wu,
    wd,
    state_in,
    state_out,
    block_state,
    att,
    u_buf,
    sums,
    pack,
    rows,
    half_send,
    half_recv,
    fin,
    back,
    in_sem,
    w_sem,
    go_sem,
    chain_send,
    chain_recv,
    sums_send,
    sums_recv,
    disp_send,
    disp_recv,
    swap_send,
    swap_recv,
    half_ssem,
    half_rsem,
    back_send,
    back_recv,
):
    z = lax.axis_index("seq")
    x = lax.axis_index("exp")
    r = lax.axis_index("rep")
    other = 1 - r
    tokens, columns = q_ref.shape
    heads = decay_ref.shape[0]
    hd = columns // heads
    part_rows = hd // PARTS
    hidden_rows = wg.shape[0]
    width = columns * n_exp * n_rep
    whole_rows = wg_hbm.shape[1]

    inputs = [
        pltpu.make_async_copy(src, dst, in_sem.at[i])
        for i, (src, dst) in enumerate(
            (
                (k_hbm, k_ref),
                (v_hbm, v_ref),
                (decay_hbm, decay_ref),
                (q_hbm, q_ref),
                (routes_hbm, routes_ref),
                (rw_hbm, rw_ref),
                (res_hbm, res_ref),
                (gate_hbm, gate_ref),
                (again_hbm, again_ref),
                (mgain_hbm, mgain_ref),
            )
        )
    ]
    for load in inputs:
        load.start()
    first = pl.multiple_of(r * hidden_rows, 16) if hidden_rows != whole_rows else 0
    loads = [
        pltpu.make_async_copy(src.at[0, pl.ds(first, hidden_rows), :], dst, w_sem.at[i])
        for i, (src, dst) in enumerate(((wg_hbm, wg), (wu_hbm, wu), (wd_hbm, wd)))
    ]

    barrier = pltpu.get_barrier_semaphore()
    plane = n_exp * n_seq
    peers = n_exp * n_rep
    me = x * n_rep + r
    last = n_seq - 1

    def greet(where):
        pl.semaphore_signal(barrier, inc=1, device_id=where, device_id_type=MESH)

    @pl.when(z < last)
    def _():
        greet({"seq": z + 1})

    @pl.when(z > 0)
    def _():
        greet({"seq": z - 1})

    def greet_peer(i):
        to = lax.rem(me + 1 + i, peers)
        greet({"exp": lax.div(to, n_rep), "rep": lax.rem(to, n_rep)})

    sweep(peers - 1, greet_peer)
    for load in loads:
        load.start()
    for load in inputs[:3]:
        load.wait()

    ti = lax.broadcasted_iota(jnp.int32, (tokens, tokens), 0)
    tj = lax.broadcasted_iota(jnp.int32, (tokens, tokens), 1)
    causal = ti >= tj
    upper = jnp.where(tj >= ti, 1.0, 0.0).astype(F32)
    cum_t = jnp.dot(
        decay_ref[...], upper, precision=lax.Precision.HIGHEST, preferred_element_type=F32
    )
    cum = jnp.transpose(cum_t)
    ending = cum[tokens - 1 : tokens, :]
    fading = jnp.exp(ending)
    to_end = jnp.exp(ending - cum)
    lift = jnp.exp(cum)
    for h in range(heads):
        cols = slice(h * hd, (h + 1) * hd)
        faded = k_ref[:, cols].astype(F32) * to_end[:, h : h + 1]
        block_state[h] = jnp.dot(
            jnp.transpose(faded).astype(BF16), v_ref[:, cols], preferred_element_type=F32
        )

    ends = (z > 0).astype(jnp.int32) + (z < last).astype(jnp.int32)
    pl.semaphore_wait(barrier, peers - 1 + ends)

    def hop(h, p):
        piece = pl.ds(p * part_rows, part_rows)
        return pltpu.make_async_remote_copy(
            src_ref=state_out.at[h, piece],
            dst_ref=state_in.at[h, piece],
            send_sem=chain_send.at[h, p],
            recv_sem=chain_recv.at[h, p],
            device_id={"seq": z + 1},
            device_id_type=MESH,
        )

    @pl.when(z == 0)
    def _():
        for h in range(heads):
            state_out[h] = block_state[h].astype(BF16)
            for p in range(PARTS):
                hop(h, p).start()

    inputs[3].wait()

    for h in range(heads):
        cols = slice(h * hd, (h + 1) * hd)
        scores = nt_dot(q_ref[:, cols], k_ref[:, cols])
        gaps = cum[:, h : h + 1] - cum_t[h : h + 1, :]
        mixing = jnp.where(causal, scores * jnp.exp(jnp.where(causal, gaps, 0.0)), 0.0)
        att[:, cols] = jnp.dot(mixing.astype(BF16), v_ref[:, cols], preferred_element_type=F32)

    for load in inputs[4:]:
        load.wait()
    lane = lax.broadcasted_iota(jnp.int32, (tokens, 128), 1)
    expert_of = lax.div(lane, SLOTS)
    slot_of = lax.rem(lane, SLOTS)
    named = jnp.transpose(routes_ref[...].astype(F32)).astype(jnp.int32)
    shares = jnp.transpose(rw_ref[...])
    first_hit = named[:, 0:1] == expert_of
    second_hit = named[:, 1:2] == expert_of
    hit = jnp.where(first_hit | second_hit, 1.0, 0.0)
    strict = jnp.where(ti > tj, 1.0, 0.0).astype(BF16)
    before = jnp.dot(strict, hit.astype(BF16), preferred_element_type=F32)
    taken = (hit > 0.5) & (before.astype(jnp.int32) == slot_of) & (slot_of < CAP)
    onehot = jnp.where(taken, 1.0, 0.0)
    combine = jnp.where(first_hit, shares[:, 0:1], shares[:, 1:2]) * onehot
    dispatch = jnp.transpose(onehot)[0 : n_exp * SLOTS, :].astype(BF16)

    def let_go(i):
        pl.semaphore_signal(go_sem, inc=1, device_id={"seq": i}, device_id_type=MESH)

    for h in range(heads):
        cols = slice(h * hd, (h + 1) * hd)

        @pl.when(z > 0)
        def _():
            for p in range(PARTS):
                piece = slice(p * part_rows, (p + 1) * part_rows)
                hop(h, p).wait_recv()

                @pl.when(z < last)
                def _():
                    state_out[h, piece] = (
                        fading[:, h : h + 1] * state_in[h, piece].astype(F32)
                        + block_state[h, piece]
                    ).astype(BF16)
                    hop(h, p).start()

            lifted = (q_ref[:, cols].astype(F32) * lift[:, h : h + 1]).astype(BF16)
            att[:, cols] += jnp.dot(lifted, state_in[h], preferred_element_type=F32)

        if h == max(heads - 3, 0):

            @pl.when(z == last)
            def _():
                sweep(last, let_go)

    res = res_ref[...].astype(F32)
    attended = att[...]
    u = jax.nn.sigmoid(gate_ref[...].astype(F32)) * attended * again_ref[...]
    u_buf[...] = u
    parts = (attended * attended, res * u, u * u, res * res)
    table = jnp.zeros((tokens, 128), F32)
    for i, part in enumerate(parts):
        table = jnp.where(lane == i, jnp.sum(part, axis=1, keepdims=True), table)
    sums[me] = jnp.transpose(table)[0:8, :]

    def tell(i):
        to = lax.rem(me + 1 + i, peers)
        pltpu.make_async_remote_copy(
            src_ref=sums.at[me],
            dst_ref=sums.at[me],
            send_sem=sums_send,
            recv_sem=sums_recv,
            device_id={"exp": lax.div(to, n_rep), "rep": lax.rem(to, n_rep)},
            device_id_type=MESH,
        ).start()

    sweep(peers - 1, tell)
    many = sums.at[pl.ds(0, peers - 1)]
    pltpu.make_async_copy(many, many, sums_recv).wait()
    total = jnp.sum(sums[...], axis=0)
    s1 = lax.rsqrt(total[0:1, :] / width + EPSILON)
    moe = total[3:4, :] + s1 * (2.0 * total[1:2, :] + s1 * total[2:3, :])
    s2 = lax.rsqrt(jnp.maximum(moe, 0.0) / width + EPSILON)
    row8 = lax.broadcasted_iota(jnp.int32, (8, tokens), 0)
    scales = jnp.transpose(jnp.where(row8 == 0, s1, s2))
    hidden = res_ref[...].astype(F32) + scales[:, 0:1] * u_buf[...]
    u_buf[...] = hidden
    normed = (hidden * scales[:, 1:2] * mgain_ref[...]).astype(BF16)

    packed = jnp.dot(dispatch, normed, preferred_element_type=F32)
    for e in range(n_exp):
        pack[e] = packed[e * SLOTS : (e + 1) * SLOTS, :].astype(BF16)
    here = x * n_seq + z
    rows[r, here] = pack[x]

    def deal(e, to, source, target, send_sem, recv_sem):
        pltpu.make_async_remote_copy(
            src_ref=source,
            dst_ref=target,
            send_sem=send_sem,
            recv_sem=recv_sem,
            device_id={"exp": e, "seq": to},
            device_id_type=MESH,
        ).start()

    def deal_rows(e, to):
        used = pl.ds(0, CAP)
        deal(e, to, pack.at[e, used], rows.at[r, here, used], disp_send, disp_recv)

    def earlier(send):
        def one(i):
            @pl.when(i < z)
            def _():
                for e in range(n_exp):
                    send(e, i)

        sweep(n_seq, one)

    def level(send):
        for j in range(1, n_exp):
            send(lax.rem(x + j, n_exp), z)

    def later(send):
        def one(i):
            @pl.when(last - i > z)
            def _():
                for e in range(n_exp):
                    send(e, last - i)

        sweep(n_seq, one)

    earlier(deal_rows)
    level(deal_rows)

    @pl.when(z < last)
    def _():
        pl.semaphore_wait(go_sem, 1)

    later(deal_rows)
    arrived = rows.at[r, pl.ds(0, plane - 1), pl.ds(0, CAP)]
    pltpu.make_async_copy(arrived, arrived, disp_recv).wait()
    swap = pltpu.make_async_remote_copy(
        src_ref=rows.at[r],
        dst_ref=rows.at[r],
        send_sem=swap_send,
        recv_sem=swap_recv,
        device_id={"rep": other},
        device_id_type=MESH,
    )
    swap.start()
    for load in loads:
        load.wait()
    slots = n_seq * SLOTS

    def project(s):
        gate_part = up_part = 0.0
        for e in range(n_exp):
            chunk = rows[s, pl.ds(e * n_seq, n_seq)].astype(F32).reshape(slots, columns)
            chunk = chunk.astype(BF16)
            at = pl.ds(pl.multiple_of((e * n_rep + s) * columns, 128), columns)
            gate_part += nt_dot(wg[:, at], chunk)
            up_part += nt_dot(wu[:, at], chunk)
        return gate_part, up_part

    gate_val, up_val = project(r)
    swap.wait()
    gate_part, up_part = project(other)
    gate_val += gate_part
    up_val += up_part
    inner = gate_val / (1.0 + jnp.exp(-gate_val)) * up_val
    if hidden_rows == whole_rows:
        unit = lax.broadcasted_iota(jnp.int32, inner.shape, 0)
        inner = jnp.where(lax.div(unit, whole_rows // n_rep) == r, inner, 0.0)
    inner = jnp.transpose(inner).astype(BF16)

    def product(e, s):
        at = pl.multiple_of((e * n_rep + s) * columns, 128)
        return jnp.dot(inner, wd[:, pl.ds(at, columns)], preferred_element_type=F32)

    def half(e):
        return pltpu.make_async_remote_copy(
            src_ref=half_send.at[e],
            dst_ref=half_recv.at[e],
            send_sem=half_ssem.at[e],
            recv_sem=half_rsem.at[e],
            device_id={"rep": other},
            device_id_type=MESH,
        )

    for e in range(n_exp):
        half_send[e] = product(e, other).astype(BF16)
        half(e).start()

    here_back = x * n_seq + z
    for e in range(n_exp):
        own = product(e, r)
        half(e).wait_recv()
        whole = (own + half_recv[e].astype(F32)).reshape(n_seq, SLOTS, columns)
        fin[pl.ds(e * n_seq, n_seq)] = whole.astype(BF16)

    back[here_back] = fin[here_back]

    def hand_back(e, to):
        used = pl.ds(0, CAP)
        source = fin.at[e * n_seq + to, used]
        deal(e, to, source, back.at[here_back, used], back_send, back_recv)

    earlier(hand_back)
    later(hand_back)
    level(hand_back)
    returned = back.at[pl.ds(0, plane - 1), pl.ds(0, CAP)]
    pltpu.make_async_copy(returned, returned, back_recv).wait()
    coarse = combine.astype(BF16)
    fine = (combine - coarse.astype(F32)).astype(BF16)
    result = u_buf[...]
    for e in range(n_exp):
        rows_e = jnp.sum(back[pl.ds(e * n_seq, n_seq)].astype(F32), axis=0)
        slot = lax.broadcasted_iota(jnp.int32, rows_e.shape, 0)
        rows_e = jnp.where(slot < CAP, rows_e, 0.0).astype(BF16)
        lanes = slice(e * SLOTS, (e + 1) * SLOTS)
        result += jnp.dot(coarse[:, lanes], rows_e, preferred_element_type=F32)
        result += jnp.dot(fine[:, lanes], rows_e, preferred_element_type=F32)
    out_ref[...] = result.astype(BF16)

    for h in range(heads):

        @pl.when(z < last)
        def _():
            for p in range(PARTS):
                hop(h, p).wait_send()

    pltpu.make_async_copy(many, many, sums_send).wait()
    pltpu.make_async_copy(arrived, arrived, disp_send).wait()
    for e in range(n_exp):
        half(e).wait_send()
    pltpu.make_async_copy(returned, returned, back_send).wait()


def direct_kernel(
    n_seq,
    n_exp,
    n_rep,
    k_hbm,
    v_hbm,
    decay_hbm,
    q_hbm,
    routes_hbm,
    rw_hbm,
    res_hbm,
    gate_hbm,
    again_hbm,
    mgain_hbm,
    wg_hbm,
    wu_hbm,
    wd_hbm,
    out_ref,
    k_ref,
    v_ref,
    decay_ref,
    q_ref,
    routes_ref,
    rw_ref,
    res_ref,
    gate_ref,
    again_ref,
    mgain_ref,
    wg,
    wu,
    wd,
    state_in,
    state_out,
    own_state,
    block_state,
    lifted,
    att,
    u_buf,
    sums,
    first_sums,
    end_send,
    end_recv,
    q_send,
    q_recv,
    part_send,
    part_recv,
    tail_recv,
    extra_send,
    extra_recv,
    near,
    acc,
    fade,
    res_pack,
    res_rows,
    pack,
    rows,
    inner_head,
    inner_tail,
    fin,
    back,
    in_sem,
    w_sem,
    go_sem,
    chain_send,
    chain_recv,
    sums_send,
    sums_recv,
    first_ssem,
    first_rsem,
    q_ssem,
    q_rsem,
    end_ssem,
    end_rsem,
    part_ssem,
    part_rsem,
    extra_ssem,
    extra_rsem,
    res_ssem,
    res_rsem,
    disp_send,
    disp_recv,
    swap_send,
    swap_recv,
    inner_ssem,
    inner_rsem,
    back_send,
    back_recv,
):
    z = lax.axis_index("seq")
    x = lax.axis_index("exp")
    r = lax.axis_index("rep")
    other = 1 - r
    tokens, columns = q_ref.shape
    heads = decay_ref.shape[0]
    hd = columns // heads
    part_rows = hd // PARTS
    hidden_rows = wg.shape[0]
    width = columns * n_exp * n_rep
    cut = inner_head.shape[2]
    plane = n_exp * n_seq
    peers = n_exp * n_rep
    me = x * n_rep + r
    last = n_seq - 1
    middle = max(last - 1, 0)
    picked = n_exp * SLOTS
    used = pl.ds(0, CAP)
    here = x * n_seq + z

    def home(b):
        return b if b < last else middle

    inputs = {
        name: pltpu.make_async_copy(src, dst, in_sem.at[i])
        for i, (name, src, dst) in enumerate(
            (
                ("decay", decay_hbm, decay_ref),
                ("routes", routes_hbm, routes_ref),
                ("q", q_hbm, q_ref),
                ("k", k_hbm, k_ref),
                ("v", v_hbm, v_ref),
                ("res", res_hbm, res_ref),
                ("gate", gate_hbm, gate_ref),
                ("again", again_hbm, again_ref),
                ("mgain", mgain_hbm, mgain_ref),
                ("rw", rw_hbm, rw_ref),
            )
        )
    }
    for load in inputs.values():
        load.start()

    barrier = pltpu.get_barrier_semaphore()

    def greet(where):
        pl.semaphore_signal(barrier, inc=1, device_id=where, device_id_type=MESH)

    for i in range(n_seq):

        @pl.when((i != z) & ((i > 0) | (z == 1)))
        def _():
            greet({"seq": i})

    for i in range(peers - 1):
        to = lax.rem(me + 1 + i, peers)
        greet({"exp": lax.div(to, n_rep), "rep": lax.rem(to, n_rep)})

    first = pl.ds(pl.multiple_of(r * hidden_rows, 16), hidden_rows)
    loads = [
        pltpu.make_async_copy(src.at[0, first, :], dst, w_sem.at[i])
        for i, (src, dst) in enumerate(((wg_hbm, wg), (wu_hbm, wu)))
    ]
    for e in range(n_exp):
        at = pl.ds(pl.multiple_of((e * n_rep + r) * columns, 128), columns)
        loads.append(
            pltpu.make_async_copy(wd_hbm.at[0, :, at], wd.at[e], w_sem.at[len(loads)])
        )
    for load in loads:
        load.start()

    def remote(src, dst, send_sem, recv_sem, where):
        return pltpu.make_async_remote_copy(
            src_ref=src,
            dst_ref=dst,
            send_sem=send_sem,
            recv_sem=recv_sem,
            device_id=where,
            device_id_type=MESH,
        )

    inputs["decay"].wait()
    inputs["routes"].wait()
    ti = lax.broadcasted_iota(jnp.int32, (tokens, tokens), 0)
    tj = lax.broadcasted_iota(jnp.int32, (tokens, tokens), 1)
    causal = ti >= tj
    upper = jnp.where(tj >= ti, 1.0, 0.0).astype(F32)
    cum_t = jnp.dot(
        decay_ref[...], upper, precision=lax.Precision.HIGHEST, preferred_element_type=F32
    )
    cum = jnp.transpose(cum_t)
    ending = cum[tokens - 1 : tokens, :]
    fade[...] = jnp.broadcast_to(jnp.exp(cum_t[:, tokens - 1 : tokens]), fade.shape)
    to_end = jnp.exp(ending - cum)
    lift = jnp.exp(cum)
    end_send[...] = jnp.zeros(end_send.shape, F32)
    end_send[:, 0:heads] = ending
    lane = lax.broadcasted_iota(jnp.int32, (tokens, 128), 1)
    expert_of = lax.div(lane, SLOTS)
    slot_of = lax.rem(lane, SLOTS)
    named = jnp.transpose(routes_ref[...].astype(F32)).astype(jnp.int32)
    first_hit = named[:, 0:1] == expert_of
    second_hit = named[:, 1:2] == expert_of
    hit = jnp.where(first_hit | second_hit, 1.0, 0.0)
    strict = jnp.where(ti > tj, 1.0, 0.0).astype(BF16)
    before = jnp.dot(strict, hit.astype(BF16), preferred_element_type=F32)
    taken = (hit > 0.5) & (before.astype(jnp.int32) == slot_of) & (slot_of < CAP)
    onehot = jnp.where(taken, 1.0, 0.0)
    dispatch = jnp.transpose(onehot)[0:picked, :].astype(BF16)

    def pick(values):
        return jnp.dot(dispatch, values, preferred_element_type=F32)

    def put(ref, values):
        for e in range(n_exp):
            ref[e, :, 0:columns] = values[e * SLOTS : (e + 1) * SLOTS, :].astype(BF16)

    def take(ref):
        return ref[...].astype(F32)[:, :, 0:columns].reshape(picked, columns)

    inputs["q"].wait()
    for h in range(heads):
        cols = slice(h * hd, (h + 1) * hd)
        lifted[:, cols] = (q_ref[:, cols].astype(F32) * lift[:, h : h + 1]).astype(BF16)
    put(q_send, pick(lifted[...]))

    def keep_state():
        inputs["k"].wait()
        inputs["v"].wait()
        for h in range(heads):
            cols = slice(h * hd, (h + 1) * hd)
            faded = k_ref[:, cols].astype(F32) * to_end[:, h : h + 1]
            state = jnp.dot(
                jnp.transpose(faded).astype(BF16), v_ref[:, cols], preferred_element_type=F32
            )
            block_state[h] = state
            own_state[h] = state.astype(BF16)

    @pl.when(z < last - 1)
    def _():
        keep_state()

    pl.semaphore_wait(barrier, jnp.where(z == 0, 1, last) + peers - 1)

    def let_go():
        for i in range(1, n_exp):
            pl.semaphore_signal(
                go_sem,
                inc=1,
                device_id={"exp": lax.rem(x + i, n_exp)},
                device_id_type=MESH,
            )

    @pl.when(z > 0)
    def _():
        let_go()

    def ask(to):
        where = {"seq": to}
        return (
            remote(
                q_send.at[:, used], q_recv.at[z, :, used], q_ssem.at[to], q_rsem.at[z], where
            ),
            remote(end_send, end_recv.at[z], end_ssem.at[to], end_rsem.at[z], where),
        )

    def asks(which):
        for to in which:

            @pl.when(to < z)
            def _():
                for copy in ask(to):
                    copy.start()

    asks(range(1))

    @pl.when(z == last - 1)
    def _():
        keep_state()

    def hop(h, p, src):
        piece = pl.ds(p * part_rows, part_rows)
        return remote(
            src.at[h, piece],
            state_in.at[h, piece],
            chain_send.at[h, p],
            chain_recv.at[h, p],
            {"seq": z + 1},
        )

    def set_off(which):
        @pl.when((z == 0) & (z < last))
        def _():
            for h in which:
                for p in range(PARTS):
                    hop(h, p, own_state).start()

    quarter = heads // 4
    lead = heads - quarter
    set_off(range(lead))

    @pl.when(z == last)
    def _():
        inputs["k"].wait()
        inputs["v"].wait()

    asks(range(1, last))

    for h in range(heads):
        cols = slice(h * hd, (h + 1) * hd)
        scores = nt_dot(q_ref[:, cols], k_ref[:, cols])
        gaps = cum[:, h : h + 1] - cum_t[h : h + 1, :]
        mixing = jnp.where(causal, scores * jnp.exp(jnp.where(causal, gaps, 0.0)), 0.0)
        att[:, cols] = jnp.dot(mixing.astype(BF16), v_ref[:, cols], preferred_element_type=F32)

    for name in ("res", "gate", "again", "mgain", "rw"):
        inputs[name].wait()
    near_att = pick(att[...].astype(BF16))
    near_res = pick(res_ref[...])
    near_v = jax.nn.sigmoid(pick(gate_ref[...])) * again_ref[...]
    near[0] = near_att
    near[1] = near_v
    near[2] = near_res

    spot = lax.broadcasted_iota(jnp.int32, (picked, 128), 1)

    def peer_of(i):
        to = lax.rem(me + 1 + i, peers)
        return {"exp": lax.div(to, n_rep), "rep": lax.rem(to, n_rep)}

    def products(attended, gated, residual):
        u = gated * attended
        parts = (attended * attended, residual * u, u * u, residual * residual)
        return u, [jnp.sum(part, axis=1, keepdims=True) for part in parts]

    def first_tell(i):
        return remote(
            first_sums.at[me], first_sums.at[me], first_ssem, first_rsem, peer_of(i)
        )

    @pl.when(z == 0)
    def _():
        _, wholes = products(near_att, near_v, near_res)
        table = jnp.zeros((picked, 128), F32)
        for n, whole in enumerate(wholes):
            table = jnp.where(spot == n, whole, table)
        first_sums[me] = table
        for i in range(peers - 1):
            first_tell(i).start()

    def to_home(i):
        return remote(
            extra_send.at[i, :, used],
            extra_recv.at[i, :, used],
            extra_ssem.at[i],
            extra_rsem.at[i],
            {"seq": middle},
        )

    @pl.when(z > 0)
    def _():
        put(res_pack, near_res * mgain_ref[...])
        res_rows[r, here] = res_pack[x]

    if middle != last:

        @pl.when(z == last)
        def _():
            for i, value in enumerate((near_att, near_v, near_res)):
                put(extra_send.at[i], value)
                to_home(i).start()

    def own_line(send, order=None):
        for i in order or [n for k in range(n_seq) for n in (last - k, k)][:n_seq]:

            @pl.when(i != z)
            def _():
                send(x, i)

    def other_lines(send, order=None):
        for j in range(1, n_exp):
            for i in order or [n for k in range(n_seq) for n in (last - k, k)][:n_seq]:
                send(lax.rem(x + j, n_exp), i)

    def send_res(e, to):
        remote(
            res_pack.at[e, used],
            res_rows.at[r, here, used],
            res_ssem,
            res_rsem,
            {"exp": e, "seq": to},
        ).start()

    def keep(b, i):
        rows[r, x * n_seq + b] = pack[i, x]

    def spread(b, i):
        spot_of = x * n_seq + b

        def send(e, to):
            remote(
                pack.at[i, e, used],
                rows.at[r, spot_of, used],
                disp_send,
                disp_recv.at[b],
                {"exp": e, "seq": to},
            ).start()

        return send

    def hand_out(b, i, attended, gated, residual):
        u, wholes = products(attended, gated, residual)
        table = jnp.zeros((picked, 128), F32)
        for n, whole in enumerate(wholes):
            coarse = whole.astype(BF16).astype(F32)
            table = jnp.where(spot == n, coarse, table)
            table = jnp.where(spot == n + len(wholes), whole - coarse, table)
        put(pack.at[i], u * mgain_ref[...])
        for e in range(n_exp):
            pack[i, e, :, columns:] = table[e * SLOTS : (e + 1) * SLOTS, :].astype(BF16)
        keep(b, i)
        return spread(b, i)

    def norms(total):
        s1 = lax.rsqrt(total[0] / width + EPSILON)
        moe = total[3] + s1 * (2.0 * total[1] + s1 * total[2])
        return s1, lax.rsqrt(jnp.maximum(moe, 0.0) / width + EPSILON)

    def send_all_res():
        own_line(send_res)
        pl.semaphore_wait(go_sem, n_exp - 1)
        other_lines(send_res)

    @pl.when(z > 0)
    def _():
        send_all_res()

    def offer(b):
        target = tail_recv if b == last else part_recv
        return remote(
            part_send.at[b, :, used],
            target.at[z, :, used],
            part_ssem.at[b],
            part_rsem.at[1 if b == last else 0, z],
            {"seq": home(b)},
        )

    def relay(h):
        for p in range(PARTS):
            piece = slice(p * part_rows, (p + 1) * part_rows)
            hop(h, p, state_out).wait_recv()
            state_out[h, piece] = (
                fade[h : h + 1, :] * state_in[h, piece].astype(F32) + block_state[h, piece]
            ).astype(BF16)
            hop(h, p, state_out).start()

    def relays(where, which):
        @pl.when(where)
        def _():
            for h in which:
                relay(h)

    chained = (z > 0) & (z < last)
    for b in range(1, n_seq):

        @pl.when(z < b)
        def _():
            ask_q = remote(q_send.at[:, used], q_recv.at[b, :, used], q_ssem.at[0], q_rsem.at[b], {"seq": 0})
            ask_e = remote(end_send, end_recv.at[b], end_ssem.at[0], end_rsem.at[b], {"seq": 0})
            ask_q.wait_recv()
            ask_e.wait_recv()
            between = jnp.zeros((1, 128), F32)
            for m in range(1, b):
                between += jnp.where(m > z, end_recv[m], 0.0)
            between = jnp.exp(between)
            asked = take(q_recv.at[b]).astype(BF16)
            given = [
                jnp.dot(
                    asked[:, h * hd : (h + 1) * hd], own_state[h], preferred_element_type=F32
                )
                * between[:, h : h + 1]
                for h in range(heads)
            ]
            given = jnp.concatenate(given, axis=1)
            put(part_send.at[b], given)

            @pl.when(z != home(b))
            def _():
                offer(b).start()

            if b == last:

                @pl.when(z == home(b))
                def _():
                    put(tail_recv.at[z], given)

    @pl.when(z == 0)
    def _():
        let_go()

    relays(chained & (z == 1), range(quarter))

    @pl.when(z == 0)
    def _():
        everyone = first_sums.at[pl.ds(0, peers - 1)]
        pltpu.make_async_copy(everyone, everyone, first_rsem).wait()
        total = jnp.sum(first_sums[...], axis=0)
        s1, s2 = norms([total[:, n : n + 1] for n in range(4)])
        normed = (near[2] + s1 * (near[0] * near[1])) * s2 * mgain_ref[...]
        put(pack.at[0], normed)
        keep(0, 0)
        own_line(spread(0, 0))

    @pl.when(z == 0)
    def _():
        pl.semaphore_wait(go_sem, n_exp - 1)
        other_lines(spread(0, 0))

    set_off(range(lead, heads))

    def wait_part(which, source):
        buffer = tail_recv if which else part_recv
        remote(
            part_send.at[0, :, used],
            buffer.at[source, :, used],
            part_ssem.at[0],
            part_rsem.at[which, source],
            {"seq": 0},
        ).wait_recv()

    @pl.when((z > 0) & (z < last))
    def _():
        acc[...] = near[0]
        for source in range(last):

            @pl.when(source < z)
            def _():
                wait_part(0, source)
                acc[...] += take(part_recv.at[source])

        send = hand_out(z, 0, acc[...], near[1], near[2])
        other_lines(send)
        own_line(send)


    @pl.when(z == middle)
    def _():
        for i in range(3):
            to_home(i).wait_recv()
        whole = take(extra_recv.at[0])
        whole += take(tail_recv.at[middle])
        for source in range(last):
            if source != middle:
                wait_part(1, source)
                whole += take(tail_recv.at[source])
        send = hand_out(last, 1, whole, take(extra_recv.at[1]), take(extra_recv.at[2]))
        order = sorted(range(n_seq), key=lambda i: -abs(i - middle))
        other_lines(send, order)
        own_line(send, order)

    slots = n_seq * SLOTS

    def pair(s, e):
        return jnp.concatenate(
            [
                table[s, pl.ds(e * n_seq, n_seq)]
                .astype(F32)[:, :, 0:columns]
                .reshape(slots, columns)
                .astype(BF16)
                for table in (rows, res_rows)
            ],
            axis=0,
        )

    def project(s, lines):
        gate_part = up_part = 0.0
        for e in range(n_exp):
            chunk = pair(s, e)
            at = pl.ds(pl.multiple_of((e * n_rep + s) * columns, 128), columns)
            gate_part += nt_dot(wg[lines, at], chunk)
            up_part += nt_dot(wu[lines, at], chunk)
        return gate_part, up_part

    def swap(table, i):
        return remote(
            table.at[r], table.at[r], swap_send.at[i], swap_recv.at[i], {"rep": other}
        )

    res_sent = res_rows.at[r, pl.ds(0, plane - 1), used]
    for n in range(2):

        @pl.when(jnp.where(z > 0, 1, 0) == n)
        def _():
            arrived = res_rows.at[r, pl.ds(0, plane - n_exp - n), used]
            pltpu.make_async_copy(arrived, arrived, res_rsem).wait()

    swap(res_rows, 0).start()
    relays(chained & (z == 1), range(quarter, heads))
    relays(chained & (z > 1), range(quarter))
    for load in loads:
        load.wait()

    mine = jnp.where(z < last, 1, 0) + jnp.where(z == middle, 1, 0)
    for b in range(n_seq):
        for own in range(2):

            @pl.when(jnp.where(z == home(b), 1, 0) == own)
            def _():
                if n_exp - own > 0:
                    arrived = rows.at[r, pl.ds(0, n_exp - own), used]
                    pltpu.make_async_copy(arrived, arrived, disp_recv.at[b]).wait()

    swap(rows, 1).start()
    gate_own, up_own = project(r, slice(0, hidden_rows))
    relays(chained & (z > 1), range(quarter, lead - 1))
    swap(res_rows, 0).wait()
    swap(rows, 1).wait()
    table = 0.0
    for s in range(n_rep):
        for e in range(n_exp):
            table += rows[s, pl.ds(e * n_seq, n_seq)].astype(F32)[:, :, columns:]
    table = table.reshape(slots, 128)
    s1, s2 = norms([table[:, n : n + 1] + table[:, n + 4 : n + 5] for n in range(4)])
    whole = lax.broadcasted_iota(jnp.int32, (slots, 1), 0) < SLOTS

    def scaled(values):
        values = jnp.transpose(values)
        fresh = values[0:slots, :]
        return jnp.where(whole, fresh, s2 * (values[slots:, :] + s1 * fresh))

    def share(i):
        part = (inner_head, inner_tail)[i]
        return remote(
            part.at[r], part.at[r], inner_ssem.at[i], inner_rsem.at[i], {"rep": other}
        )

    for i, lines in enumerate((slice(0, cut), slice(cut, hidden_rows))):
        gate_part, up_part = project(other, lines)
        gate_val = scaled(gate_own[lines] + gate_part)
        up_val = scaled(up_own[lines] + up_part)
        inner = gate_val / (1.0 + jnp.exp(-gate_val)) * up_val
        (inner_head, inner_tail)[i][r] = inner.astype(BF16)
        share(i).start()

    relays(chained & (z > 1), range(lead - 1, heads))

    def product(e, s, i):
        part = (inner_head, inner_tail)[i]
        lines = pl.ds(pl.multiple_of(s * hidden_rows + i * cut, 16), part.shape[2])
        return jnp.dot(part[s], wd[e, lines, :], preferred_element_type=F32)

    def hand_back(e, to):
        remote(
            fin.at[e * n_seq + to, used],
            back.at[here, used],
            back_send,
            back_recv.at[here],
            {"exp": e, "seq": to},
        ).start()

    turns = [lax.rem(x + j, n_exp) for j in range(1, n_exp + 1)]
    totals = [product(e, r, 0) + product(e, r, 1) for e in turns]
    share(0).wait_recv()
    totals = [total + product(e, other, 0) for total, e in zip(totals, turns)]
    share(1).wait_recv()
    for n, (total, e) in enumerate(zip(totals, turns)):
        whole = (total + product(e, other, 1)).reshape(n_seq, SLOTS, columns)
        fin[pl.ds(e * n_seq, n_seq)] = whole.astype(BF16)
        if n < n_exp - 1:
            for i in range(n_seq):
                hand_back(e, i)

    back[here] = fin[here]
    own_line(hand_back, range(n_seq))
    @pl.when(z == last)
    def _():
        for h in range(heads):
            for p in range(PARTS):
                hop(h, p, state_out).wait_recv()

    @pl.when(z > 0)
    def _():
        for h in range(heads):
            cols = slice(h * hd, (h + 1) * hd)
            att[:, cols] += jnp.dot(
                lifted[:, cols], state_in[h], preferred_element_type=F32
            )

    attended = att[...]
    square = jnp.sum(attended * attended, axis=1, keepdims=True)
    table = jnp.where(lane == 0, square, 0.0)
    sums[me] = jnp.transpose(table)[0:8, :]

    def tell(i):
        return remote(sums.at[me], sums.at[me], sums_send, sums_recv, peer_of(i))

    for i in range(peers - 1):
        tell(i).start()
    u_buf[...] = jax.nn.sigmoid(gate_ref[...].astype(F32)) * attended * again_ref[...]
    shares = jnp.transpose(rw_ref[...])
    combine = jnp.where(first_hit, shares[:, 0:1], shares[:, 1:2]) * onehot
    coarse = combine.astype(BF16)
    fine = (combine - coarse.astype(F32)).astype(BF16)

    for to in range(last):

        @pl.when(to < z)
        def _():
            for copy in ask(to):
                copy.wait_send()

    if middle != last:

        @pl.when(z == last)
        def _():
            for i in range(3):
                to_home(i).wait_send()

    for b in range(1, n_seq):

        @pl.when((z < b) & (z != home(b)))
        def _():
            offer(b).wait_send()

    @pl.when(z < last)
    def _():
        for h in range(heads):
            for p in range(PARTS):
                hop(h, p, state_out).wait_send()

    @pl.when(z > 0)
    def _():
        pltpu.make_async_copy(res_sent, res_sent, res_ssem).wait()

    @pl.when(z == 0)
    def _():
        everyone = first_sums.at[pl.ds(0, peers - 1)]
        pltpu.make_async_copy(everyone, everyone, first_ssem).wait()

    for n in range(1, 3):

        @pl.when(mine == n)
        def _():
            for _ in range(n):
                sent = rows.at[r, pl.ds(0, plane - 1), used]
                pltpu.make_async_copy(sent, sent, disp_send).wait()

    for i in range(2):
        share(i).wait_send()

    many = sums.at[pl.ds(0, peers - 1)]
    pltpu.make_async_copy(many, many, sums_recv).wait()
    total = jnp.sum(sums[...], axis=0)
    scale = lax.rsqrt(total / width + EPSILON)
    scale = jnp.transpose(scale)[:, 0:1]
    u_buf[...] = res_ref[...].astype(F32) + scale * u_buf[...]
    pltpu.make_async_copy(many, many, sums_send).wait()

    returned = back.at[pl.ds(0, plane - 1), used]
    for spot_of in [e * n_seq + n for n in range(n_seq) for e in range(n_exp)]:

        @pl.when(spot_of != here)
        def _():
            one = back.at[spot_of, used]
            pltpu.make_async_copy(one, one, back_recv.at[spot_of]).wait()

    slot = lax.rem(lax.broadcasted_iota(jnp.int32, (picked, columns), 0), SLOTS)
    owed = jnp.concatenate(
        [
            jnp.sum(back[pl.ds(e * n_seq, n_seq)].astype(F32), axis=0)
            for e in range(n_exp)
        ],
        axis=0,
    )
    owed = jnp.where(slot < CAP, owed, 0.0).astype(BF16)
    result = u_buf[...]
    for part in (coarse, fine):
        result += jnp.dot(part[:, 0:picked], owed, preferred_element_type=F32)
    out_ref[...] = result.astype(BF16)
    pltpu.make_async_copy(returned, returned, back_send).wait()


def solution(mesh):
    n_seq, n_exp, n_rep = (mesh.shape[a] for a in ("seq", "exp", "rep"))

    def shards(
        queries,
        key_rows,
        value_rows,
        decay_log,
        residual,
        out_gate,
        attn_gain,
        moe_gain,
        routes,
        route_weights,
        w_gate,
        w_up,
        w_down,
    ):
        tokens, columns = queries.shape
        heads = decay_log.shape[1]
        hd = columns // heads
        _, whole_rows, width = w_gate.shape
        even = whole_rows % (16 * n_rep) == 0
        hidden_rows = whole_rows // n_rep if even else whole_rows
        plane = n_exp * n_seq
        slots = n_seq * SLOTS
        vmem = pl.BlockSpec(memory_space=pltpu.VMEM)
        hbm = pl.BlockSpec(memory_space=pltpu.HBM)
        dma = pltpu.SemaphoreType.DMA
        cut = hidden_rows // 192 * 128
        if 2 < n_seq <= SHORT and even and cut > 0:
            wide = columns + 128
            return pl.pallas_call(
                lambda *refs: direct_kernel(n_seq, n_exp, n_rep, *refs),
                name="layer",
                out_shape=pltpu.VMEM((tokens, columns), BF16),
                in_specs=[hbm] * 13,
                out_specs=vmem,
                scratch_shapes=[
                    pltpu.VMEM((tokens, columns), BF16),
                    pltpu.VMEM((tokens, columns), BF16),
                    pltpu.VMEM((heads, tokens), F32),
                    pltpu.VMEM((tokens, columns), BF16),
                    pltpu.VMEM((2, tokens), jnp.int32),
                    pltpu.VMEM((2, tokens), F32),
                    pltpu.VMEM((tokens, columns), BF16),
                    pltpu.VMEM((tokens, columns), BF16),
                    pltpu.VMEM((1, columns), F32),
                    pltpu.VMEM((1, columns), F32),
                    pltpu.VMEM((hidden_rows, width), BF16),
                    pltpu.VMEM((hidden_rows, width), BF16),
                    pltpu.VMEM((n_exp, whole_rows, columns), BF16),
                    pltpu.VMEM((heads, hd, hd), BF16),
                    pltpu.VMEM((heads, hd, hd), BF16),
                    pltpu.VMEM((heads, hd, hd), BF16),
                    pltpu.VMEM((heads, hd, hd), F32),
                    pltpu.VMEM((tokens, columns), BF16),
                    pltpu.VMEM((tokens, columns), F32),
                    pltpu.VMEM((tokens, columns), F32),
                    pltpu.VMEM((n_exp * n_rep, 8, tokens), F32),
                    pltpu.VMEM((n_exp * n_rep, n_exp * SLOTS, 128), F32),
                    pltpu.VMEM((1, 128), F32),
                    pltpu.VMEM((n_seq, 1, 128), F32),
                    pltpu.VMEM((n_exp, SLOTS, columns), BF16),
                    pltpu.VMEM((n_seq, n_exp, SLOTS, columns), BF16),
                    pltpu.VMEM((n_seq, n_exp, SLOTS, columns), BF16),
                    pltpu.VMEM((n_seq, n_exp, SLOTS, columns), BF16),
                    pltpu.VMEM((n_seq, n_exp, SLOTS, columns), BF16),
                    pltpu.VMEM((3, n_exp, SLOTS, columns), BF16),
                    pltpu.VMEM((3, n_exp, SLOTS, columns), BF16),
                    pltpu.VMEM((3, n_exp * SLOTS, columns), F32),
                    pltpu.VMEM((n_exp * SLOTS, columns), F32),
                    pltpu.VMEM((heads, 128), F32),
                    pltpu.VMEM((n_exp, SLOTS, columns), BF16),
                    pltpu.VMEM((n_rep, plane, SLOTS, columns), BF16),
                    pltpu.VMEM((2, n_exp, SLOTS, wide), BF16),
                    pltpu.VMEM((n_rep, plane, SLOTS, wide), BF16),
                    pltpu.VMEM((n_rep, slots, cut), BF16),
                    pltpu.VMEM((n_rep, slots, hidden_rows - cut), BF16),
                    pltpu.VMEM((plane, SLOTS, columns), BF16),
                    pltpu.VMEM((plane, SLOTS, columns), BF16),
                    dma((10,)),
                    dma((2 + n_exp,)),
                    pltpu.SemaphoreType.REGULAR,
                    dma((heads, PARTS)),
                    dma((heads, PARTS)),
                    dma,
                    dma,
                    dma,
                    dma,
                    dma((n_seq,)),
                    dma((n_seq,)),
                    dma((n_seq,)),
                    dma((n_seq,)),
                    dma((n_seq,)),
                    dma((2, n_seq)),
                    dma((3,)),
                    dma((3,)),
                    dma,
                    dma,
                    dma,
                    dma((n_seq,)),
                    dma((2,)),
                    dma((2,)),
                    dma((2,)),
                    dma((2,)),
                    dma,
                    dma((plane,)),
                ],
                compiler_params=pltpu.CompilerParams(
                    collective_id=0, has_side_effects=True, vmem_limit_bytes=63000000
                ),
            )(
                key_rows,
                value_rows,
                decay_log.T,
                queries,
                routes.T,
                route_weights.T,
                residual,
                out_gate,
                attn_gain.reshape(1, columns),
                moe_gain.reshape(1, columns),
                w_gate,
                w_up,
                w_down,
            )
        return pl.pallas_call(
            lambda *refs: chain_kernel(n_seq, n_exp, n_rep, *refs),
            name="layer",
            out_shape=pltpu.VMEM((tokens, columns), BF16),
            in_specs=[hbm] * 13,
            out_specs=vmem,
            scratch_shapes=[
                pltpu.VMEM((tokens, columns), BF16),
                pltpu.VMEM((tokens, columns), BF16),
                pltpu.VMEM((heads, tokens), F32),
                pltpu.VMEM((tokens, columns), BF16),
                pltpu.VMEM((2, tokens), jnp.int32),
                pltpu.VMEM((2, tokens), F32),
                pltpu.VMEM((tokens, columns), BF16),
                pltpu.VMEM((tokens, columns), BF16),
                pltpu.VMEM((1, columns), F32),
                pltpu.VMEM((1, columns), F32),
                pltpu.VMEM((hidden_rows, width), BF16),
                pltpu.VMEM((hidden_rows, width), BF16),
                pltpu.VMEM((hidden_rows, width), BF16),
                pltpu.VMEM((heads, hd, hd), BF16),
                pltpu.VMEM((heads, hd, hd), BF16),
                pltpu.VMEM((heads, hd, hd), F32),
                pltpu.VMEM((tokens, columns), F32),
                pltpu.VMEM((tokens, columns), F32),
                pltpu.VMEM((n_exp * n_rep, 8, tokens), F32),
                pltpu.VMEM((n_exp, SLOTS, columns), BF16),
                pltpu.VMEM((n_rep, plane, SLOTS, columns), BF16),
                pltpu.VMEM((n_exp, slots, columns), BF16),
                pltpu.VMEM((n_exp, slots, columns), BF16),
                pltpu.VMEM((plane, SLOTS, columns), BF16),
                pltpu.VMEM((plane, SLOTS, columns), BF16),
                dma((10,)),
                dma((3,)),
                pltpu.SemaphoreType.REGULAR,
                dma((heads, PARTS)),
                dma((heads, PARTS)),
                dma,
                dma,
                dma,
                dma,
                dma,
                dma,
                dma((n_exp,)),
                dma((n_exp,)),
                dma,
                dma,
            ],
            compiler_params=pltpu.CompilerParams(collective_id=0, has_side_effects=True, vmem_limit_bytes=63000000),
        )(
            key_rows,
            value_rows,
            decay_log.T,
            queries,
            routes.T,
            route_weights.T,
            residual,
            out_gate,
            attn_gain.reshape(1, columns),
            moe_gain.reshape(1, columns),
            w_gate,
            w_up,
            w_down,
        )

    block = P(("groups", "seq"), ("exp", "rep"))
    gain = P(("exp", "rep"))
    route = P(("groups", "seq"), None)
    weight = P("exp", "seq", None)
    return jax.shard_map(
        shards,
        mesh=mesh,
        in_specs=(block,) * 6 + (gain, gain, route, route) + (weight,) * 3,
        out_specs=block,
        check_vma=False,
    )
```
